32 devices in a mesh: model: 4 (over z), data: 8 (over y, x, core).
Axes of the slice: x: 2, y: 2, z: 4, core: 2. Of those that a mesh axis runs over, the one named last changes fastest.
Arguments:
- emb_param: float32 [16384, 768], P('model', 'data')
- head_param: float32 [768, 16384], P('data', 'model')
- emb_grad: float32 [8, 16384, 768], P('data', 'model')
- head_grad: float32 [8, 768, 16384], P('data', None, 'model')
- emb_row: float32 [16384], P('model')
- emb_col: float32 [768], P('data')
- head_row: float32 [16384], P('model')
- head_col: float32 [768], P('data')
Outputs:
- output 1: float32 [16384, 768], P('model', 'data')
- output 2: float32 [768, 16384], P('data', 'model')
- output 3: float32 [16384], P('model')
- output 4: float32 [768], P('data')
- output 5: float32 [16384], P('model')
- output 6: float32 [768], P('data')
- output 7: bfloat16 [16384, 768], P('model', 'data')
- output 8: bfloat16 [768, 16384], P('data', 'model')
All inputs are finite; a program needn't handle non-finite values.
Results may differ from the reference program's by a relative error of at most 0.001.
Values sent between devices are 32-bit elements.
A program may use at most 1 GiB of HBM per device.

```python
import jax
import jax.numpy as jnp

VOCAB_SIZE = 16384
EMBED_DIM = 768
DATA_REPLICAS = 8
TRAIN_STEP = 10

DECAY_EXP = 0.8
EPS_ONE = 1e-30
CLIP_LIMIT = 1.0
SCALE_FLOOR = 1e-3
LEARN_RATE = float(TRAIN_STEP) ** -0.5
BETA_TWO = 1.0 - float(TRAIN_STEP) ** -DECAY_EXP


def vocab_trend(count):
    position = jnp.arange(count, dtype=jnp.float32) / count
    return 0.4 + 1.2 * (1.0 - position)


def touch_mask(mask_key):
    freq_tier = (8 * jnp.arange(VOCAB_SIZE, dtype=jnp.int32)) // VOCAB_SIZE
    limit = jnp.right_shift(jnp.full((VOCAB_SIZE,), 1024, jnp.int32), freq_tier)
    draws = jax.random.randint(mask_key, (DATA_REPLICAS, VOCAB_SIZE), 0, 1024, dtype=jnp.int32)
    touched = (draws < limit[None, :]).astype(jnp.float32)
    return touched, limit.astype(jnp.float32) / 1024.0


def setup_inputs(seed: int = 0) -> dict:
    rand_keys = jax.random.split(jax.random.key(seed), 16)
    row_trend = vocab_trend(VOCAB_SIZE)
    col_trend = 0.5 + jnp.arange(EMBED_DIM, dtype=jnp.float32) / EMBED_DIM
    rep_scale = DATA_REPLICAS ** -0.5
    emb_param = jax.random.normal(rand_keys[0], (VOCAB_SIZE, EMBED_DIM), jnp.float32) * row_trend[:, None] * col_trend[None, :]
    head_param = 0.5 * jax.random.normal(rand_keys[1], (EMBED_DIM, VOCAB_SIZE), jnp.float32) * col_trend[:, None] * row_trend[None, :]
    emb_rows = jnp.exp(0.5 * jax.random.normal(rand_keys[2], (VOCAB_SIZE,), jnp.float32)) * row_trend
    emb_cols = jnp.exp(0.5 * jax.random.normal(rand_keys[3], (EMBED_DIM,), jnp.float32))
    head_rows = jnp.exp(0.5 * jax.random.normal(rand_keys[4], (VOCAB_SIZE,), jnp.float32)) * row_trend
    head_cols = jnp.exp(0.5 * jax.random.normal(rand_keys[5], (EMBED_DIM,), jnp.float32))
    touched, density = touch_mask(rand_keys[6])
    emb_grad = (jax.random.normal(rand_keys[7], (DATA_REPLICAS, VOCAB_SIZE, EMBED_DIM), jnp.float32)
                * touched[:, :, None] * (rep_scale * emb_rows)[None, :, None] * emb_cols[None, None, :])
    head_grad = (jax.random.normal(rand_keys[8], (DATA_REPLICAS, EMBED_DIM, VOCAB_SIZE), jnp.float32)
                 * (rep_scale * head_cols)[None, :, None] * head_rows[None, None, :])
    emb_row = 0.3 * density * jnp.exp(0.7 * jax.random.normal(rand_keys[9], (VOCAB_SIZE,), jnp.float32))
    emb_col = 0.1 * jnp.exp(0.7 * jax.random.normal(rand_keys[10], (EMBED_DIM,), jnp.float32))
    head_row = 0.3 * jnp.exp(0.7 * jax.random.normal(rand_keys[11], (VOCAB_SIZE,), jnp.float32))
    head_col = 0.3 * jnp.exp(0.7 * jax.random.normal(rand_keys[12], (EMBED_DIM,), jnp.float32))
    return {"emb_param": emb_param, "head_param": head_param, "emb_grad": emb_grad, "head_grad": head_grad,
            "emb_row": emb_row, "emb_col": emb_col, "head_row": head_row, "head_col": head_col}


def adafactor_matrix(param, grad_sum, row_old, col_old, vocab_axis):
    embed_axis = 1 - vocab_axis
    grad_sq = grad_sum * grad_sum + EPS_ONE
    row_new = BETA_TWO * row_old + (1.0 - BETA_TWO) * jnp.mean(grad_sq, axis=embed_axis)
    col_new = BETA_TWO * col_old + (1.0 - BETA_TWO) * jnp.mean(grad_sq, axis=vocab_axis)
    vhat = jnp.expand_dims(row_new, embed_axis) * jnp.expand_dims(col_new, vocab_axis) / jnp.mean(row_new)
    update = grad_sum / jnp.sqrt(vhat)
    update = update / jnp.maximum(1.0, jnp.sqrt(jnp.mean(update * update)) / CLIP_LIMIT)
    step_scale = LEARN_RATE * jnp.maximum(SCALE_FLOOR, jnp.sqrt(jnp.mean(param * param)))
    return param - step_scale * update, row_new, col_new


def reference(emb_param, head_param, emb_grad, head_grad, emb_row, emb_col, head_row, head_col):
    emb_sum = jnp.sum(emb_grad, axis=0)
    head_sum = jnp.sum(head_grad, axis=0)
    emb_new, emb_row_new, emb_col_new = adafactor_matrix(emb_param, emb_sum, emb_row, emb_col, 0)
    head_new, head_row_new, head_col_new = adafactor_matrix(head_param, head_sum, head_row, head_col, 1)
    return (emb_new, head_new, emb_row_new, emb_col_new, head_row_new, head_col_new,
            emb_new.astype(jnp.bfloat16), head_new.astype(jnp.bfloat16))
```

```python
import functools

import jax
import jax.numpy as jnp
from jax import lax
from jax.experimental import pallas as pl
from jax.experimental.pallas import tpu as pltpu
from jax.sharding import PartitionSpec as P

TRAIN_STEP = 10
DECAY_EXP = 0.8
EPS_ONE = 1e-30
CLIP_LIMIT = 1.0
SCALE_FLOOR = 1e-3
LEARN_RATE = float(TRAIN_STEP) ** -0.5
BETA_TWO = 1.0 - float(TRAIN_STEP) ** -DECAY_EXP

VOCAB = 16384
EMBED = 768
ROWS = VOCAB // 4
COLS = EMBED // 8
CHUNKS = 8
WIDTH = ROWS // 2 // CHUNKS
LANES = 128
TILES = WIDTH // LANES
BLOCKS = 2 * CHUNKS
MESH = pl.DeviceIdType.MESH
PLANE = ((0, 1), (1, 0), (1, 1))


def exchange_kernel(emb_ref, head_ref, emb_p_ref, head_p_ref, emb_r_ref, head_r_ref, emb_c_ref, head_c_ref,
                    emb_out, head_out, row_out, small_out, scale_out,
                    own_e, in0_e, sum_e, sum_h, in0_h, in1_e, in1_h, in2_e, in2_h, peer_e, peer_h,
                    rows, stage_e, stage_h, par_e, par_h, rp_own, rp_in, col_acc, t_acc, rsum, psum, m_own, m_in, s_own, s_in,
                    ld_e, ld_h, s0e_s, s0e_r, s0h_s, s0h_r, s1e_s, s1e_r, s1h_s, s1h_r, s2e_s, s2e_r, s2h_s, s2h_r,
                    de_s, de_r, dh_s, dh_r, rp_s, rp_r, fw_s, fw_r, m_s, m_r, sc_s, sc_r, p_sem, out_sem):
    model = lax.axis_index("model")
    data = lax.axis_index("data")
    c = data % 2
    x = (data // 2) % 2
    y = data // 4
    oc, ox, oy = 1 - c, 1 - x, 1 - y

    def plane_id(fy, fx, fc):
        step = fy * (4 - 8 * y) + fx * (2 - 4 * x) + fc * (1 - 2 * c)
        return (model, data + step)

    def column_id(dz, fc):
        return ((model + dz) % 4, data + fc * (1 - 2 * c))

    core_peer, x_peer, y_peer = plane_id(0, 0, 1), plane_id(0, 1, 0), plane_id(1, 0, 0)

    def remote(src, dst, send, recv, peer):
        return pltpu.make_async_remote_copy(src_ref=src, dst_ref=dst, send_sem=send, recv_sem=recv,
                                            device_id=peer, device_id_type=MESH)

    def vocab_at(core, k):
        return pl.ds(pl.multiple_of(core * (ROWS // 2) + k * WIDTH, WIDTH), WIDTH)

    def load_e(k):
        return pltpu.make_async_copy(emb_ref.at[vocab_at(c, k), :], own_e.at[k], ld_e.at[k])

    def load_h(k):
        return pltpu.make_async_copy(head_ref.at[:, :, :, :, vocab_at(c, k)], sum_h.at[k], ld_h.at[k])

    def zero_e(k):
        return remote(emb_ref.at[vocab_at(oc, k), :], in0_e.at[k], s0e_s.at[k], s0e_r.at[k], core_peer)

    def zero_h(k):
        return remote(head_ref.at[:, :, :, :, vocab_at(oc, k)], in0_h.at[k], s0h_s.at[k], s0h_r.at[k], core_peer)

    def one_e(k):
        return remote(sum_e.at[k, oy], in1_e.at[k], s1e_s.at[k], s1e_r.at[k], y_peer)

    def one_h(k):
        return remote(sum_h.at[k, :, ox], in1_h.at[k], s1h_s.at[k], s1h_r.at[k], x_peer)

    def two_e(k):
        return remote(in1_e.at[k, ox], in2_e.at[k], s2e_s.at[k], s2e_r.at[k], x_peer)

    def two_h(k):
        return remote(in1_h.at[k, oy], in2_h.at[k], s2h_s.at[k], s2h_r.at[k], y_peer)

    def swap_e(k):
        return remote(in2_e.at[k, oc], peer_e.at[k], de_s.at[k], de_r.at[k], core_peer)

    def swap_h(k):
        return remote(in2_h.at[k, oc], peer_h.at[k], dh_s.at[k], dh_r.at[k], core_peer)

    def row_msg(k, i):
        fy, fx = PLANE[i]
        return remote(rp_own.at[k], rp_in.at[i, k], rp_s.at[i, k], rp_r.at[i, k], plane_id(fy, fx, 0))

    def row_fwd(k):
        return remote(rows.at[c * CHUNKS + k], rows.at[c * CHUNKS + k], fw_s.at[k], fw_r.at[k], core_peer)

    def row_fwd_in(k):
        return remote(rows.at[oc * CHUNKS + k], rows.at[oc * CHUNKS + k], fw_s.at[k], fw_r.at[k], core_peer)

    par_loads = (pltpu.make_async_copy(emb_p_ref, par_e, p_sem.at[0]), pltpu.make_async_copy(head_p_ref, par_h, p_sem.at[1]))

    for k in range(CHUNKS):
        load_e(k).start()
        load_h(k).start()

    barrier = pltpu.get_barrier_semaphore()
    greeted = 0
    for fy in range(2):
        for fx in range(2):
            for fc in range(2):
                if fy + fx + fc:
                    pl.semaphore_signal(barrier, inc=1, device_id=plane_id(fy, fx, fc), device_id_type=MESH)
                    greeted += 1
    for dz in range(1, 4):
        for fc in range(2):
            pl.semaphore_signal(barrier, inc=1, device_id=column_id(dz, fc), device_id_type=MESH)
            greeted += 1
    pl.semaphore_wait(barrier, greeted)

    for k in range(CHUNKS):
        zero_e(k).start()
        zero_h(k).start()
    for cp in par_loads:
        cp.start()

    col_acc[...] = jnp.zeros_like(col_acc)
    t_acc[...] = jnp.zeros_like(t_acc)
    rsum[...] = jnp.zeros_like(rsum)
    psum[...] = jnp.zeros_like(psum)

    def combine_cores(k):
        load_e(k).wait()
        zero_e(k).wait_recv()
        for j in range(EMBED // LANES):
            part = pl.ds(LANES * j, LANES)
            strip = (own_e[k, :, part] + in0_e[k, :, part]).T
            at = 0
            while at < LANES:
                eighth, row = divmod(LANES * j + at, COLS)
                size = min(LANES - at, COLS - row)
                sum_e[k, eighth // 4, eighth // 2 % 2, eighth % 2, row:row + size, :] = strip[at:at + size, :]
                at += size
        one_e(k).start()
        load_h(k).wait()
        zero_h(k).wait_recv()
        for a in range(2):
            for b in range(2):
                sum_h[k, a, b] = sum_h[k, a, b] + in0_h[k, a, b]
        one_h(k).start()

    def first_sum(k):
        one_e(k).wait_recv()
        in1_e[k, ox] = in1_e[k, ox] + sum_e[k, y, ox]
        two_e(k).start()
        in1_e[k, x] = in1_e[k, x] + sum_e[k, y, x]
        one_h(k).wait_recv()
        in1_h[k, oy] = in1_h[k, oy] + sum_h[k, oy, x]
        two_h(k).start()
        in1_h[k, y] = in1_h[k, y] + sum_h[k, y, x]

    def finish(k):
        two_e(k).wait_recv()
        for core in range(2):
            in2_e[k, core] = in2_e[k, core] + in1_e[k, x, core]
        swap_e(k).start()
        two_h(k).wait_recv()
        for core in range(2):
            in2_h[k, core] = in2_h[k, core] + in1_h[k, y, core]
        swap_h(k).start()
        for t, total in enumerate((in2_e, in2_h)):
            for i in range(TILES):
                row_part = jnp.zeros((1, LANES), jnp.float32)
                for core in range(2):
                    g = total[k, core, :, i * LANES:(i + 1) * LANES]
                    sq = g * g + EPS_ONE
                    col_acc[t, core] = col_acc[t, core] + sq
                    row_part = row_part + jnp.sum(sq, axis=0, keepdims=True)
                rp_own[k, t * TILES + i:t * TILES + i + 1, :] = row_part
        for i in range(3):
            row_msg(k, i).start()

    def row_stats(k):
        for i in range(3):
            row_msg(k, i).wait_recv()
        block = c * CHUNKS + k
        row_sq = (rp_own[k] + rp_in[0, k]) + (rp_in[1, k] + rp_in[2, k])
        old = jnp.concatenate([emb_r_ref[block], head_r_ref[block]], axis=0)
        row_new = BETA_TWO * old + (1.0 - BETA_TWO) * (row_sq / EMBED)
        rows[block] = row_new
        rsum[...] = rsum[...] + row_new
        inv = 1.0 / row_new
        for t, total in enumerate((in2_e, in2_h)):
            for i in range(TILES):
                r = inv[t * TILES + i:t * TILES + i + 1, :]
                for core in range(2):
                    g = total[k, core, :, i * LANES:(i + 1) * LANES]
                    t_acc[t, core] = t_acc[t, core] + (g * g) * r

    def out_e(block):
        at = pl.ds(pl.multiple_of(block * WIDTH, WIDTH), WIDTH)
        return pltpu.make_async_copy(stage_e.at[:, at], emb_out.at[:, at], out_sem.at[0])

    def out_h(block):
        at = pl.ds(pl.multiple_of(block * WIDTH, WIDTH), WIDTH)
        return pltpu.make_async_copy(stage_h.at[:, at], head_out.at[:, at], out_sem.at[1])

    def scale_rows(block, get_e, get_h):
        factor = lax.rsqrt(rows[block])
        base = pl.multiple_of(block * WIDTH, WIDTH)
        for i in range(TILES):
            lanes = slice(i * LANES, (i + 1) * LANES)
            at = pl.ds(base + i * LANES, LANES)
            stage_e[:, at] = get_e(lanes) * factor[i:i + 1, :]
            stage_h[:, at] = get_h(lanes) * factor[TILES + i:TILES + i + 1, :]
        out_e(block).start()
        out_h(block).start()

    def scale_own(k):
        scale_rows(c * CHUNKS + k, lambda lanes: in2_e[k, c, :, lanes], lambda lanes: in2_h[k, c, :, lanes])

    def scale_peer(k):
        row_fwd_in(k).wait_recv()
        swap_e(k).wait_recv()
        swap_h(k).wait_recv()
        scale_rows(oc * CHUNKS + k, lambda lanes: peer_e[k, :, lanes], lambda lanes: peer_h[k, :, lanes])

    def param_sq(k):
        size = ROWS // CHUNKS
        at = pl.ds(pl.multiple_of(k * size, size), size)
        for t, par in enumerate((par_e, par_h)):
            v = par[:, at]
            v = jnp.sum(v * v, axis=0, keepdims=True)
            for i in range(size // LANES):
                psum[t:t + 1, :] = psum[t:t + 1, :] + v[:, i * LANES:(i + 1) * LANES]

    combine_cores(0)
    for cp in par_loads:
        cp.wait()

    @pl.loop(0, CHUNKS)
    def _(k):
        @pl.when(k + 1 < CHUNKS)
        def _():
            combine_cores(k + 1)

        param_sq(k)
        first_sum(k)

        @pl.when(k >= 1)
        def _():
            finish(k - 1)

        @pl.when(k >= 2)
        def _():
            row_stats(k - 2)
            row_fwd(k - 2).start()
            scale_own(k - 2)

        @pl.when(k >= 3)
        def _():
            scale_peer(k - 3)

    finish(CHUNKS - 1)
    row_stats(CHUNKS - 2)
    row_fwd(CHUNKS - 2).start()
    row_stats(CHUNKS - 1)
    row_fwd(CHUNKS - 1).start()

    lane = lax.broadcasted_iota(jnp.int32, (1, LANES), 1)
    diag = lax.broadcasted_iota(jnp.int32, (COLS, LANES), 0) == lax.broadcasted_iota(jnp.int32, (COLS, LANES), 1)

    def as_row(acc):
        col = jnp.sum(acc, axis=1, keepdims=True)
        return jnp.sum(jnp.where(diag, col, 0.0), axis=0, keepdims=True)

    def total_of(v):
        return jnp.sum(jnp.sum(v, axis=1, keepdims=True), axis=0, keepdims=True)

    for t in range(2):
        r_part = total_of(rsum[t * TILES:(t + 1) * TILES, :])
        p_part = jnp.sum(psum[t:t + 1, :], axis=1, keepdims=True)
        for core in range(2):
            row = as_row(col_acc[t, core])
            row = jnp.where(lane == COLS, r_part, jnp.where(lane == COLS + 1, p_part, row))
            m_own[core, 2 * t:2 * t + 1, :] = row
            m_own[core, 2 * t + 1:2 * t + 2, :] = as_row(t_acc[t, core])

    columns = [(dz, fc) for dz in range(4) for fc in range(2) if dz + fc]

    def column_msg(i):
        dz, fc = columns[i]
        slot = columns.index(((4 - dz) % 4, fc))
        return remote(m_own.at[oc if fc else c], m_in.at[slot], m_s.at[i], m_r.at[slot], column_id(dz, fc))

    def column_msg_in(i):
        dz, fc = columns[i]
        return remote(m_own.at[c], m_in.at[i], m_s.at[i], m_r.at[i], column_id(dz, fc))

    for i in range(len(columns)):
        column_msg(i).start()

    scale_own(CHUNKS - 2)
    scale_own(CHUNKS - 1)
    for i in range(len(columns)):
        column_msg_in(i).wait_recv()

    total = m_own[c]
    for i in range(len(columns)):
        total = total + m_in[i]
    factors, means, message = [], [], jnp.zeros((1, LANES), jnp.float32)
    for t, c_ref in enumerate((emb_c_ref, head_c_ref)):
        cols = total[2 * t:2 * t + 1, :]
        r_mean = jnp.sum(jnp.where(lane == COLS, cols, 0.0), axis=1, keepdims=True) / VOCAB
        p_col = jnp.sum(jnp.where(lane == COLS + 1, cols, 0.0), axis=1, keepdims=True)
        col_new = BETA_TWO * c_ref[...] + (1.0 - BETA_TWO) * (cols[:, :COLS] / VOCAB)
        u_sq = jnp.sum(total[2 * t + 1:2 * t + 2, :COLS] * (r_mean / col_new), axis=1, keepdims=True)
        message = jnp.where(lane == 2 * t, u_sq, jnp.where(lane == 2 * t + 1, 0.5 * p_col, message))
        small_out[t:t + 1, :COLS] = col_new
        factors.append(lax.rsqrt(col_new) * jnp.sqrt(r_mean))
    s_own[...] = message

    flips = [(fy, fx, fc) for fy in range(2) for fx in range(2) for fc in range(2) if fy + fx + fc]

    def scalar_msg(i):
        return remote(s_own, s_in.at[i], sc_s.at[i], sc_r.at[i], plane_id(*flips[i]))

    for i in range(len(flips)):
        scalar_msg(i).start()
    square = diag[:, :COLS]
    factor_cols = [jnp.sum(jnp.where(square, factor, 0.0), axis=1, keepdims=True) for factor in factors]

    @pl.loop(CHUNKS - 3, CHUNKS)
    def _(k):
        scale_peer(k)

    row_out[...] = rows[...]
    for i in range(len(flips)):
        scalar_msg(i).wait_recv()
    message = s_own[...]
    for i in range(len(flips)):
        message = message + s_in[i]
    count = float(VOCAB * EMBED)
    steps = []
    for t in range(2):
        u_sq = jnp.sum(jnp.where(lane == 2 * t, message, 0.0), axis=1, keepdims=True)
        p_sq = jnp.sum(jnp.where(lane == 2 * t + 1, message, 0.0), axis=1, keepdims=True)
        u_rms = jnp.sqrt(u_sq / count)
        p_rms = jnp.sqrt(p_sq / count)
        steps.append(LEARN_RATE * jnp.maximum(SCALE_FLOOR, p_rms) / jnp.maximum(1.0, u_rms / CLIP_LIMIT))
    for t in range(2):
        scale_out[t] = jnp.broadcast_to(factor_cols[t] * steps[t], (COLS, LANES))

    @pl.loop(0, CHUNKS)
    def _(k):
        for make in (zero_e, zero_h, one_e, one_h, two_e, two_h, swap_e, swap_h, row_fwd):
            make(k).wait_send()
        for i in range(3):
            row_msg(k, i).wait_send()

    for i in range(len(columns)):
        column_msg(i).wait_send()
    for i in range(len(flips)):
        scalar_msg(i).wait_send()
    pltpu.make_async_copy(stage_e, emb_out, out_sem.at[0]).wait()
    pltpu.make_async_copy(stage_h, head_out, out_sem.at[1]).wait()


def update_kernel(emb_p, head_p, emb_g, head_g, rows, small, scale,
                  emb_new, head_new, emb_rows, head_rows, emb_cols, head_cols, emb_half, head_half):
    e_new = emb_p[...] - emb_g[...] * scale[0, :, 0:1]
    emb_new[...] = e_new
    emb_half[...] = e_new.astype(jnp.bfloat16)
    h_new = head_p[...] - head_g[...] * scale[1, :, 0:1]
    head_new[...] = h_new
    head_half[...] = h_new.astype(jnp.bfloat16)

    @pl.when(pl.program_id(0) == 0)
    def _():
        emb_rows[...] = rows[:, :TILES, :]
        head_rows[...] = rows[:, TILES:, :]
        emb_cols[...] = small[0:1, :COLS]
        head_cols[...] = small[1:2, :COLS]


def local_step(emb_p, head_p, emb_g, head_g, emb_r, emb_c, head_r, head_c):
    f32 = jnp.float32
    n, w = CHUNKS, WIDTH
    dma = pltpu.SemaphoreType.DMA
    hbm = pl.BlockSpec(memory_space=pl.ANY)
    vmem = pl.BlockSpec(memory_space=pltpu.VMEM)
    rows_shape = (BLOCKS, TILES, LANES)
    table = jax.ShapeDtypeStruct((COLS, ROWS), f32)
    half = jax.ShapeDtypeStruct((COLS, ROWS), jnp.bfloat16)
    emb_p = emb_p.T
    scratch = [
        pltpu.VMEM((n, w, EMBED), f32), pltpu.VMEM((n, w, EMBED), f32),
        pltpu.VMEM((n, 2, 2, 2, COLS, w), f32), pltpu.VMEM((n, 2, 2, 2, COLS, w), f32), pltpu.VMEM((n, 2, 2, 2, COLS, w), f32),
        pltpu.VMEM((n, 2, 2, COLS, w), f32), pltpu.VMEM((n, 2, 2, COLS, w), f32),
        pltpu.VMEM((n, 2, COLS, w), f32), pltpu.VMEM((n, 2, COLS, w), f32),
        pltpu.VMEM((n, COLS, w), f32), pltpu.VMEM((n, COLS, w), f32),
        pltpu.VMEM((BLOCKS, 2 * TILES, LANES), f32),
        pltpu.VMEM((COLS, ROWS), f32), pltpu.VMEM((COLS, ROWS), f32),
        pltpu.VMEM((COLS, ROWS), f32), pltpu.VMEM((COLS, ROWS), f32),
        pltpu.VMEM((n, 2 * TILES, LANES), f32), pltpu.VMEM((3, n, 2 * TILES, LANES), f32),
        pltpu.VMEM((2, 2, COLS, LANES), f32), pltpu.VMEM((2, 2, COLS, LANES), f32),
        pltpu.VMEM((2 * TILES, LANES), f32), pltpu.VMEM((2, LANES), f32),
        pltpu.VMEM((2, 4, LANES), f32), pltpu.VMEM((7, 4, LANES), f32),
        pltpu.VMEM((1, LANES), f32), pltpu.VMEM((7, 1, LANES), f32),
    ]
    scratch += [dma((n,))] * 18 + [dma((3, n))] * 2 + [dma((n,))] * 2 + [dma((7,))] * 4 + [dma((2,))] * 2
    emb_s, head_s, row_new, small, scale = pl.pallas_call(
        exchange_kernel,
        out_shape=(table, table, jax.ShapeDtypeStruct((BLOCKS, 2 * TILES, LANES), f32),
                   jax.ShapeDtypeStruct((2, LANES), f32), jax.ShapeDtypeStruct((2, COLS, LANES), f32)),
        in_specs=[hbm] * 4 + [vmem] * 4,
        out_specs=(hbm, hbm, vmem, vmem, vmem),
        scratch_shapes=scratch,
        compiler_params=pltpu.CompilerParams(collective_id=0, has_side_effects=True, vmem_limit_bytes=63 * 2 ** 20),
        name="exchange",
    )(emb_g.reshape(ROWS, EMBED), head_g.reshape(2, 2, 2, COLS, ROWS), emb_p, head_p,
      emb_r.reshape(rows_shape), head_r.reshape(rows_shape), emb_c.reshape(1, COLS), head_c.reshape(1, COLS))

    steps = 4
    part = ROWS // steps
    wide = pl.BlockSpec((COLS, part), lambda i: (0, i))

    def whole(*shape):
        return pl.BlockSpec(shape, lambda i: (0,) * len(shape))

    outs = pl.pallas_call(
        update_kernel,
        grid=(steps,),
        out_shape=(table, table,
                   jax.ShapeDtypeStruct(rows_shape, f32), jax.ShapeDtypeStruct(rows_shape, f32),
                   jax.ShapeDtypeStruct((1, COLS), f32), jax.ShapeDtypeStruct((1, COLS), f32),
                   half, half),
        in_specs=[wide] * 4 + [whole(BLOCKS, 2 * TILES, LANES), whole(2, LANES), whole(2, COLS, LANES)],
        out_specs=(wide, wide, whole(*rows_shape), whole(*rows_shape), whole(1, COLS), whole(1, COLS), wide, wide),
        name="update",
    )(emb_p, head_p, emb_s, head_s, row_new, small, scale)
    emb_new, head_new, emb_rn, head_rn, emb_cn, head_cn, emb_half, head_half = outs
    return (emb_new.T, head_new, emb_rn.reshape(ROWS), emb_cn.reshape(COLS), head_rn.reshape(ROWS),
            head_cn.reshape(COLS), emb_half.T, head_half)


def solution(mesh):
    arg_specs = (P("model", "data"), P("data", "model"), P("data", "model", None), P("data", None, "model"),
                 P("model"), P("data"), P("model"), P("data"))
    result_specs = (P("model", "data"), P("data", "model"), P("model"), P("data"), P("model"), P("data"),
                    P("model", "data"), P("data", "model"))
    mapped = jax.shard_map(local_step, mesh=mesh, in_specs=arg_specs, out_specs=result_specs, check_vma=False)

    def update_tables(emb_param, head_param, emb_grad, head_grad, emb_row, emb_col, head_row, head_col):
        return mapped(emb_param, head_param, emb_grad, head_grad, emb_row, emb_col, head_row, head_col)

    return update_tables
```

```python
import functools

import jax
import jax.numpy as jnp
from jax import lax
from jax.experimental import pallas as pl
from jax.experimental.pallas import tpu as pltpu
from jax.sharding import PartitionSpec as P

TRAIN_STEP = 10
DECAY_EXP = 0.8
EPS_ONE = 1e-30
CLIP_LIMIT = 1.0
SCALE_FLOOR = 1e-3
LEARN_RATE = float(TRAIN_STEP) ** -0.5
BETA_TWO = 1.0 - float(TRAIN_STEP) ** -DECAY_EXP

VOCAB = 16384
EMBED = 768
ROWS = VOCAB // 4
COLS = EMBED // 8
CHUNKS = 8
WIDTH = ROWS // 2 // CHUNKS
LANES = 128
TILES = WIDTH // LANES
BLOCKS = 2 * CHUNKS
PARTS = 4
MESH = pl.DeviceIdType.MESH
PLANE = ((0, 1), (1, 0), (1, 1))


def exchange_kernel(emb_ref, head_ref, emb_p_ref, head_p_ref, emb_r_ref, head_r_ref, emb_c_ref, head_c_ref,
                    stage_e, stage_h, par_e, par_h, emb_rows_out, head_rows_out, emb_cols_out, head_cols_out, scale_out,
                    own_e, in0_e, sum_e, sum_h, in0_h, in1_e, in1_h, in2_e, in2_h, peer_e, peer_h,
                    rows, old_rows, old_cols, rp_own, rp_in, col_acc, t_acc, rsum, psum, m_own, m_in, s_own, s_in,
                    ld_e, ld_h, s0e_s, s0e_r, s0h_s, s0h_r, s1e_s, s1e_r, s1h_s, s1h_r, s2e_s, s2e_r, s2h_s, s2h_r,
                    de_s, de_r, dh_s, dh_r, rp_s, rp_r, fw_s, fw_r, m_s, m_r, sc_s, sc_r, in_sem):
    model = lax.axis_index("model")
    data = lax.axis_index("data")
    c = data % 2
    x = (data // 2) % 2
    y = data // 4
    oc, ox, oy = 1 - c, 1 - x, 1 - y

    def plane_id(fy, fx, fc):
        step = fy * (4 - 8 * y) + fx * (2 - 4 * x) + fc * (1 - 2 * c)
        return (model, data + step)

    def column_id(dz, fc):
        return ((model + dz) % 4, data + fc * (1 - 2 * c))

    core_peer, x_peer, y_peer = plane_id(0, 0, 1), plane_id(0, 1, 0), plane_id(1, 0, 0)

    def remote(src, dst, send, recv, peer):
        return pltpu.make_async_remote_copy(src_ref=src, dst_ref=dst, send_sem=send, recv_sem=recv,
                                            device_id=peer, device_id_type=MESH)

    def vocab_at(core, k):
        return pl.ds(pl.multiple_of(core * (ROWS // 2) + k * WIDTH, WIDTH), WIDTH)

    def load_e(k):
        return pltpu.make_async_copy(emb_ref.at[vocab_at(c, k), :], own_e.at[k], ld_e.at[k])

    def load_h(k):
        return pltpu.make_async_copy(head_ref.at[:, :, :, :, vocab_at(c, k)], sum_h.at[k], ld_h.at[k])

    def zero_e(k):
        return remote(emb_ref.at[vocab_at(oc, k), :], in0_e.at[k], s0e_s.at[k], s0e_r.at[k], core_peer)

    def zero_h(k):
        return remote(head_ref.at[:, :, :, :, vocab_at(oc, k)], in0_h.at[k], s0h_s.at[k], s0h_r.at[k], core_peer)

    def one_e(k):
        return remote(sum_e.at[k, oy], in1_e.at[k], s1e_s.at[k], s1e_r.at[k], y_peer)

    def one_h(k):
        return remote(sum_h.at[k, :, ox], in1_h.at[k], s1h_s.at[k], s1h_r.at[k], x_peer)

    def two_e(k):
        return remote(in1_e.at[k, ox], in2_e.at[k], s2e_s.at[k], s2e_r.at[k], x_peer)

    def two_h(k):
        return remote(in1_h.at[k, oy], in2_h.at[k], s2h_s.at[k], s2h_r.at[k], y_peer)

    def swap_e(k):
        return remote(in2_e.at[k, oc], peer_e.at[k], de_s.at[k], de_r.at[k], core_peer)

    def swap_h(k):
        return remote(in2_h.at[k, oc], peer_h.at[k], dh_s.at[k], dh_r.at[k], core_peer)

    def row_msg(k, i):
        fy, fx = PLANE[i]
        return remote(rp_own.at[k], rp_in.at[i, k], rp_s.at[i, k], rp_r.at[i, k], plane_id(fy, fx, 0))

    def row_fwd(k):
        return remote(rows.at[c * CHUNKS + k], rows.at[c * CHUNKS + k], fw_s.at[k], fw_r.at[k], core_peer)

    def row_fwd_in(k):
        return remote(rows.at[oc * CHUNKS + k], rows.at[oc * CHUNKS + k], fw_s.at[k], fw_r.at[k], core_peer)

    small_loads = [pltpu.make_async_copy(src, dst, in_sem.at[i]) for i, (src, dst) in enumerate(
        ((emb_p_ref, par_e), (head_p_ref, par_h), (emb_r_ref, old_rows.at[0]), (head_r_ref, old_rows.at[1]),
         (emb_c_ref, old_cols.at[0]), (head_c_ref, old_cols.at[1])))]

    barrier = pltpu.get_barrier_semaphore()
    greeted = 0
    for fy in range(2):
        for fx in range(2):
            for fc in range(2):
                if fy + fx + fc:
                    pl.semaphore_signal(barrier, inc=1, device_id=plane_id(fy, fx, fc), device_id_type=MESH)
                    greeted += 1
    for dz in range(1, 4):
        for fc in range(2):
            pl.semaphore_signal(barrier, inc=1, device_id=column_id(dz, fc), device_id_type=MESH)
            greeted += 1
    for k in range(CHUNKS):
        load_e(k).start()
        load_h(k).start()
    pl.semaphore_wait(barrier, greeted)

    for k in range(CHUNKS):
        zero_e(k).start()
        zero_h(k).start()
    for cp in small_loads:
        cp.start()

    col_acc[...] = jnp.zeros_like(col_acc)
    t_acc[...] = jnp.zeros_like(t_acc)
    rsum[...] = jnp.zeros_like(rsum)
    psum[...] = jnp.zeros_like(psum)

    def combine_cores(k):
        load_e(k).wait()
        zero_e(k).wait_recv()
        for j in range(EMBED // LANES):
            part = pl.ds(LANES * j, LANES)
            strip = (own_e[k, :, part] + in0_e[k, :, part]).T
            at = 0
            while at < LANES:
                eighth, row = divmod(LANES * j + at, COLS)
                size = min(LANES - at, COLS - row)
                sum_e[k, eighth // 4, eighth // 2 % 2, eighth % 2, row:row + size, :] = strip[at:at + size, :]
                at += size
        one_e(k).start()
        load_h(k).wait()
        zero_h(k).wait_recv()
        for a in range(2):
            for b in range(2):
                sum_h[k, a, b] = sum_h[k, a, b] + in0_h[k, a, b]
        one_h(k).start()

    def first_sum(k):
        one_e(k).wait_recv()
        in1_e[k, ox] = in1_e[k, ox] + sum_e[k, y, ox]
        two_e(k).start()
        in1_e[k, x] = in1_e[k, x] + sum_e[k, y, x]
        one_h(k).wait_recv()
        in1_h[k, oy] = in1_h[k, oy] + sum_h[k, oy, x]
        two_h(k).start()
        in1_h[k, y] = in1_h[k, y] + sum_h[k, y, x]

    def finish(k):
        two_e(k).wait_recv()
        for core in range(2):
            in2_e[k, core] = in2_e[k, core] + in1_e[k, x, core]
        swap_e(k).start()
        two_h(k).wait_recv()
        for core in range(2):
            in2_h[k, core] = in2_h[k, core] + in1_h[k, y, core]
        swap_h(k).start()
        for t, total in enumerate((in2_e, in2_h)):
            for i in range(TILES):
                row_part = jnp.zeros((1, LANES), jnp.float32)
                for core in range(2):
                    g = total[k, core, :, i * LANES:(i + 1) * LANES]
                    sq = g * g + EPS_ONE
                    col_acc[t, core] = col_acc[t, core] + sq
                    row_part = row_part + jnp.sum(sq, axis=0, keepdims=True)
                rp_own[k, t * TILES + i:t * TILES + i + 1, :] = row_part
        for i in range(3):
            row_msg(k, i).start()

    def row_stats(k):
        for i in range(3):
            row_msg(k, i).wait_recv()
        block = c * CHUNKS + k
        row_sq = (rp_own[k] + rp_in[0, k]) + (rp_in[1, k] + rp_in[2, k])
        old = jnp.concatenate([old_rows[0, block], old_rows[1, block]], axis=0)
        row_new = BETA_TWO * old + (1.0 - BETA_TWO) * (row_sq / EMBED)
        rows[block] = row_new
        rsum[...] = rsum[...] + row_new
        inv = 1.0 / row_new
        for t, total in enumerate((in2_e, in2_h)):
            for i in range(TILES):
                r = inv[t * TILES + i:t * TILES + i + 1, :]
                for core in range(2):
                    g = total[k, core, :, i * LANES:(i + 1) * LANES]
                    t_acc[t, core] = t_acc[t, core] + (g * g) * r

    def scale_rows(block, get_e, get_h):
        factor = lax.rsqrt(rows[block])
        base = pl.multiple_of(block * WIDTH, WIDTH)
        for i in range(TILES):
            lanes = slice(i * LANES, (i + 1) * LANES)
            at = pl.ds(base + i * LANES, LANES)
            stage_e[:, at] = get_e(lanes) * factor[i:i + 1, :]
            stage_h[:, at] = get_h(lanes) * factor[TILES + i:TILES + i + 1, :]

    def scale_own(k):
        scale_rows(c * CHUNKS + k, lambda lanes: in2_e[k, c, :, lanes], lambda lanes: in2_h[k, c, :, lanes])

    def scale_peer(k):
        row_fwd_in(k).wait_recv()
        swap_e(k).wait_recv()
        swap_h(k).wait_recv()
        scale_rows(oc * CHUNKS + k, lambda lanes: peer_e[k, :, lanes], lambda lanes: peer_h[k, :, lanes])

    def param_sq(k):
        size = ROWS // CHUNKS
        at = pl.ds(pl.multiple_of(k * size, size), size)
        for t, par in enumerate((par_e, par_h)):
            v = par[:, at]
            v = jnp.sum(v * v, axis=0, keepdims=True)
            for i in range(size // LANES):
                psum[t:t + 1, :] = psum[t:t + 1, :] + v[:, i * LANES:(i + 1) * LANES]

    combine_cores(0)
    for cp in small_loads:
        cp.wait()

    @pl.loop(0, CHUNKS)
    def _(k):
        @pl.when(k + 1 < CHUNKS)
        def _():
            combine_cores(k + 1)

        param_sq(k)
        first_sum(k)

        @pl.when(k >= 1)
        def _():
            finish(k - 1)

        @pl.when(k >= 2)
        def _():
            row_stats(k - 2)
            row_fwd(k - 2).start()
            scale_own(k - 2)

        @pl.when(k >= 3)
        def _():
            scale_peer(k - 3)

    finish(CHUNKS - 1)
    row_stats(CHUNKS - 2)
    row_fwd(CHUNKS - 2).start()
    row_stats(CHUNKS - 1)
    row_fwd(CHUNKS - 1).start()

    lane = lax.broadcasted_iota(jnp.int32, (1, LANES), 1)
    diag = lax.broadcasted_iota(jnp.int32, (COLS, LANES), 0) == lax.broadcasted_iota(jnp.int32, (COLS, LANES), 1)

    def as_row(acc):
        col = jnp.sum(acc, axis=1, keepdims=True)
        return jnp.sum(jnp.where(diag, col, 0.0), axis=0, keepdims=True)

    def total_of(v):
        return jnp.sum(jnp.sum(v, axis=1, keepdims=True), axis=0, keepdims=True)

    for t in range(2):
        r_part = total_of(rsum[t * TILES:(t + 1) * TILES, :])
        p_part = jnp.sum(psum[t:t + 1, :], axis=1, keepdims=True)
        for core in range(2):
            row = as_row(col_acc[t, core])
            row = jnp.where(lane == COLS, r_part, jnp.where(lane == COLS + 1, p_part, row))
            m_own[core, 2 * t:2 * t + 1, :] = row
            m_own[core, 2 * t + 1:2 * t + 2, :] = as_row(t_acc[t, core])

    columns = [(dz, fc) for dz in range(4) for fc in range(2) if dz + fc]

    def column_msg(i):
        dz, fc = columns[i]
        slot = columns.index(((4 - dz) % 4, fc))
        return remote(m_own.at[oc if fc else c], m_in.at[slot], m_s.at[i], m_r.at[slot], column_id(dz, fc))

    def column_msg_in(i):
        dz, fc = columns[i]
        return remote(m_own.at[c], m_in.at[i], m_s.at[i], m_r.at[i], column_id(dz, fc))

    for i in range(len(columns)):
        column_msg(i).start()

    scale_own(CHUNKS - 2)
    scale_own(CHUNKS - 1)
    for i in range(len(columns)):
        column_msg_in(i).wait_recv()

    total = m_own[c]
    for i in range(len(columns)):
        total = total + m_in[i]
    factors, means, message = [], [], jnp.zeros((1, LANES), jnp.float32)
    for t, c_out in enumerate((emb_cols_out, head_cols_out)):
        cols = total[2 * t:2 * t + 1, :]
        r_mean = jnp.sum(jnp.where(lane == COLS, cols, 0.0), axis=1, keepdims=True) / VOCAB
        p_col = jnp.sum(jnp.where(lane == COLS + 1, cols, 0.0), axis=1, keepdims=True)
        col_new = BETA_TWO * old_cols[t] + (1.0 - BETA_TWO) * (cols[:, :COLS] / VOCAB)
        u_sq = jnp.sum(total[2 * t + 1:2 * t + 2, :COLS] * (r_mean / col_new), axis=1, keepdims=True)
        message = jnp.where(lane == 2 * t, u_sq, jnp.where(lane == 2 * t + 1, 0.5 * p_col, message))
        c_out[...] = col_new
        factors.append(lax.rsqrt(col_new) * jnp.sqrt(r_mean))
    s_own[...] = message

    flips = [(fy, fx, fc) for fy in range(2) for fx in range(2) for fc in range(2) if fy + fx + fc]

    def scalar_msg(i):
        return remote(s_own, s_in.at[i], sc_s.at[i], sc_r.at[i], plane_id(*flips[i]))

    for i in range(len(flips)):
        scalar_msg(i).start()
    square = diag[:, :COLS]
    factor_cols = [jnp.sum(jnp.where(square, factor, 0.0), axis=1, keepdims=True) for factor in factors]

    @pl.loop(CHUNKS - 3, CHUNKS)
    def _(k):
        scale_peer(k)

    emb_rows_out[...] = rows[:, :TILES, :]
    head_rows_out[...] = rows[:, TILES:, :]
    for i in range(len(flips)):
        scalar_msg(i).wait_recv()
    message = s_own[...]
    for i in range(len(flips)):
        message = message + s_in[i]
    count = float(VOCAB * EMBED)
    steps = []
    for t in range(2):
        u_sq = jnp.sum(jnp.where(lane == 2 * t, message, 0.0), axis=1, keepdims=True)
        p_sq = jnp.sum(jnp.where(lane == 2 * t + 1, message, 0.0), axis=1, keepdims=True)
        u_rms = jnp.sqrt(u_sq / count)
        p_rms = jnp.sqrt(p_sq / count)
        steps.append(LEARN_RATE * jnp.maximum(SCALE_FLOOR, p_rms) / jnp.maximum(1.0, u_rms / CLIP_LIMIT))
    for t in range(2):
        scale_out[t] = jnp.broadcast_to(factor_cols[t] * steps[t], (COLS, LANES))

    @pl.loop(0, CHUNKS)
    def _(k):
        for make in (zero_e, zero_h, one_e, one_h, two_e, two_h, swap_e, swap_h, row_fwd):
            make(k).wait_send()
        for i in range(3):
            row_msg(k, i).wait_send()

    for i in range(len(columns)):
        column_msg(i).wait_send()
    for i in range(len(flips)):
        scalar_msg(i).wait_send()


def update_kernel(emb_g, head_g, emb_p, head_p, emb_rows, head_rows, emb_cols, head_cols, scale,
                  emb_new, head_new, emb_rows_new, head_rows_new, emb_cols_new, head_cols_new, emb_half, head_half,
                  new_buf, half_buf, small_sem, new_sem, half_sem):
    small = [pltpu.make_async_copy(src, dst, small_sem.at[i]) for i, (src, dst) in enumerate(
        ((emb_rows, emb_rows_new), (head_rows, head_rows_new), (emb_cols, emb_cols_new), (head_cols, head_cols_new)))]
    for cp in small:
        cp.start()
    big = []
    size = ROWS // PARTS
    for i in range(PARTS):
        part = slice(i * size, (i + 1) * size)
        for t, (p, g, new, half) in enumerate(((emb_p, emb_g, emb_new, emb_half), (head_p, head_g, head_new, head_half))):
            value = p[:, part] - g[:, part] * scale[t, :, 0:1]
            new_buf[t, :, part] = value
            half_buf[t, :, part] = value.astype(jnp.bfloat16)
            big.append(pltpu.make_async_copy(new_buf.at[t, :, part], new.at[:, part], new_sem.at[t, i]))
            big.append(pltpu.make_async_copy(half_buf.at[t, :, part], half.at[:, part], half_sem.at[t, i]))
            big[-2].start()
            big[-1].start()
    for cp in small + big:
        cp.wait()


def local_step(emb_p, head_p, emb_g, head_g, emb_r, emb_c, head_r, head_c):
    f32 = jnp.float32
    n, w = CHUNKS, WIDTH
    dma = pltpu.SemaphoreType.DMA
    hbm = pl.BlockSpec(memory_space=pltpu.HBM)
    vmem = pl.BlockSpec(memory_space=pltpu.VMEM)
    rows_shape = (BLOCKS, TILES, LANES)
    table = jax.ShapeDtypeStruct((COLS, ROWS), f32)
    half = jax.ShapeDtypeStruct((COLS, ROWS), jnp.bfloat16)
    emb_p = emb_p.T
    scratch = [
        pltpu.VMEM((n, w, EMBED), f32), pltpu.VMEM((n, w, EMBED), f32),
        pltpu.VMEM((n, 2, 2, 2, COLS, w), f32), pltpu.VMEM((n, 2, 2, 2, COLS, w), f32), pltpu.VMEM((n, 2, 2, 2, COLS, w), f32),
        pltpu.VMEM((n, 2, 2, COLS, w), f32), pltpu.VMEM((n, 2, 2, COLS, w), f32),
        pltpu.VMEM((n, 2, COLS, w), f32), pltpu.VMEM((n, 2, COLS, w), f32),
        pltpu.VMEM((n, COLS, w), f32), pltpu.VMEM((n, COLS, w), f32),
        pltpu.VMEM((BLOCKS, 2 * TILES, LANES), f32),
        pltpu.VMEM((2, BLOCKS, TILES, LANES), f32), pltpu.VMEM((2, 1, COLS), f32),
        pltpu.VMEM((n, 2 * TILES, LANES), f32), pltpu.VMEM((3, n, 2 * TILES, LANES), f32),
        pltpu.VMEM((2, 2, COLS, LANES), f32), pltpu.VMEM((2, 2, COLS, LANES), f32),
        pltpu.VMEM((2 * TILES, LANES), f32), pltpu.VMEM((2, LANES), f32),
        pltpu.VMEM((2, 4, LANES), f32), pltpu.VMEM((7, 4, LANES), f32),
        pltpu.VMEM((1, LANES), f32), pltpu.VMEM((7, 1, LANES), f32),
    ]
    scratch += [dma((n,))] * 18 + [dma((3, n))] * 2 + [dma((n,))] * 2 + [dma((7,))] * 4 + [dma((6,))]
    kept = [pltpu.VMEM((COLS, ROWS), f32)] * 4 + [pltpu.VMEM(rows_shape, f32)] * 2 + [pltpu.VMEM((1, COLS), f32)] * 2
    kept.append(pltpu.VMEM((2, COLS, LANES), f32))
    state = pl.pallas_call(
        exchange_kernel,
        out_shape=tuple(kept),
        in_specs=[hbm] * 8,
        out_specs=(vmem,) * 9,
        scratch_shapes=scratch,
        compiler_params=pltpu.CompilerParams(collective_id=0, has_side_effects=True, vmem_limit_bytes=60_000_000),
        name="exchange",
    )(emb_g.reshape(ROWS, EMBED), head_g.reshape(2, 2, 2, COLS, ROWS), emb_p, head_p,
      emb_r.reshape(rows_shape), head_r.reshape(rows_shape), emb_c.reshape(1, COLS), head_c.reshape(1, COLS))

    outs = pl.pallas_call(
        update_kernel,
        out_shape=(table, table, jax.ShapeDtypeStruct(rows_shape, f32), jax.ShapeDtypeStruct(rows_shape, f32),
                   jax.ShapeDtypeStruct((1, COLS), f32), jax.ShapeDtypeStruct((1, COLS), f32), half, half),
        in_specs=[vmem] * 9,
        out_specs=(hbm,) * 8,
        scratch_shapes=[pltpu.VMEM((2, COLS, ROWS), f32), pltpu.VMEM((2, COLS, ROWS), jnp.bfloat16),
                        dma((4,)), dma((2, PARTS)), dma((2, PARTS))],
        compiler_params=pltpu.CompilerParams(vmem_limit_bytes=16 * 2 ** 20),
        name="update",
    )(*state)
    emb_new, head_new, emb_rn, head_rn, emb_cn, head_cn, emb_half, head_half = outs
    return (emb_new.T, head_new, emb_rn.reshape(ROWS), emb_cn.reshape(COLS), head_rn.reshape(ROWS),
            head_cn.reshape(COLS), emb_half.T, head_half)


def solution(mesh):
    arg_specs = (P("model", "data"), P("data", "model"), P("data", "model", None), P("data", None, "model"),
                 P("model"), P("data"), P("model"), P("data"))
    result_specs = (P("model", "data"), P("data", "model"), P("model"), P("data"), P("model"), P("data"),
                    P("model", "data"), P("data", "model"))
    mapped = jax.shard_map(local_step, mesh=mesh, in_specs=arg_specs, out_specs=result_specs, check_vma=False)

    def update_tables(emb_param, head_param, emb_grad, head_grad, emb_row, emb_col, head_row, head_col):
        return mapped(emb_param, head_param, emb_grad, head_grad, emb_row, emb_col, head_row, head_col)

    return update_tables
```

```python
import functools

import jax
import jax.numpy as jnp
from jax import lax
from jax.experimental import pallas as pl
from jax.experimental.pallas import tpu as pltpu
from jax.sharding import PartitionSpec as P

TRAIN_STEP = 10
DECAY_EXP = 0.8
EPS_ONE = 1e-30
CLIP_LIMIT = 1.0
SCALE_FLOOR = 1e-3
LEARN_RATE = float(TRAIN_STEP) ** -0.5
BETA_TWO = 1.0 - float(TRAIN_STEP) ** -DECAY_EXP

VOCAB = 16384
EMBED = 768
ROWS = VOCAB // 4
COLS = EMBED // 8
LANES = 128
CHUNKS = ROWS // 2 // LANES
GROUPS = ((0, 1), (1, 1), (2, 2), (4, 4), (8, 8))
PAIRS = CHUNKS // 2
BLOCKS = 2 * PAIRS
RING = 4
PARTS = 4
MESH = pl.DeviceIdType.MESH
PLANE = ((0, 1), (1, 0), (1, 1))


def exchange_kernel(emb_ref, head_ref, emb_p_ref, head_p_ref, emb_r_ref, head_r_ref, emb_c_ref, head_c_ref,
                    stage_e, stage_h, par_e, par_h, emb_rows_out, head_rows_out, emb_cols_out, head_cols_out, scale_out,
                    own_e, in0_e, sum_e, sum_h, in0_h, in1_e, in1_h, in2_e, in2_h, peer,
                    rows, old_rows, old_cols, rp_own, rp_in, col_acc, t_acc, rsum, psum, m_own, m_in, s_own, s_in,
                    ld_e, ld_h, s0e_r, s0h_r, s1e_r, s1h_r, s2e_r, s2h_r, swap_r, rp_r, fw_r, send, last_r, in_sem):
    model = lax.axis_index("model")
    data = lax.axis_index("data")
    c = data % 2
    x = (data // 2) % 2
    y = data // 4
    oc, ox, oy = 1 - c, 1 - x, 1 - y

    def plane_id(fy, fx, fc):
        step = fy * (4 - 8 * y) + fx * (2 - 4 * x) + fc * (1 - 2 * c)
        return (model, data + step)

    def column_id(dz, fc):
        return ((model + dz) % 4, data + fc * (1 - 2 * c))

    core_peer, x_peer, y_peer = plane_id(0, 0, 1), plane_id(0, 1, 0), plane_id(1, 0, 0)

    def remote(src, dst, send_sem, recv_sem, peer_id):
        return pltpu.make_async_remote_copy(src_ref=src, dst_ref=dst, send_sem=send_sem, recv_sem=recv_sem,
                                            device_id=peer_id, device_id_type=MESH)

    def arrived(ref, sem):
        pltpu.make_async_copy(ref, ref, sem).wait()

    def vocab_at(core, first, count):
        return pl.ds(pl.multiple_of(core * (ROWS // 2) + first * LANES, LANES), count * LANES)

    half_of = 4 * COLS

    def first_e(q):
        cols = pl.ds(pl.multiple_of((oy if q == 0 else y) * half_of, LANES), half_of)
        return (pltpu.make_async_copy(emb_ref.at[vocab_at(c, 0, 1), cols], own_e.at[0:LANES, cols], ld_e.at[q]),
                remote(emb_ref.at[vocab_at(oc, 0, 1), cols], in0_e.at[0:LANES, cols], send.at[0], s0e_r.at[q], core_peer))

    def first_h(q):
        part = ox if q == 0 else x
        return (pltpu.make_async_copy(head_ref.at[:, part, :, :, vocab_at(c, 0, 1)], sum_h.at[0, :, part], ld_h.at[q]),
                remote(head_ref.at[:, part, :, :, vocab_at(oc, 0, 1)], in0_h.at[0, :, part], send.at[1], s0h_r.at[q], core_peer))

    def group_e(i):
        first, count = GROUPS[i]
        at = slice(first * LANES, (first + count) * LANES)
        return (pltpu.make_async_copy(emb_ref.at[vocab_at(c, first, count), :], own_e.at[at, :], ld_e.at[i + 1]),
                remote(emb_ref.at[vocab_at(oc, first, count), :], in0_e.at[at, :], send.at[0], s0e_r.at[i + 1], core_peer))

    def group_h(i):
        first, count = GROUPS[i]
        pairs = []
        for j in range(first, first + count):
            pairs.append((pltpu.make_async_copy(head_ref.at[:, :, :, :, vocab_at(c, j, 1)], sum_h.at[j], ld_h.at[i + 1]),
                          remote(head_ref.at[:, :, :, :, vocab_at(oc, j, 1)], in0_h.at[j], send.at[1], s0h_r.at[i + 1],
                                 core_peer)))
        return pairs

    def one_e(k):
        return remote(sum_e.at[k, oy], in1_e.at[k], send.at[2], s1e_r.at[k % RING], y_peer)

    def one_h(k):
        return remote(sum_h.at[k, :, ox], in1_h.at[k], send.at[3], s1h_r.at[k % RING], x_peer)

    def two_e(k):
        return remote(in1_e.at[k, ox], in2_e.at[k], send.at[4], s2e_r.at[k % RING], x_peer)

    def two_h(k):
        return remote(in1_h.at[k, oy], in2_h.at[k], send.at[5], s2h_r.at[k % RING], y_peer)

    def swap(q):
        return [remote(total.at[pl.ds(2 * q, 2), oc], peer.at[q, t], send.at[6], swap_r.at[q], core_peer)
                for t, total in enumerate((in2_e, in2_h))]

    def row_msg(q, i):
        fy, fx = PLANE[i]
        return remote(rp_own.at[q], rp_in.at[q, i], send.at[7], rp_r.at[q], plane_id(fy, fx, 0))

    def row_fwd(q):
        return remote(rows.at[c * PAIRS + q], rows.at[c * PAIRS + q], send.at[8], fw_r.at[q], core_peer)

    small_loads = [pltpu.make_async_copy(src, dst, in_sem.at[i]) for i, (src, dst) in (
        (0, (emb_p_ref, par_e)), (1, (head_p_ref, par_h)), (2, (emb_r_ref, old_rows.at[0])), (2, (head_r_ref, old_rows.at[1])),
        (3, (emb_c_ref, old_cols.at[0])), (3, (head_c_ref, old_cols.at[1])))]

    barrier = pltpu.get_barrier_semaphore()
    greeted = 0
    for fy in range(2):
        for fx in range(2):
            for fc in range(2):
                if fy + fx + fc:
                    pl.semaphore_signal(barrier, inc=1, device_id=plane_id(fy, fx, fc), device_id_type=MESH)
                    greeted += 1
    for dz in range(1, 4):
        for fc in range(2):
            pl.semaphore_signal(barrier, inc=1, device_id=column_id(dz, fc), device_id_type=MESH)
            greeted += 1
    for q in range(2):
        first_e(q)[0].start()
        first_h(q)[0].start()
    for i in range(1, len(GROUPS)):
        group_e(i)[0].start()
        for cp, _ in group_h(i):
            cp.start()
    pl.semaphore_wait(barrier, greeted)

    for q in range(2):
        first_e(q)[1].start()
        first_h(q)[1].start()
    for i in range(1, len(GROUPS)):
        group_e(i)[1].start()
        for _, cp in group_h(i):
            cp.start()
    for cp in small_loads:
        cp.start()

    col_acc[...] = jnp.zeros_like(col_acc)
    t_acc[...] = jnp.zeros_like(t_acc)
    rsum[...] = jnp.zeros_like(rsum)
    psum[...] = jnp.zeros_like(psum)

    def flip_e(k, half):
        at = pl.ds(pl.multiple_of(k * LANES, LANES), LANES)
        for j in range(half_of // LANES):
            cols = pl.ds(pl.multiple_of(half * half_of + j * LANES, LANES), LANES)
            strip = (own_e[at, cols] + in0_e[at, cols]).T
            done = 0
            while done < LANES:
                block, row = divmod(LANES * j + done, COLS)
                size = min(LANES - done, COLS - row)
                sum_e[k, half, block // 2, block % 2, row:row + size, :] = strip[done:done + size, :]
                done += size

    def add_h(k, part):
        for a in range(2):
            for b in range(2):
                sum_h[k, a, part, b] = sum_h[k, a, part, b] + in0_h[k, a, part, b]

    def combine_cores(k):
        flip_e(k, oy)
        one_e(k).start()
        add_h(k, ox)
        one_h(k).start()
        flip_e(k, y)
        add_h(k, x)

    def first_sum(k):
        one_e(k).wait_recv()
        in1_e[k, ox] = in1_e[k, ox] + sum_e[k, y, ox]
        two_e(k).start()
        in1_e[k, x] = in1_e[k, x] + sum_e[k, y, x]
        one_h(k).wait_recv()
        in1_h[k, oy] = in1_h[k, oy] + sum_h[k, oy, x]
        two_h(k).start()
        in1_h[k, y] = in1_h[k, y] + sum_h[k, y, x]

    def finish(k, q, i):
        two_e(k).wait_recv()
        for core in range(2):
            in2_e[k, core] = in2_e[k, core] + in1_e[k, x, core]
        two_h(k).wait_recv()
        for core in range(2):
            in2_h[k, core] = in2_h[k, core] + in1_h[k, y, core]
        for t, total in enumerate((in2_e, in2_h)):
            row_part = jnp.zeros((1, LANES), jnp.float32)
            for core in range(2):
                g = total[k, core]
                sq = g * g + EPS_ONE
                col_acc[t, core] = col_acc[t, core] + sq
                row_part = row_part + jnp.sum(sq, axis=0, keepdims=True)
            rp_own[q, 2 * t + i:2 * t + i + 1, :] = row_part

    def publish(q):
        for i in range(3):
            row_msg(q, i).start()
        for cp in swap(q):
            cp.start()

    def row_stats(q):
        arrived(rp_in.at[q], rp_r.at[q])
        block = c * PAIRS + q
        row_sq = (rp_own[q] + rp_in[q, 0]) + (rp_in[q, 1] + rp_in[q, 2])
        old = jnp.concatenate([old_rows[0, block], old_rows[1, block]], axis=0)
        row_new = BETA_TWO * old + (1.0 - BETA_TWO) * (row_sq / EMBED)
        rows[block] = row_new
        rsum[...] = rsum[...] + row_new
        inv = 1.0 / row_new
        for t, total in enumerate((in2_e, in2_h)):
            for core in range(2):
                acc = t_acc[t, core]
                for i in range(2):
                    g = total[2 * q + i, core]
                    acc = acc + (g * g) * inv[2 * t + i:2 * t + i + 1, :]
                t_acc[t, core] = acc

    def scale_rows(block, get):
        factor = lax.rsqrt(rows[block])
        base = pl.multiple_of(block * (2 * LANES), 2 * LANES)
        for t, stage in enumerate((stage_e, stage_h)):
            for i in range(2):
                stage[:, pl.ds(base + i * LANES, LANES)] = get(t, i) * factor[2 * t + i:2 * t + i + 1, :]

    def scale_own(q):
        totals = (in2_e, in2_h)
        scale_rows(c * PAIRS + q, lambda t, i: totals[t][2 * q + i, c])

    def scale_peer(q):
        arrived(rows.at[oc * PAIRS + q], fw_r.at[q])
        arrived(peer.at[q], swap_r.at[q])
        scale_rows(oc * PAIRS + q, lambda t, i: peer[q, t, i])

    def param_sq(k):
        size = ROWS // CHUNKS
        at = pl.ds(pl.multiple_of(k * size, size), size)
        for t, par in enumerate((par_e, par_h)):
            v = par[:, at]
            v = jnp.sum(v * v, axis=0, keepdims=True)
            for i in range(size // LANES):
                psum[t:t + 1, :] = psum[t:t + 1, :] + v[:, i * LANES:(i + 1) * LANES]

    for q in range(2):
        load, cross = first_e(q)
        load.wait()
        cross.wait_recv()
        flip_e(0, oy if q == 0 else y)
        if q == 0:
            one_e(0).start()
        load, cross = first_h(q)
        load.wait()
        cross.wait_recv()
        add_h(0, ox if q == 0 else x)
        if q == 0:
            one_h(0).start()
    arrived(par_e, in_sem.at[0])
    arrived(par_h, in_sem.at[1])
    arrived(old_rows, in_sem.at[2])
    arrived(old_cols, in_sem.at[3])

    @pl.loop(0, CHUNKS)
    def _(k):
        for i in range(1, len(GROUPS)):
            first, count = GROUPS[i]

            @pl.when(k + 1 == first)
            def _():
                at = slice(first * LANES, (first + count) * LANES)
                arrived(own_e.at[at, :], ld_e.at[i + 1])
                arrived(in0_e.at[at, :], s0e_r.at[i + 1])
                arrived(sum_h.at[first:first + count], ld_h.at[i + 1])
                arrived(in0_h.at[first:first + count], s0h_r.at[i + 1])

        @pl.when(k + 1 < CHUNKS)
        def _():
            combine_cores(k + 1)

        param_sq(k)
        first_sum(k)
        pair = k // 2

        @pl.when((k >= 1) & (k % 2 == 1))
        def _():
            finish(k - 1, pair, 0)

        @pl.when((k >= 2) & (k % 2 == 0))
        def _():
            finish(k - 1, pair - 1, 1)
            publish(pair - 1)

        @pl.when((k >= 4) & (k % 2 == 0))
        def _():
            row_stats(pair - 2)
            row_fwd(pair - 2).start()
            scale_own(pair - 2)

        @pl.when((k >= 6) & (k % 2 == 0))
        def _():
            scale_peer(pair - 3)

    finish(CHUNKS - 1, PAIRS - 1, 1)
    publish(PAIRS - 1)
    row_stats(PAIRS - 2)
    row_fwd(PAIRS - 2).start()
    row_stats(PAIRS - 1)
    row_fwd(PAIRS - 1).start()

    lane = lax.broadcasted_iota(jnp.int32, (1, LANES), 1)
    diag = lax.broadcasted_iota(jnp.int32, (COLS, LANES), 0) == lax.broadcasted_iota(jnp.int32, (COLS, LANES), 1)

    def as_row(acc):
        col = jnp.sum(acc, axis=1, keepdims=True)
        return jnp.sum(jnp.where(diag, col, 0.0), axis=0, keepdims=True)

    def total_of(v):
        return jnp.sum(jnp.sum(v, axis=1, keepdims=True), axis=0, keepdims=True)

    for t in range(2):
        r_part = total_of(rsum[2 * t:2 * t + 2, :])
        p_part = jnp.sum(psum[t:t + 1, :], axis=1, keepdims=True)
        for core in range(2):
            row = as_row(col_acc[t, core])
            row = jnp.where(lane == COLS, r_part, jnp.where(lane == COLS + 1, p_part, row))
            m_own[core, 2 * t:2 * t + 1, :] = row
            m_own[core, 2 * t + 1:2 * t + 2, :] = as_row(t_acc[t, core])

    columns = [(dz, fc) for dz in range(4) for fc in range(2) if dz + fc]

    def column_msg(i):
        dz, fc = columns[i]
        slot = columns.index(((4 - dz) % 4, fc))
        return remote(m_own.at[oc if fc else c], m_in.at[slot], send.at[9], last_r.at[0], column_id(dz, fc))

    for i in range(len(columns)):
        column_msg(i).start()

    scale_own(PAIRS - 2)
    scale_own(PAIRS - 1)
    arrived(m_in, last_r.at[0])

    total = m_own[c]
    for i in range(len(columns)):
        total = total + m_in[i]
    factors, message = [], jnp.zeros((1, LANES), jnp.float32)
    for t, c_out in enumerate((emb_cols_out, head_cols_out)):
        cols = total[2 * t:2 * t + 1, :]
        r_mean = jnp.sum(jnp.where(lane == COLS, cols, 0.0), axis=1, keepdims=True) / VOCAB
        p_col = jnp.sum(jnp.where(lane == COLS + 1, cols, 0.0), axis=1, keepdims=True)
        col_new = BETA_TWO * old_cols[t] + (1.0 - BETA_TWO) * (cols[:, :COLS] / VOCAB)
        u_sq = jnp.sum(total[2 * t + 1:2 * t + 2, :COLS] * (r_mean / col_new), axis=1, keepdims=True)
        message = jnp.where(lane == 2 * t, u_sq, jnp.where(lane == 2 * t + 1, 0.5 * p_col, message))
        c_out[...] = col_new
        factors.append(lax.rsqrt(col_new) * jnp.sqrt(r_mean))
    s_own[...] = message

    flips = [(fy, fx, fc) for fy in range(2) for fx in range(2) for fc in range(2) if fy + fx + fc]

    def scalar_msg(i):
        return remote(s_own, s_in.at[i], send.at[10], last_r.at[1], plane_id(*flips[i]))

    for i in range(len(flips)):
        scalar_msg(i).start()
    square = diag[:, :COLS]
    factor_cols = [jnp.sum(jnp.where(square, factor, 0.0), axis=1, keepdims=True) for factor in factors]

    @pl.loop(PAIRS - 3, PAIRS)
    def _(q):
        scale_peer(q)

    emb_rows_out[...] = rows[:, :2, :]
    head_rows_out[...] = rows[:, 2:, :]
    arrived(in0_e, send.at[0])
    arrived(in0_h, send.at[1])
    arrived(in1_e, send.at[2])
    arrived(in1_h, send.at[3])
    arrived(in2_e, send.at[4])
    arrived(in2_h, send.at[5])
    arrived(peer, send.at[6])
    arrived(rp_in, send.at[7])
    arrived(rows.at[0:PAIRS], send.at[8])
    arrived(m_in, send.at[9])
    arrived(s_in, last_r.at[1])
    message = s_own[...]
    for i in range(len(flips)):
        message = message + s_in[i]
    count = float(VOCAB * EMBED)
    for t in range(2):
        u_sq = jnp.sum(jnp.where(lane == 2 * t, message, 0.0), axis=1, keepdims=True)
        p_sq = jnp.sum(jnp.where(lane == 2 * t + 1, message, 0.0), axis=1, keepdims=True)
        u_rms = jnp.sqrt(u_sq / count)
        p_rms = jnp.sqrt(p_sq / count)
        step = LEARN_RATE * jnp.maximum(SCALE_FLOOR, p_rms) / jnp.maximum(1.0, u_rms / CLIP_LIMIT)
        scale_out[t] = jnp.broadcast_to(factor_cols[t] * step, (COLS, LANES))
    arrived(s_in, send.at[10])


def update_kernel(emb_g, head_g, emb_p, head_p, emb_rows, head_rows, emb_cols, head_cols, scale,
                  emb_new, head_new, emb_rows_new, head_rows_new, emb_cols_new, head_cols_new, emb_half, head_half,
                  new_buf, half_buf, small_sem, big_sem):
    small = [pltpu.make_async_copy(src, dst, small_sem.at[i]) for i, (src, dst) in enumerate(
        ((emb_rows, emb_rows_new), (head_rows, head_rows_new), (emb_cols, emb_cols_new), (head_cols, head_cols_new)))]
    for cp in small:
        cp.start()
    size = ROWS // PARTS
    for i in range(PARTS):
        part = slice(i * size, (i + 1) * size)
        for t, (p, g, new, half) in enumerate(((emb_p, emb_g, emb_new, emb_half), (head_p, head_g, head_new, head_half))):
            value = p[:, part] - g[:, part] * scale[t, :, 0:1]
            new_buf[t, :, part] = value
            half_buf[t, :, part] = value.astype(jnp.bfloat16)
            pltpu.make_async_copy(new_buf.at[t, :, part], new.at[:, part], big_sem.at[0]).start()
            pltpu.make_async_copy(half_buf.at[t, :, part], half.at[:, part], big_sem.at[1]).start()
    for cp in small:
        cp.wait()
    pltpu.make_async_copy(new_buf, new_buf, big_sem.at[0]).wait()
    pltpu.make_async_copy(half_buf, half_buf, big_sem.at[1]).wait()


def local_step(emb_p, head_p, emb_g, head_g, emb_r, emb_c, head_r, head_c):
    f32 = jnp.float32
    n = CHUNKS
    dma = pltpu.SemaphoreType.DMA
    hbm = pl.BlockSpec(memory_space=pltpu.HBM)
    vmem = pl.BlockSpec(memory_space=pltpu.VMEM)
    rows_shape = (BLOCKS, 2, LANES)
    table = jax.ShapeDtypeStruct((COLS, ROWS), f32)
    half = jax.ShapeDtypeStruct((COLS, ROWS), jnp.bfloat16)
    emb_p = emb_p.T
    shapes = [(ROWS // 2, EMBED)] * 2 + [(n, 2, 2, 2, COLS, LANES)] * 3
    shapes += [(n, 2, 2, COLS, LANES)] * 2 + [(n, 2, COLS, LANES)] * 2 + [(PAIRS, 2, 2, COLS, LANES)]
    shapes += [(BLOCKS, 4, LANES), (2, *rows_shape), (2, 1, COLS)]
    shapes += [(PAIRS, 4, LANES), (PAIRS, 3, 4, LANES)]
    shapes += [(2, 2, COLS, LANES)] * 2 + [(4, LANES), (2, LANES)]
    shapes += [(2, 4, LANES), (7, 4, LANES), (1, LANES), (7, 1, LANES)]
    scratch = [pltpu.VMEM(shape, f32) for shape in shapes]
    scratch += [dma((len(GROUPS) + 1,))] * 4 + [dma((RING,))] * 4 + [dma((PAIRS,))] * 3
    scratch += [dma((11,)), dma((2,)), dma((4,))]
    kept = [pltpu.VMEM((COLS, ROWS), f32)] * 4 + [pltpu.VMEM(rows_shape, f32)] * 2 + [pltpu.VMEM((1, COLS), f32)] * 2
    kept.append(pltpu.VMEM((2, COLS, LANES), f32))
    state = pl.pallas_call(
        exchange_kernel,
        out_shape=tuple(kept),
        in_specs=[hbm] * 8,
        out_specs=(vmem,) * 9,
        scratch_shapes=scratch,
        compiler_params=pltpu.CompilerParams(collective_id=0, has_side_effects=True, vmem_limit_bytes=60_000_000),
        name="exchange",
    )(emb_g.reshape(ROWS, EMBED), head_g.reshape(2, 2, 2, COLS, ROWS), emb_p, head_p,
      emb_r.reshape(rows_shape), head_r.reshape(rows_shape), emb_c.reshape(1, COLS), head_c.reshape(1, COLS))

    outs = pl.pallas_call(
        update_kernel,
        out_shape=(table, table, jax.ShapeDtypeStruct(rows_shape, f32), jax.ShapeDtypeStruct(rows_shape, f32),
                   jax.ShapeDtypeStruct((1, COLS), f32), jax.ShapeDtypeStruct((1, COLS), f32), half, half),
        in_specs=[vmem] * 9,
        out_specs=(hbm,) * 8,
        scratch_shapes=[pltpu.VMEM((2, COLS, ROWS), f32), pltpu.VMEM((2, COLS, ROWS), jnp.bfloat16),
                        dma((4,)), dma((2,))],
        compiler_params=pltpu.CompilerParams(vmem_limit_bytes=16 * 2 ** 20),
        name="update",
    )(*state)
    emb_new, head_new, emb_rn, head_rn, emb_cn, head_cn, emb_half, head_half = outs
    return (emb_new.T, head_new, emb_rn.reshape(ROWS), emb_cn.reshape(COLS), head_rn.reshape(ROWS),
            head_cn.reshape(COLS), emb_half.T, head_half)


def solution(mesh):
    arg_specs = (P("model", "data"), P("data", "model"), P("data", "model", None), P("data", None, "model"),
                 P("model"), P("data"), P("model"), P("data"))
    result_specs = (P("model", "data"), P("data", "model"), P("model"), P("data"), P("model"), P("data"),
                    P("model", "data"), P("data", "model"))
    mapped = jax.shard_map(local_step, mesh=mesh, in_specs=arg_specs, out_specs=result_specs, check_vma=False)

    def update_tables(emb_param, head_param, emb_grad, head_grad, emb_row, emb_col, head_row, head_col):
        return mapped(emb_param, head_param, emb_grad, head_grad, emb_row, emb_col, head_row, head_col)

    return update_tables
```

```python
import functools

import jax
import jax.numpy as jnp
from jax import lax
from jax.experimental import pallas as pl
from jax.experimental.pallas import tpu as pltpu
from jax.sharding import PartitionSpec as P

TRAIN_STEP = 10
DECAY_EXP = 0.8
EPS_ONE = 1e-30
CLIP_LIMIT = 1.0
SCALE_FLOOR = 1e-3
LEARN_RATE = float(TRAIN_STEP) ** -0.5
BETA_TWO = 1.0 - float(TRAIN_STEP) ** -DECAY_EXP

VOCAB = 16384
EMBED = 768
ROWS = VOCAB // 4
COLS = EMBED // 8
LANES = 128
CHUNKS = ROWS // 2 // LANES
GROUPS = ((0, 1), (1, 1), (2, 2), (4, 12))
PAIRS = CHUNKS // 2
BLOCKS = 2 * PAIRS
RING = 4
PARTS = 3
MESH = pl.DeviceIdType.MESH
PLANE = ((0, 1), (1, 0), (1, 1))


def exchange_kernel(emb_ref, head_ref, emb_p_ref, head_p_ref, emb_r_ref, head_r_ref, emb_c_ref, head_c_ref,
                    stage_e, stage_h, par_e, par_h, emb_rows_out, head_rows_out, emb_cols_out, head_cols_out, scale_out,
                    both_e, sum_e, both_h, in1_e, in1_h, in2_e, in2_h, peer,
                    rows, old_rows, old_cols, rp_own, rp_in, col_acc, t_acc, rsum, psum, m_own, m_in, s_own, s_in,
                    s0e_r, s0h_r, s1e_r, s1h_r, s2e_r, s2h_r, swap_r, rp_r, fw_r, send, last_r, in_sem, token):
    model = lax.axis_index("model")
    data = lax.axis_index("data")
    c = data % 2
    x = (data // 2) % 2
    y = data // 4
    oc, ox, oy = 1 - c, 1 - x, 1 - y

    def plane_id(fy, fx, fc):
        step = fy * (4 - 8 * y) + fx * (2 - 4 * x) + fc * (1 - 2 * c)
        return (model, data + step)

    def column_id(dz, fc):
        return ((model + dz) % 4, data + fc * (1 - 2 * c))

    core_peer, x_peer, y_peer = plane_id(0, 0, 1), plane_id(0, 1, 0), plane_id(1, 0, 0)

    def remote(src, dst, send_sem, recv_sem, peer_id):
        return pltpu.make_async_remote_copy(src_ref=src, dst_ref=dst, send_sem=send_sem, recv_sem=recv_sem,
                                            device_id=peer_id, device_id_type=MESH)

    def arrived(ref, sem):
        pltpu.make_async_copy(ref, ref, sem).wait()

    def vocab_at(core, first, count):
        return pl.ds(pl.multiple_of(core * (ROWS // 2) + first * LANES, LANES), count * LANES)

    half_of = 4 * COLS

    def first_e(q):
        cols = pl.ds(pl.multiple_of((oy if q == 0 else y) * half_of, LANES), half_of)
        return (pltpu.make_async_copy(emb_ref.at[vocab_at(c, 0, 1), cols], both_e.at[0, 0:LANES, cols], s0e_r.at[q]),
                remote(emb_ref.at[vocab_at(oc, 0, 1), cols], both_e.at[1, 0:LANES, cols], send.at[0], s0e_r.at[q], core_peer))

    def first_h(q):
        part = ox if q == 0 else x
        return (pltpu.make_async_copy(head_ref.at[:, part, :, :, vocab_at(c, 0, 1)], both_h.at[0, 0, :, part], s0h_r.at[q]),
                remote(head_ref.at[:, part, :, :, vocab_at(oc, 0, 1)], both_h.at[1, 0, :, part], send.at[1], s0h_r.at[q], core_peer))

    def group_e(i):
        first, count = GROUPS[i]
        at = slice(first * LANES, (first + count) * LANES)
        return (pltpu.make_async_copy(emb_ref.at[vocab_at(c, first, count), :], both_e.at[0, at, :], s0e_r.at[i + 1]),
                remote(emb_ref.at[vocab_at(oc, first, count), :], both_e.at[1, at, :], send.at[0], s0e_r.at[i + 1], core_peer))

    def group_h(i):
        first, count = GROUPS[i]
        pairs = []
        for j in range(first, first + count):
            pairs.append((pltpu.make_async_copy(head_ref.at[:, :, :, :, vocab_at(c, j, 1)], both_h.at[0, j], s0h_r.at[i + 1]),
                          remote(head_ref.at[:, :, :, :, vocab_at(oc, j, 1)], both_h.at[1, j], send.at[1], s0h_r.at[i + 1],
                                 core_peer)))
        return pairs

    def one_e(k):
        return remote(sum_e.at[k, oy], in1_e.at[k], send.at[2], s1e_r.at[k % RING], y_peer)

    def one_h(k):
        return remote(both_h.at[0, k, :, ox], in1_h.at[k], send.at[3], s1h_r.at[k % RING], x_peer)

    def two_e(k):
        return remote(in1_e.at[k, ox], in2_e.at[k], send.at[4], s2e_r.at[k % RING], x_peer)

    def two_h(k):
        return remote(in1_h.at[k, oy], in2_h.at[k], send.at[5], s2h_r.at[k % RING], y_peer)

    def swap(q):
        return [remote(total.at[pl.ds(2 * q, 2), oc], peer.at[q, t], send.at[6], swap_r.at[q % RING], core_peer)
                for t, total in enumerate((in2_e, in2_h))]

    def row_msg(q, i):
        fy, fx = PLANE[i]
        return remote(rp_own.at[q], rp_in.at[q, i], send.at[7], rp_r.at[q % RING], plane_id(fy, fx, 0))

    def row_fwd(q):
        return remote(rows.at[c * PAIRS + q], rows.at[c * PAIRS + q], send.at[8], fw_r.at[q % RING], core_peer)

    small_loads = [pltpu.make_async_copy(src, dst, in_sem.at[i]) for i, (src, dst) in (
        (0, (emb_p_ref, par_e)), (1, (head_p_ref, par_h)), (2, (emb_r_ref, old_rows.at[0])), (2, (head_r_ref, old_rows.at[1])),
        (3, (emb_c_ref, old_cols.at[0])), (3, (head_c_ref, old_cols.at[1])))]

    barrier = pltpu.get_barrier_semaphore()
    above, below = column_id(1, 0), column_id(3, 0)
    for peer_id in (core_peer, x_peer, y_peer, above, below):
        pl.semaphore_signal(barrier, inc=1, device_id=peer_id, device_id_type=MESH)
    for q in range(2):
        first_e(q)[0].start()
        first_h(q)[0].start()
    for i in range(1, len(GROUPS)):
        group_e(i)[0].start()
        for cp, _ in group_h(i):
            cp.start()
    pl.semaphore_wait(barrier, 5)

    for q in range(2):
        first_e(q)[1].start()
        first_h(q)[1].start()
    for i in range(1, len(GROUPS)):
        group_e(i)[1].start()
        for _, cp in group_h(i):
            cp.start()
    for cp in small_loads:
        cp.start()
    for peer_id in (above, below):
        pl.semaphore_signal(token, inc=1, device_id=peer_id, device_id_type=MESH)

    col_acc[...] = jnp.zeros_like(col_acc)
    t_acc[...] = jnp.zeros_like(t_acc)
    rsum[...] = jnp.zeros_like(rsum)
    psum[...] = jnp.zeros_like(psum)

    def flip_e(k, half):
        at = pl.ds(pl.multiple_of(k * LANES, LANES), LANES)
        for j in range(half_of // LANES):
            cols = pl.ds(pl.multiple_of(half * half_of + j * LANES, LANES), LANES)
            strip = (both_e[0, at, cols] + both_e[1, at, cols]).T
            done = 0
            while done < LANES:
                block, row = divmod(LANES * j + done, COLS)
                size = min(LANES - done, COLS - row)
                sum_e[k, half, block // 2, block % 2, row:row + size, :] = strip[done:done + size, :]
                done += size

    def add_h(k, part):
        for a in range(2):
            for b in range(2):
                both_h[0, k, a, part, b] = both_h[0, k, a, part, b] + both_h[1, k, a, part, b]

    def combine_cores(k):
        flip_e(k, oy)
        one_e(k).start()
        add_h(k, ox)
        one_h(k).start()
        flip_e(k, y)
        add_h(k, x)

    def first_sum(k):
        one_e(k).wait_recv()
        in1_e[k, ox] = in1_e[k, ox] + sum_e[k, y, ox]
        two_e(k).start()
        in1_e[k, x] = in1_e[k, x] + sum_e[k, y, x]
        one_h(k).wait_recv()
        in1_h[k, oy] = in1_h[k, oy] + both_h[0, k, oy, x]
        two_h(k).start()
        in1_h[k, y] = in1_h[k, y] + both_h[0, k, y, x]

    def finish(k, q, i):
        two_e(k).wait_recv()
        for core in range(2):
            in2_e[k, core] = in2_e[k, core] + in1_e[k, x, core]
        two_h(k).wait_recv()
        for core in range(2):
            in2_h[k, core] = in2_h[k, core] + in1_h[k, y, core]
        for t, total in enumerate((in2_e, in2_h)):
            row_part = jnp.zeros((1, LANES), jnp.float32)
            for core in range(2):
                g = total[k, core]
                sq = g * g + EPS_ONE
                col_acc[t, core] = col_acc[t, core] + sq
                row_part = row_part + jnp.sum(sq, axis=0, keepdims=True)
            rp_own[q, 2 * t + i:2 * t + i + 1, :] = row_part

    def publish(q):
        for i in range(3):
            row_msg(q, i).start()
        for cp in swap(q):
            cp.start()

    def row_stats(q):
        arrived(rp_in.at[q], rp_r.at[q % RING])
        block = c * PAIRS + q
        row_sq = (rp_own[q] + rp_in[q, 0]) + (rp_in[q, 1] + rp_in[q, 2])
        old = jnp.concatenate([old_rows[0, block], old_rows[1, block]], axis=0)
        row_new = BETA_TWO * old + (1.0 - BETA_TWO) * (row_sq / EMBED)
        rows[block] = row_new
        rsum[...] = rsum[...] + row_new
        inv = 1.0 / row_new
        for t, total in enumerate((in2_e, in2_h)):
            for core in range(2):
                acc = t_acc[t, core]
                for i in range(2):
                    g = total[2 * q + i, core]
                    acc = acc + (g * g) * inv[2 * t + i:2 * t + i + 1, :]
                t_acc[t, core] = acc

    def scale_rows(block, get):
        factor = lax.rsqrt(rows[block])
        base = pl.multiple_of(block * (2 * LANES), 2 * LANES)
        for t, stage in enumerate((stage_e, stage_h)):
            for i in range(2):
                stage[:, pl.ds(base + i * LANES, LANES)] = get(t, i) * factor[2 * t + i:2 * t + i + 1, :]

    def scale_own(q):
        totals = (in2_e, in2_h)
        scale_rows(c * PAIRS + q, lambda t, i: totals[t][2 * q + i, c])

    def scale_peer(q):
        arrived(rows.at[oc * PAIRS + q], fw_r.at[q % RING])
        arrived(peer.at[q], swap_r.at[q % RING])
        scale_rows(oc * PAIRS + q, lambda t, i: peer[q, t, i])

    def param_sq(k):
        size = ROWS // CHUNKS
        at = pl.ds(pl.multiple_of(k * size, size), size)
        for t, par in enumerate((par_e, par_h)):
            v = par[:, at]
            v = jnp.sum(v * v, axis=0, keepdims=True)
            for i in range(size // LANES):
                psum[t:t + 1, :] = psum[t:t + 1, :] + v[:, i * LANES:(i + 1) * LANES]

    for q in range(2):
        cols = pl.ds(pl.multiple_of((oy if q == 0 else y) * half_of, LANES), half_of)
        arrived(both_e.at[:, 0:LANES, cols], s0e_r.at[q])
        flip_e(0, oy if q == 0 else y)
        if q == 0:
            one_e(0).start()
        part = ox if q == 0 else x
        arrived(both_h.at[:, 0, :, part], s0h_r.at[q])
        add_h(0, part)
        if q == 0:
            one_h(0).start()
    pl.semaphore_wait(token, 2)
    arrived(par_e, in_sem.at[0])
    arrived(par_h, in_sem.at[1])
    arrived(old_rows, in_sem.at[2])
    arrived(old_cols, in_sem.at[3])

    @pl.loop(0, CHUNKS)
    def _(k):
        for i in range(1, len(GROUPS)):
            first, count = GROUPS[i]

            @pl.when(k + 1 == first)
            def _():
                at = slice(first * LANES, (first + count) * LANES)
                arrived(both_e.at[:, at, :], s0e_r.at[i + 1])
                arrived(both_h.at[:, first:first + count], s0h_r.at[i + 1])

        @pl.when(k + 1 < CHUNKS)
        def _():
            combine_cores(k + 1)

        param_sq(k)
        first_sum(k)
        pair = k // 2

        @pl.when((k >= 1) & (k % 2 == 1))
        def _():
            finish(k - 1, pair, 0)

        @pl.when((k >= 2) & (k % 2 == 0))
        def _():
            finish(k - 1, pair - 1, 1)
            publish(pair - 1)

        @pl.when((k >= 6) & (k % 2 == 0))
        def _():
            scale_peer(pair - 3)

        @pl.when((k >= 4) & (k % 2 == 0))
        def _():
            row_stats(pair - 2)
            row_fwd(pair - 2).start()
            scale_own(pair - 2)

    finish(CHUNKS - 1, PAIRS - 1, 1)
    publish(PAIRS - 1)
    row_stats(PAIRS - 2)
    row_fwd(PAIRS - 2).start()
    row_stats(PAIRS - 1)
    row_fwd(PAIRS - 1).start()

    lane = lax.broadcasted_iota(jnp.int32, (1, LANES), 1)
    diag = lax.broadcasted_iota(jnp.int32, (COLS, LANES), 0) == lax.broadcasted_iota(jnp.int32, (COLS, LANES), 1)

    def as_row(acc):
        col = jnp.sum(acc, axis=1, keepdims=True)
        return jnp.sum(jnp.where(diag, col, 0.0), axis=0, keepdims=True)

    def total_of(v):
        return jnp.sum(jnp.sum(v, axis=1, keepdims=True), axis=0, keepdims=True)

    for t in range(2):
        r_part = total_of(rsum[2 * t:2 * t + 2, :])
        p_part = jnp.sum(psum[t:t + 1, :], axis=1, keepdims=True)
        for core in range(2):
            row = as_row(col_acc[t, core])
            row = jnp.where(lane == COLS, r_part, jnp.where(lane == COLS + 1, p_part, row))
            m_own[core, 2 * t:2 * t + 1, :] = row
            m_own[core, 2 * t + 1:2 * t + 2, :] = as_row(t_acc[t, core])

    columns = [(dz, fc) for dz in range(4) for fc in range(2) if dz + fc]

    def column_msg(i):
        dz, fc = columns[i]
        slot = columns.index(((4 - dz) % 4, fc))
        return remote(m_own.at[oc if fc else c], m_in.at[slot], send.at[9], last_r.at[0], column_id(dz, fc))

    for i in range(len(columns)):
        column_msg(i).start()

    scale_own(PAIRS - 2)
    scale_own(PAIRS - 1)
    arrived(m_in, last_r.at[0])

    total = m_own[c]
    for i in range(len(columns)):
        total = total + m_in[i]
    factors, message = [], jnp.zeros((1, LANES), jnp.float32)
    for t, c_out in enumerate((emb_cols_out, head_cols_out)):
        cols = total[2 * t:2 * t + 1, :]
        r_mean = jnp.sum(jnp.where(lane == COLS, cols, 0.0), axis=1, keepdims=True) / VOCAB
        p_col = jnp.sum(jnp.where(lane == COLS + 1, cols, 0.0), axis=1, keepdims=True)
        col_new = BETA_TWO * old_cols[t] + (1.0 - BETA_TWO) * (cols[:, :COLS] / VOCAB)
        u_sq = jnp.sum(total[2 * t + 1:2 * t + 2, :COLS] * (r_mean / col_new), axis=1, keepdims=True)
        message = jnp.where(lane == 2 * t, u_sq, jnp.where(lane == 2 * t + 1, 0.5 * p_col, message))
        c_out[...] = col_new
        factors.append(lax.rsqrt(col_new) * jnp.sqrt(r_mean))
    s_own[...] = message

    flips = [(fy, fx, fc) for fy in range(2) for fx in range(2) for fc in range(2) if fy + fx + fc]

    def scalar_msg(i):
        return remote(s_own, s_in.at[i], send.at[10], last_r.at[1], plane_id(*flips[i]))

    for i in range(len(flips)):
        scalar_msg(i).start()
    square = diag[:, :COLS]
    factor_cols = [jnp.sum(jnp.where(square, factor, 0.0), axis=1, keepdims=True) for factor in factors]

    @pl.loop(PAIRS - 3, PAIRS)
    def _(q):
        scale_peer(q)

    emb_rows_out[...] = rows[:, :2, :]
    head_rows_out[...] = rows[:, 2:, :]
    arrived(both_e.at[0], send.at[0])
    arrived(both_h.at[0], send.at[1])
    arrived(in1_e, send.at[2])
    arrived(in1_h, send.at[3])
    arrived(in2_e, send.at[4])
    arrived(in2_h, send.at[5])
    arrived(peer, send.at[6])
    arrived(rp_in, send.at[7])
    arrived(rows.at[0:PAIRS], send.at[8])
    arrived(m_in, send.at[9])
    arrived(s_in, last_r.at[1])
    message = s_own[...]
    for i in range(len(flips)):
        message = message + s_in[i]
    count = float(VOCAB * EMBED)
    for t in range(2):
        u_sq = jnp.sum(jnp.where(lane == 2 * t, message, 0.0), axis=1, keepdims=True)
        p_sq = jnp.sum(jnp.where(lane == 2 * t + 1, message, 0.0), axis=1, keepdims=True)
        u_rms = jnp.sqrt(u_sq / count)
        p_rms = jnp.sqrt(p_sq / count)
        step = LEARN_RATE * jnp.maximum(SCALE_FLOOR, p_rms) / jnp.maximum(1.0, u_rms / CLIP_LIMIT)
        scale_out[t] = jnp.broadcast_to(factor_cols[t] * step, (COLS, LANES))
    arrived(s_in, send.at[10])


def update_kernel(emb_g, head_g, emb_p, head_p, emb_rows, head_rows, emb_cols, head_cols, scale,
                  emb_new, head_new, emb_rows_new, head_rows_new, emb_cols_new, head_cols_new, emb_half, head_half,
                  new_buf, half_buf, small_sem, big_sem):
    small = [pltpu.make_async_copy(src, dst, small_sem.at[i]) for i, (src, dst) in enumerate(
        ((emb_rows, emb_rows_new), (head_rows, head_rows_new), (emb_cols, emb_cols_new), (head_cols, head_cols_new)))]
    for cp in small:
        cp.start()
    size = COLS // PARTS
    for i in range(PARTS):
        part = slice(i * size, (i + 1) * size)
        for t, (p, g, new, half) in enumerate(((emb_p, emb_g, emb_new, emb_half), (head_p, head_g, head_new, head_half))):
            value = p[part, :] - g[part, :] * scale[t, part, 0:1]
            new_buf[t, part, :] = value
            half_buf[t, part, :] = value.astype(jnp.bfloat16)
            pltpu.make_async_copy(new_buf.at[t, part, :], new.at[part, :], big_sem.at[0]).start()
            pltpu.make_async_copy(half_buf.at[t, part, :], half.at[part, :], big_sem.at[1]).start()
    for cp in small:
        cp.wait()
    pltpu.make_async_copy(new_buf, new_buf, big_sem.at[0]).wait()
    pltpu.make_async_copy(half_buf, half_buf, big_sem.at[1]).wait()


def local_step(emb_p, head_p, emb_g, head_g, emb_r, emb_c, head_r, head_c):
    f32 = jnp.float32
    n = CHUNKS
    dma = pltpu.SemaphoreType.DMA
    hbm = pl.BlockSpec(memory_space=pltpu.HBM)
    vmem = pl.BlockSpec(memory_space=pltpu.VMEM)
    rows_shape = (BLOCKS, 2, LANES)
    table = jax.ShapeDtypeStruct((COLS, ROWS), f32)
    half = jax.ShapeDtypeStruct((COLS, ROWS), jnp.bfloat16)
    emb_p = emb_p.T
    shapes = [(2, ROWS // 2, EMBED), (n, 2, 2, 2, COLS, LANES), (2, n, 2, 2, 2, COLS, LANES)]
    shapes += [(n, 2, 2, COLS, LANES)] * 2 + [(n, 2, COLS, LANES)] * 2 + [(PAIRS, 2, 2, COLS, LANES)]
    shapes += [(BLOCKS, 4, LANES), (2, *rows_shape), (2, 1, COLS)]
    shapes += [(PAIRS, 4, LANES), (PAIRS, 3, 4, LANES)]
    shapes += [(2, 2, COLS, LANES)] * 2 + [(4, LANES), (2, LANES)]
    shapes += [(2, 4, LANES), (7, 4, LANES), (1, LANES), (7, 1, LANES)]
    scratch = [pltpu.VMEM(shape, f32) for shape in shapes]
    scratch += [dma((len(GROUPS) + 1,))] * 2 + [dma((RING,))] * 7
    scratch += [dma((11,)), dma((2,)), dma((4,)), pltpu.SemaphoreType.REGULAR]
    kept = [pltpu.VMEM((COLS, ROWS), f32)] * 4 + [pltpu.VMEM(rows_shape, f32)] * 2 + [pltpu.VMEM((1, COLS), f32)] * 2
    kept.append(pltpu.VMEM((2, COLS, LANES), f32))
    state = pl.pallas_call(
        exchange_kernel,
        out_shape=tuple(kept),
        in_specs=[hbm] * 8,
        out_specs=(vmem,) * 9,
        scratch_shapes=scratch,
        compiler_params=pltpu.CompilerParams(collective_id=0, has_side_effects=True, vmem_limit_bytes=60_000_000),
        name="exchange",
    )(emb_g.reshape(ROWS, EMBED), head_g.reshape(2, 2, 2, COLS, ROWS), emb_p, head_p,
      emb_r.reshape(rows_shape), head_r.reshape(rows_shape), emb_c.reshape(1, COLS), head_c.reshape(1, COLS))

    outs = pl.pallas_call(
        update_kernel,
        out_shape=(table, table, jax.ShapeDtypeStruct(rows_shape, f32), jax.ShapeDtypeStruct(rows_shape, f32),
                   jax.ShapeDtypeStruct((1, COLS), f32), jax.ShapeDtypeStruct((1, COLS), f32), half, half),
        in_specs=[vmem] * 9,
        out_specs=(hbm,) * 8,
        scratch_shapes=[pltpu.VMEM((2, COLS, ROWS), f32), pltpu.VMEM((2, COLS, ROWS), jnp.bfloat16),
                        dma((4,)), dma((2,))],
        compiler_params=pltpu.CompilerParams(vmem_limit_bytes=16 * 2 ** 20),
        name="update",
    )(*state)
    emb_new, head_new, emb_rn, head_rn, emb_cn, head_cn, emb_half, head_half = outs
    return (emb_new.T, head_new, emb_rn.reshape(ROWS), emb_cn.reshape(COLS), head_rn.reshape(ROWS),
            head_cn.reshape(COLS), emb_half.T, head_half)


def solution(mesh):
    arg_specs = (P("model", "data"), P("data", "model"), P("data", "model", None), P("data", None, "model"),
                 P("model"), P("data"), P("model"), P("data"))
    result_specs = (P("model", "data"), P("data", "model"), P("model"), P("data"), P("model"), P("data"),
                    P("model", "data"), P("data", "model"))
    mapped = jax.shard_map(local_step, mesh=mesh, in_specs=arg_specs, out_specs=result_specs, check_vma=False)

    def update_tables(emb_param, head_param, emb_grad, head_grad, emb_row, emb_col, head_row, head_col):
        return mapped(emb_param, head_param, emb_grad, head_grad, emb_row, emb_col, head_row, head_col)

    return update_tables
```

```python
import functools

import jax
import jax.numpy as jnp
from jax import lax
from jax.experimental import pallas as pl
from jax.experimental.pallas import tpu as pltpu
from jax.sharding import PartitionSpec as P

TRAIN_STEP = 10
DECAY_EXP = 0.8
EPS_ONE = 1e-30
CLIP_LIMIT = 1.0
SCALE_FLOOR = 1e-3
LEARN_RATE = float(TRAIN_STEP) ** -0.5
BETA_TWO = 1.0 - float(TRAIN_STEP) ** -DECAY_EXP

VOCAB = 16384
EMBED = 768
ROWS = VOCAB // 4
COLS = EMBED // 8
LANES = 128
CHUNKS = ROWS // 2 // LANES
GROUPS = ((0, 1), (1, 1), (2, 2), (4, 12))
PAIRS = CHUNKS // 2
BLOCKS = 2 * PAIRS
RING = 4
PARTS = 3
MESH = pl.DeviceIdType.MESH
PLANE = ((0, 1), (1, 0), (1, 1))


def exchange_kernel(emb_ref, head_ref, emb_p_ref, head_p_ref, emb_r_ref, head_r_ref, emb_c_ref, head_c_ref,
                    stage_e, stage_h, par_e, par_h, emb_rows_out, head_rows_out, emb_cols_out, head_cols_out, scale_out,
                    both_e, sum_e, both_h, in1_e, in1_h, in2_e, in2_h, peer,
                    rows, old_rows, old_cols, rp_own, rp_in, col_acc, t_acc, rsum, psum, m_own, m_in, m_sum, s_own, s_in,
                    s0e_r, s0h_r, s1e_r, s1h_r, s2e_r, s2h_r, swap_r, rp_r, fw_r, send, last_r, in_sem, token):
    model = lax.axis_index("model")
    data = lax.axis_index("data")
    c = data % 2
    x = (data // 2) % 2
    y = data // 4
    oc, ox, oy = 1 - c, 1 - x, 1 - y

    def plane_id(fy, fx, fc):
        step = fy * (4 - 8 * y) + fx * (2 - 4 * x) + fc * (1 - 2 * c)
        return (model, data + step)

    def column_id(dz, fc):
        return ((model + dz) % 4, data + fc * (1 - 2 * c))

    core_peer, x_peer, y_peer = plane_id(0, 0, 1), plane_id(0, 1, 0), plane_id(1, 0, 0)

    def remote(src, dst, send_sem, recv_sem, peer_id):
        return pltpu.make_async_remote_copy(src_ref=src, dst_ref=dst, send_sem=send_sem, recv_sem=recv_sem,
                                            device_id=peer_id, device_id_type=MESH)

    def arrived(ref, sem):
        pltpu.make_async_copy(ref, ref, sem).wait()

    def vocab_at(core, first, count):
        return pl.ds(pl.multiple_of(core * (ROWS // 2) + first * LANES, LANES), count * LANES)

    half_of = 4 * COLS

    def first_e(q):
        cols = pl.ds(pl.multiple_of((oy if q == 0 else y) * half_of, LANES), half_of)
        return (pltpu.make_async_copy(emb_ref.at[vocab_at(c, 0, 1), cols], both_e.at[0, 0:LANES, cols], s0e_r.at[q]),
                remote(emb_ref.at[vocab_at(oc, 0, 1), cols], both_e.at[1, 0:LANES, cols], send.at[0], s0e_r.at[q], core_peer))

    def first_h(q):
        part = ox if q == 0 else x
        return (pltpu.make_async_copy(head_ref.at[:, part, :, :, vocab_at(c, 0, 1)], both_h.at[0, 0, :, part], s0h_r.at[q]),
                remote(head_ref.at[:, part, :, :, vocab_at(oc, 0, 1)], both_h.at[1, 0, :, part], send.at[1], s0h_r.at[q], core_peer))

    def group_e(i):
        first, count = GROUPS[i]
        at = slice(first * LANES, (first + count) * LANES)
        return (pltpu.make_async_copy(emb_ref.at[vocab_at(c, first, count), :], both_e.at[0, at, :], s0e_r.at[i + 1]),
                remote(emb_ref.at[vocab_at(oc, first, count), :], both_e.at[1, at, :], send.at[0], s0e_r.at[i + 1], core_peer))

    def group_h(i):
        first, count = GROUPS[i]
        pairs = []
        for j in range(first, first + count):
            pairs.append((pltpu.make_async_copy(head_ref.at[:, :, :, :, vocab_at(c, j, 1)], both_h.at[0, j], s0h_r.at[i + 1]),
                          remote(head_ref.at[:, :, :, :, vocab_at(oc, j, 1)], both_h.at[1, j], send.at[1], s0h_r.at[i + 1],
                                 core_peer)))
        return pairs

    def one_e(k):
        return remote(sum_e.at[k, oy], in1_e.at[k], send.at[2], s1e_r.at[k % RING], y_peer)

    def one_h(k):
        return remote(both_h.at[0, k, :, ox], in1_h.at[k], send.at[3], s1h_r.at[k % RING], x_peer)

    def two_e(k):
        return remote(in1_e.at[k, ox], in2_e.at[k], send.at[4], s2e_r.at[k % RING], x_peer)

    def two_h(k):
        return remote(in1_h.at[k, oy], in2_h.at[k], send.at[5], s2h_r.at[k % RING], y_peer)

    def swap(q):
        return [remote(total.at[pl.ds(2 * q, 2), oc], peer.at[q, t], send.at[6], swap_r.at[q % RING], core_peer)
                for t, total in enumerate((in2_e, in2_h))]

    def row_msg(q, i):
        fy, fx = PLANE[i]
        return remote(rp_own.at[q], rp_in.at[q, i], send.at[7], rp_r.at[q % RING], plane_id(fy, fx, 0))

    def row_fwd(q):
        return remote(rows.at[c * PAIRS + q], rows.at[c * PAIRS + q], send.at[8], fw_r.at[q % RING], core_peer)

    small_loads = [pltpu.make_async_copy(src, dst, in_sem.at[i]) for i, (src, dst) in (
        (0, (emb_p_ref, par_e)), (1, (head_p_ref, par_h)), (2, (emb_r_ref, old_rows.at[0])), (2, (head_r_ref, old_rows.at[1])),
        (3, (emb_c_ref, old_cols.at[0, c])), (3, (head_c_ref, old_cols.at[1, c])))]
    small_loads += [remote(src, old_cols.at[t, c], send.at[11], in_sem.at[4], core_peer)
                    for t, src in enumerate((emb_c_ref, head_c_ref))]

    barrier = pltpu.get_barrier_semaphore()
    above, below = column_id(1, 0), column_id(3, 0)
    for peer_id in (core_peer, x_peer, y_peer):
        pl.semaphore_signal(barrier, inc=1, device_id=peer_id, device_id_type=MESH)

    z_count = 1 + model * (3 - model) // 2

    def along_z(act):
        @pl.when(model < 3)
        def _():
            act(above)

        @pl.when(model > 0)
        def _():
            act(below)

    along_z(lambda peer_id: pl.semaphore_signal(barrier, inc=1, device_id=peer_id, device_id_type=MESH))
    for q in range(2):
        first_e(q)[0].start()
        first_h(q)[0].start()
    for i in range(1, len(GROUPS)):
        group_e(i)[0].start()
        for cp, _ in group_h(i):
            cp.start()
    pl.semaphore_wait(barrier, 3 + z_count)

    for q in range(2):
        first_e(q)[1].start()
        first_h(q)[1].start()
    for i in range(1, len(GROUPS)):
        group_e(i)[1].start()
        for _, cp in group_h(i):
            cp.start()
    for cp in small_loads:
        cp.start()
    along_z(lambda peer_id: pl.semaphore_signal(token.at[0], inc=1, device_id=peer_id, device_id_type=MESH))

    col_acc[...] = jnp.zeros_like(col_acc)
    t_acc[...] = jnp.zeros_like(t_acc)
    rsum[...] = jnp.zeros_like(rsum)
    psum[...] = jnp.zeros_like(psum)

    def flip_e(k, half):
        at = pl.ds(pl.multiple_of(k * LANES, LANES), LANES)
        for j in range(half_of // LANES):
            cols = pl.ds(pl.multiple_of(half * half_of + j * LANES, LANES), LANES)
            strip = (both_e[0, at, cols] + both_e[1, at, cols]).T
            done = 0
            while done < LANES:
                block, row = divmod(LANES * j + done, COLS)
                size = min(LANES - done, COLS - row)
                sum_e[k, half, block // 2, block % 2, row:row + size, :] = strip[done:done + size, :]
                done += size

    def add_h(k, part):
        for a in range(2):
            for b in range(2):
                both_h[0, k, a, part, b] = both_h[0, k, a, part, b] + both_h[1, k, a, part, b]

    def combine_cores(k):
        flip_e(k, oy)
        one_e(k).start()
        add_h(k, ox)
        one_h(k).start()
        flip_e(k, y)
        add_h(k, x)

    def first_sum(k):
        one_e(k).wait_recv()
        in1_e[k, ox] = in1_e[k, ox] + sum_e[k, y, ox]
        two_e(k).start()
        in1_e[k, x] = in1_e[k, x] + sum_e[k, y, x]
        one_h(k).wait_recv()
        in1_h[k, oy] = in1_h[k, oy] + both_h[0, k, oy, x]
        two_h(k).start()
        in1_h[k, y] = in1_h[k, y] + both_h[0, k, y, x]

    def finish(k, q, i):
        two_e(k).wait_recv()
        for core in range(2):
            in2_e[k, core] = in2_e[k, core] + in1_e[k, x, core]
        two_h(k).wait_recv()
        for core in range(2):
            in2_h[k, core] = in2_h[k, core] + in1_h[k, y, core]
        for t, total in enumerate((in2_e, in2_h)):
            row_part = jnp.zeros((1, LANES), jnp.float32)
            for core in range(2):
                g = total[k, core]
                sq = g * g + EPS_ONE
                col_acc[t, core] = col_acc[t, core] + sq
                row_part = row_part + jnp.sum(sq, axis=0, keepdims=True)
            rp_own[q, 2 * t + i:2 * t + i + 1, :] = row_part

    def publish(q):
        for i in range(3):
            row_msg(q, i).start()
        for cp in swap(q):
            cp.start()

    def row_stats(q):
        arrived(rp_in.at[q], rp_r.at[q % RING])
        block = c * PAIRS + q
        row_sq = (rp_own[q] + rp_in[q, 0]) + (rp_in[q, 1] + rp_in[q, 2])
        old = jnp.concatenate([old_rows[0, block], old_rows[1, block]], axis=0)
        row_new = BETA_TWO * old + (1.0 - BETA_TWO) * (row_sq / EMBED)
        rows[block] = row_new
        rsum[...] = rsum[...] + row_new
        inv = 1.0 / row_new
        for t, total in enumerate((in2_e, in2_h)):
            for core in range(2):
                acc = t_acc[t, core]
                for i in range(2):
                    g = total[2 * q + i, core]
                    acc = acc + (g * g) * inv[2 * t + i:2 * t + i + 1, :]
                t_acc[t, core] = acc

    def scale_rows(block, get):
        factor = lax.rsqrt(rows[block])
        base = pl.multiple_of(block * (2 * LANES), 2 * LANES)
        for t, stage in enumerate((stage_e, stage_h)):
            for i in range(2):
                stage[:, pl.ds(base + i * LANES, LANES)] = get(t, i) * factor[2 * t + i:2 * t + i + 1, :]

    def scale_own(q):
        totals = (in2_e, in2_h)
        scale_rows(c * PAIRS + q, lambda t, i: totals[t][2 * q + i, c])

    def scale_peer(q):
        arrived(rows.at[oc * PAIRS + q], fw_r.at[q % RING])
        arrived(peer.at[q], swap_r.at[q % RING])
        scale_rows(oc * PAIRS + q, lambda t, i: peer[q, t, i])

    def param_sq(k):
        size = ROWS // CHUNKS
        at = pl.ds(pl.multiple_of(k * size, size), size)
        for t, par in enumerate((par_e, par_h)):
            v = par[:, at]
            v = jnp.sum(v * v, axis=0, keepdims=True)
            for i in range(size // LANES):
                psum[t:t + 1, :] = psum[t:t + 1, :] + v[:, i * LANES:(i + 1) * LANES]

    for q in range(2):
        cols = pl.ds(pl.multiple_of((oy if q == 0 else y) * half_of, LANES), half_of)
        arrived(both_e.at[:, 0:LANES, cols], s0e_r.at[q])
        flip_e(0, oy if q == 0 else y)
        if q == 0:
            one_e(0).start()
        part = ox if q == 0 else x
        arrived(both_h.at[:, 0, :, part], s0h_r.at[q])
        add_h(0, part)
        if q == 0:
            one_h(0).start()
    @pl.loop(0, CHUNKS)
    def _(k):
        for i in range(1, len(GROUPS)):
            first, count = GROUPS[i]

            @pl.when(k + 1 == first)
            def _():
                at = slice(first * LANES, (first + count) * LANES)
                arrived(both_e.at[:, at, :], s0e_r.at[i + 1])
                arrived(both_h.at[:, first:first + count], s0h_r.at[i + 1])

        @pl.when(k + 1 < CHUNKS)
        def _():
            combine_cores(k + 1)

        first_sum(k)
        pair = k // 2

        @pl.when(k == 0)
        def _():
            arrived(par_e, in_sem.at[0])
            arrived(par_h, in_sem.at[1])
            arrived(old_rows, in_sem.at[2])
            arrived(old_cols.at[:, c], in_sem.at[3])
            arrived(old_cols.at[:, oc], in_sem.at[4])
            pl.semaphore_wait(token.at[0], z_count)
            along_z(lambda peer_id: pl.semaphore_signal(token.at[1], inc=1, device_id=peer_id, device_id_type=MESH))

        @pl.when(k == 1)
        def _():
            pl.semaphore_wait(token.at[1], z_count)

        param_sq(k)

        @pl.when((k >= 1) & (k % 2 == 1))
        def _():
            finish(k - 1, pair, 0)

        @pl.when((k >= 2) & (k % 2 == 0))
        def _():
            finish(k - 1, pair - 1, 1)
            publish(pair - 1)

        @pl.when((k >= 6) & (k % 2 == 0))
        def _():
            scale_peer(pair - 3)

        @pl.when((k >= 4) & (k % 2 == 0))
        def _():
            row_stats(pair - 2)
            row_fwd(pair - 2).start()
            scale_own(pair - 2)

    finish(CHUNKS - 1, PAIRS - 1, 1)
    publish(PAIRS - 1)
    row_stats(PAIRS - 2)
    row_fwd(PAIRS - 2).start()
    row_stats(PAIRS - 1)
    row_fwd(PAIRS - 1).start()

    lane = lax.broadcasted_iota(jnp.int32, (1, LANES), 1)
    diag = lax.broadcasted_iota(jnp.int32, (COLS, LANES), 0) == lax.broadcasted_iota(jnp.int32, (COLS, LANES), 1)

    def as_row(acc):
        col = jnp.sum(acc, axis=1, keepdims=True)
        return jnp.sum(jnp.where(diag, col, 0.0), axis=0, keepdims=True)

    def total_of(v):
        return jnp.sum(jnp.sum(v, axis=1, keepdims=True), axis=0, keepdims=True)

    for t in range(2):
        r_part = total_of(rsum[2 * t:2 * t + 2, :])
        p_part = jnp.sum(psum[t:t + 1, :], axis=1, keepdims=True)
        for core in range(2):
            row = as_row(col_acc[t, core])
            row = jnp.where(lane == COLS, r_part, jnp.where(lane == COLS + 1, p_part, row))
            m_own[core, 2 * t:2 * t + 1, :] = row
            m_own[core, 2 * t + 1:2 * t + 2, :] = as_row(t_acc[t, core])

    columns = [(dz, fc) for dz in range(4) for fc in range(2) if dz + fc]

    def column_msg(i):
        dz, fc = columns[i]
        slot = columns.index(((4 - dz) % 4, fc))
        return remote(m_own, m_in.at[slot], send.at[9], last_r.at[0], column_id(dz, fc))

    for i in range(len(columns)):
        column_msg(i).start()

    scale_own(PAIRS - 2)
    scale_own(PAIRS - 1)
    arrived(m_in, last_r.at[0])

    total = m_own[...]
    for i in range(len(columns)):
        total = total + m_in[i]
    m_sum[...] = total
    message = jnp.zeros((1, LANES), jnp.float32)
    for t in range(2):
        cols = total[0, 2 * t:2 * t + 1, :]
        r_mean = jnp.sum(jnp.where(lane == COLS, cols, 0.0), axis=1, keepdims=True) / VOCAB
        p_col = jnp.sum(jnp.where(lane == COLS + 1, cols, 0.0), axis=1, keepdims=True)
        u_sq = jnp.zeros((1, 1), jnp.float32)
        for core in range(2):
            col_new = BETA_TWO * old_cols[t, core] + (1.0 - BETA_TWO) * (total[core, 2 * t:2 * t + 1, :COLS] / VOCAB)
            u_sq = u_sq + jnp.sum(total[core, 2 * t + 1:2 * t + 2, :COLS] * (r_mean / col_new), axis=1, keepdims=True)
        message = jnp.where(lane == 2 * t, u_sq, jnp.where(lane == 2 * t + 1, p_col, message))
    s_own[...] = message

    def scalar_msg(i, fc):
        return remote(s_own, s_in.at[i], send.at[10], last_r.at[1], plane_id(*PLANE[i], fc))

    @pl.when(c == 1)
    def _():
        for fc in (1, 0):
            for i in (2, 0, 1):
                scalar_msg(i, fc).start()

    factor_cols = []
    for t, c_out in enumerate((emb_cols_out, head_cols_out)):
        cols = m_sum[c, 2 * t:2 * t + 1, :]
        r_mean = jnp.sum(jnp.where(lane == COLS, cols, 0.0), axis=1, keepdims=True) / VOCAB
        col_new = BETA_TWO * old_cols[t, c] + (1.0 - BETA_TWO) * (cols[:, :COLS] / VOCAB)
        c_out[...] = col_new
        factor = lax.rsqrt(col_new) * jnp.sqrt(r_mean)
        factor_cols.append(jnp.sum(jnp.where(diag[:, :COLS], factor, 0.0), axis=1, keepdims=True))

    @pl.loop(PAIRS - 3, PAIRS)
    def _(q):
        scale_peer(q)

    emb_rows_out[...] = rows[:, :2, :]
    head_rows_out[...] = rows[:, 2:, :]
    arrived(both_e.at[0], send.at[0])
    arrived(both_h.at[0], send.at[1])
    arrived(in1_e, send.at[2])
    arrived(in1_h, send.at[3])
    arrived(in2_e, send.at[4])
    arrived(in2_h, send.at[5])
    arrived(peer, send.at[6])
    arrived(rp_in, send.at[7])
    arrived(rows.at[0:PAIRS], send.at[8])
    arrived(m_in, send.at[9])
    arrived(old_cols.at[:, c], send.at[11])
    arrived(s_in, last_r.at[1])
    message = s_own[...]
    for i in range(3):
        message = message + s_in[i]
    count = float(VOCAB * EMBED)
    for t in range(2):
        u_sq = jnp.sum(jnp.where(lane == 2 * t, message, 0.0), axis=1, keepdims=True)
        p_sq = jnp.sum(jnp.where(lane == 2 * t + 1, message, 0.0), axis=1, keepdims=True)
        u_rms = jnp.sqrt(u_sq / count)
        p_rms = jnp.sqrt(p_sq / count)
        step = LEARN_RATE * jnp.maximum(SCALE_FLOOR, p_rms) / jnp.maximum(1.0, u_rms / CLIP_LIMIT)
        scale_out[t] = jnp.broadcast_to(factor_cols[t] * step, (COLS, LANES))

    @pl.when(c == 1)
    def _():
        for fc in range(2):
            arrived(s_in, send.at[10])


def update_kernel(emb_g, head_g, emb_p, head_p, emb_rows, head_rows, emb_cols, head_cols, scale,
                  emb_new, head_new, emb_rows_new, head_rows_new, emb_cols_new, head_cols_new, emb_half, head_half,
                  new_buf, half_buf, small_sem, big_sem):
    small = [pltpu.make_async_copy(src, dst, small_sem.at[i]) for i, (src, dst) in enumerate(
        ((emb_rows, emb_rows_new), (head_rows, head_rows_new), (emb_cols, emb_cols_new), (head_cols, head_cols_new)))]
    for cp in small:
        cp.start()
    size = COLS // PARTS
    for i in range(PARTS):
        part = slice(i * size, (i + 1) * size)
        for t, (p, g, new, half) in enumerate(((emb_p, emb_g, emb_new, emb_half), (head_p, head_g, head_new, head_half))):
            value = p[part, :] - g[part, :] * scale[t, part, 0:1]
            new_buf[t, part, :] = value
            half_buf[t, part, :] = value.astype(jnp.bfloat16)
            pltpu.make_async_copy(new_buf.at[t, part, :], new.at[part, :], big_sem.at[0]).start()
            pltpu.make_async_copy(half_buf.at[t, part, :], half.at[part, :], big_sem.at[1]).start()
    for cp in small:
        cp.wait()
    pltpu.make_async_copy(new_buf, new_buf, big_sem.at[0]).wait()
    pltpu.make_async_copy(half_buf, half_buf, big_sem.at[1]).wait()


def local_step(emb_p, head_p, emb_g, head_g, emb_r, emb_c, head_r, head_c):
    f32 = jnp.float32
    n = CHUNKS
    dma = pltpu.SemaphoreType.DMA
    hbm = pl.BlockSpec(memory_space=pltpu.HBM)
    vmem = pl.BlockSpec(memory_space=pltpu.VMEM)
    rows_shape = (BLOCKS, 2, LANES)
    table = jax.ShapeDtypeStruct((COLS, ROWS), f32)
    half = jax.ShapeDtypeStruct((COLS, ROWS), jnp.bfloat16)
    emb_p = emb_p.T
    shapes = [(2, ROWS // 2, EMBED), (n, 2, 2, 2, COLS, LANES), (2, n, 2, 2, 2, COLS, LANES)]
    shapes += [(n, 2, 2, COLS, LANES)] * 2 + [(n, 2, COLS, LANES)] * 2 + [(PAIRS, 2, 2, COLS, LANES)]
    shapes += [(BLOCKS, 4, LANES), (2, *rows_shape), (2, 2, 1, COLS)]
    shapes += [(PAIRS, 4, LANES), (PAIRS, 3, 4, LANES)]
    shapes += [(2, 2, COLS, LANES)] * 2 + [(4, LANES), (2, LANES)]
    shapes += [(2, 4, LANES), (7, 2, 4, LANES), (2, 4, LANES), (1, LANES), (3, 1, LANES)]
    scratch = [pltpu.VMEM(shape, f32) for shape in shapes]
    scratch += [dma((len(GROUPS) + 1,))] * 2 + [dma((RING,))] * 7
    scratch += [dma((12,)), dma((2,)), dma((5,)), pltpu.SemaphoreType.REGULAR((2,))]
    kept = [pltpu.VMEM((COLS, ROWS), f32)] * 4 + [pltpu.VMEM(rows_shape, f32)] * 2 + [pltpu.VMEM((1, COLS), f32)] * 2
    kept.append(pltpu.VMEM((2, COLS, LANES), f32))
    state = pl.pallas_call(
        exchange_kernel,
        out_shape=tuple(kept),
        in_specs=[hbm] * 8,
        out_specs=(vmem,) * 9,
        scratch_shapes=scratch,
        compiler_params=pltpu.CompilerParams(collective_id=0, has_side_effects=True, vmem_limit_bytes=60_000_000),
        name="exchange",
    )(emb_g.reshape(ROWS, EMBED), head_g.reshape(2, 2, 2, COLS, ROWS), emb_p, head_p,
      emb_r.reshape(rows_shape), head_r.reshape(rows_shape), emb_c.reshape(1, COLS), head_c.reshape(1, COLS))

    outs = pl.pallas_call(
        update_kernel,
        out_shape=(table, table, jax.ShapeDtypeStruct(rows_shape, f32), jax.ShapeDtypeStruct(rows_shape, f32),
                   jax.ShapeDtypeStruct((1, COLS), f32), jax.ShapeDtypeStruct((1, COLS), f32), half, half),
        in_specs=[vmem] * 9,
        out_specs=(hbm,) * 8,
        scratch_shapes=[pltpu.VMEM((2, COLS, ROWS), f32), pltpu.VMEM((2, COLS, ROWS), jnp.bfloat16),
                        dma((4,)), dma((2,))],
        compiler_params=pltpu.CompilerParams(vmem_limit_bytes=16 * 2 ** 20),
        name="update",
    )(*state)
    emb_new, head_new, emb_rn, head_rn, emb_cn, head_cn, emb_half, head_half = outs
    return (emb_new.T, head_new, emb_rn.reshape(ROWS), emb_cn.reshape(COLS), head_rn.reshape(ROWS),
            head_cn.reshape(COLS), emb_half.T, head_half)


def solution(mesh):
    arg_specs = (P("model", "data"), P("data", "model"), P("data", "model", None), P("data", None, "model"),
                 P("model"), P("data"), P("model"), P("data"))
    result_specs = (P("model", "data"), P("data", "model"), P("model"), P("data"), P("model"), P("data"),
                    P("model", "data"), P("data", "model"))
    mapped = jax.shard_map(local_step, mesh=mesh, in_specs=arg_specs, out_specs=result_specs, check_vma=False)

    def update_tables(emb_param, head_param, emb_grad, head_grad, emb_row, emb_col, head_row, head_col):
        return mapped(emb_param, head_param, emb_grad, head_grad, emb_row, emb_col, head_row, head_col)

    return update_tables
```

```python
import functools

import jax
import jax.numpy as jnp
from jax import lax
from jax.experimental import pallas as pl
from jax.experimental.pallas import tpu as pltpu
from jax.sharding import PartitionSpec as P

TRAIN_STEP = 10
DECAY_EXP = 0.8
EPS_ONE = 1e-30
CLIP_LIMIT = 1.0
SCALE_FLOOR = 1e-3
LEARN_RATE = float(TRAIN_STEP) ** -0.5
BETA_TWO = 1.0 - float(TRAIN_STEP) ** -DECAY_EXP

VOCAB = 16384
EMBED = 768
ROWS = VOCAB // 4
COLS = EMBED // 8
LANES = 128
CHUNKS = ROWS // 2 // LANES
GROUPS = ((0, 1), (1, 1), (2, 2), (4, 12))
PAIRS = CHUNKS // 2
BLOCKS = 2 * PAIRS
RING = 4
PARTS = 3
MESH = pl.DeviceIdType.MESH
PLANE = ((0, 1), (1, 0), (1, 1))


def exchange_kernel(emb_ref, head_ref, emb_p_ref, head_p_ref, emb_r_ref, head_r_ref, emb_c_ref, head_c_ref,
                    stage_e, stage_h, par_e, par_h, emb_rows_out, head_rows_out, emb_cols_out, head_cols_out, scale_out,
                    both_e, sum_e, both_h, in1_e, in1_h, in2_e, in2_h, peer,
                    rows, old_rows, old_cols, rp_own, rp_in, col_acc, t_acc, rsum, psum, m_own, m_in, m_sum, s_own, s_in,
                    s0e_r, s0h_r, s1e_r, s1h_r, s2e_r, s2h_r, swap_r, rp_r, fw_r, send, last_r, in_sem, token):
    model = lax.axis_index("model")
    data = lax.axis_index("data")
    c = data % 2
    x = (data // 2) % 2
    y = data // 4
    oc, ox, oy = 1 - c, 1 - x, 1 - y

    def plane_id(fy, fx, fc):
        step = fy * (4 - 8 * y) + fx * (2 - 4 * x) + fc * (1 - 2 * c)
        return (model, data + step)

    def column_id(dz, fc):
        return ((model + dz) % 4, data + fc * (1 - 2 * c))

    core_peer, x_peer, y_peer = plane_id(0, 0, 1), plane_id(0, 1, 0), plane_id(1, 0, 0)

    def remote(src, dst, send_sem, recv_sem, peer_id):
        return pltpu.make_async_remote_copy(src_ref=src, dst_ref=dst, send_sem=send_sem, recv_sem=recv_sem,
                                            device_id=peer_id, device_id_type=MESH)

    def arrived(ref, sem):
        pltpu.make_async_copy(ref, ref, sem).wait()

    def vocab_at(core, first, count):
        return pl.ds(pl.multiple_of(core * (ROWS // 2) + first * LANES, LANES), count * LANES)

    half_of = 4 * COLS

    def first_e(q):
        cols = pl.ds(pl.multiple_of((oy if q == 0 else y) * half_of, LANES), half_of)
        return (pltpu.make_async_copy(emb_ref.at[vocab_at(c, 0, 1), cols], both_e.at[0, 0:LANES, cols], s0e_r.at[q]),
                remote(emb_ref.at[vocab_at(oc, 0, 1), cols], both_e.at[1, 0:LANES, cols], send.at[0], s0e_r.at[q], core_peer))

    def first_h(q):
        part = ox if q == 0 else x
        return (pltpu.make_async_copy(head_ref.at[:, part, :, :, vocab_at(c, 0, 1)], both_h.at[0, 0, :, part], s0h_r.at[q]),
                remote(head_ref.at[:, part, :, :, vocab_at(oc, 0, 1)], both_h.at[1, 0, :, part], send.at[1], s0h_r.at[q], core_peer))

    def group_e(i):
        first, count = GROUPS[i]
        at = slice(first * LANES, (first + count) * LANES)
        return (pltpu.make_async_copy(emb_ref.at[vocab_at(c, first, count), :], both_e.at[0, at, :], s0e_r.at[i + 1]),
                remote(emb_ref.at[vocab_at(oc, first, count), :], both_e.at[1, at, :], send.at[0], s0e_r.at[i + 1], core_peer))

    def group_h(i):
        first, count = GROUPS[i]
        pairs = []
        for j in range(first, first + count):
            pairs.append((pltpu.make_async_copy(head_ref.at[:, :, :, :, vocab_at(c, j, 1)], both_h.at[0, j], s0h_r.at[i + 1]),
                          remote(head_ref.at[:, :, :, :, vocab_at(oc, j, 1)], both_h.at[1, j], send.at[1], s0h_r.at[i + 1],
                                 core_peer)))
        return pairs

    def one_e(k):
        return remote(sum_e.at[k, oy], in1_e.at[k], send.at[2], s1e_r.at[k % RING], y_peer)

    def one_h(k):
        return remote(both_h.at[0, k, :, ox], in1_h.at[k], send.at[3], s1h_r.at[k % RING], x_peer)

    def two_e(k):
        return remote(in1_e.at[k, ox], in2_e.at[k], send.at[4], s2e_r.at[k % RING], x_peer)

    def two_h(k):
        return remote(in1_h.at[k, oy], in2_h.at[k], send.at[5], s2h_r.at[k % RING], y_peer)

    def swap(q):
        return [remote(total.at[pl.ds(2 * q, 2), oc], peer.at[q, t], send.at[6], swap_r.at[q % RING], core_peer)
                for t, total in enumerate((in2_e, in2_h))]

    def row_msg(q, i):
        fy, fx = PLANE[i]
        return remote(rp_own.at[q], rp_in.at[q, i], send.at[7], rp_r.at[q % RING], plane_id(fy, fx, 0))

    def row_fwd(q):
        return remote(rows.at[c * PAIRS + q], rows.at[c * PAIRS + q], send.at[8], fw_r.at[q % RING], core_peer)

    small_loads = [pltpu.make_async_copy(src, dst, in_sem.at[i]) for i, (src, dst) in (
        (0, (emb_p_ref, par_e)), (1, (head_p_ref, par_h)), (2, (emb_r_ref, old_rows.at[0])), (2, (head_r_ref, old_rows.at[1])),
        (3, (emb_c_ref, old_cols.at[0, c])), (3, (head_c_ref, old_cols.at[1, c])))]
    old_cols_out = [remote(src, old_cols.at[t, c], send.at[11], in_sem.at[4], core_peer)
                    for t, src in enumerate((emb_c_ref, head_c_ref))]

    barrier = pltpu.get_barrier_semaphore()
    above, below = column_id(1, 0), column_id(3, 0)
    for peer_id in (core_peer, x_peer, y_peer):
        pl.semaphore_signal(barrier, inc=1, device_id=peer_id, device_id_type=MESH)

    z_count = 1 + model * (3 - model) // 2

    def along_z(act):
        @pl.when(model < 3)
        def _():
            act(above)

        @pl.when(model > 0)
        def _():
            act(below)

    along_z(lambda peer_id: pl.semaphore_signal(barrier, inc=1, device_id=peer_id, device_id_type=MESH))
    for q in range(2):
        first_e(q)[0].start()
        first_h(q)[0].start()
    for i in range(1, len(GROUPS)):
        group_e(i)[0].start()
        for cp, _ in group_h(i):
            cp.start()
    pl.semaphore_wait(barrier, 3 + z_count)

    for q in range(2):
        first_e(q)[1].start()
        first_h(q)[1].start()
    for cp in old_cols_out:
        cp.start()
    for i in range(1, len(GROUPS)):
        group_e(i)[1].start()
        for _, cp in group_h(i):
            cp.start()
    for cp in small_loads:
        cp.start()
    along_z(lambda peer_id: pl.semaphore_signal(token.at[0], inc=1, device_id=peer_id, device_id_type=MESH))

    col_acc[...] = jnp.zeros_like(col_acc)
    t_acc[...] = jnp.zeros_like(t_acc)
    rsum[...] = jnp.zeros_like(rsum)
    psum[...] = jnp.zeros_like(psum)

    def flip_e(k, half):
        at = pl.ds(pl.multiple_of(k * LANES, LANES), LANES)
        for j in range(half_of // LANES):
            cols = pl.ds(pl.multiple_of(half * half_of + j * LANES, LANES), LANES)
            strip = (both_e[0, at, cols] + both_e[1, at, cols]).T
            done = 0
            while done < LANES:
                block, row = divmod(LANES * j + done, COLS)
                size = min(LANES - done, COLS - row)
                sum_e[k, half, block // 2, block % 2, row:row + size, :] = strip[done:done + size, :]
                done += size

    def add_h(k, part):
        for a in range(2):
            for b in range(2):
                both_h[0, k, a, part, b] = both_h[0, k, a, part, b] + both_h[1, k, a, part, b]

    def combine_cores(k):
        flip_e(k, oy)
        one_e(k).start()
        add_h(k, ox)
        one_h(k).start()
        flip_e(k, y)
        add_h(k, x)

    def first_sum(k):
        one_e(k).wait_recv()
        in1_e[k, ox] = in1_e[k, ox] + sum_e[k, y, ox]
        two_e(k).start()
        in1_e[k, x] = in1_e[k, x] + sum_e[k, y, x]
        one_h(k).wait_recv()
        in1_h[k, oy] = in1_h[k, oy] + both_h[0, k, oy, x]
        two_h(k).start()
        in1_h[k, y] = in1_h[k, y] + both_h[0, k, y, x]

    def finish(k, q, i):
        two_e(k).wait_recv()
        for core in range(2):
            in2_e[k, core] = in2_e[k, core] + in1_e[k, x, core]
        two_h(k).wait_recv()
        for core in range(2):
            in2_h[k, core] = in2_h[k, core] + in1_h[k, y, core]
        for t, total in enumerate((in2_e, in2_h)):
            row_part = jnp.zeros((1, LANES), jnp.float32)
            for core in range(2):
                g = total[k, core]
                sq = g * g + EPS_ONE
                col_acc[t, core] = col_acc[t, core] + sq
                row_part = row_part + jnp.sum(sq, axis=0, keepdims=True)
            rp_own[q, 2 * t + i:2 * t + i + 1, :] = row_part

    def publish(q):
        for i in range(3):
            row_msg(q, i).start()
        for cp in swap(q):
            cp.start()

    def row_stats(q):
        arrived(rp_in.at[q], rp_r.at[q % RING])
        block = c * PAIRS + q
        row_sq = (rp_own[q] + rp_in[q, 0]) + (rp_in[q, 1] + rp_in[q, 2])
        old = jnp.concatenate([old_rows[0, block], old_rows[1, block]], axis=0)
        row_new = BETA_TWO * old + (1.0 - BETA_TWO) * (row_sq / EMBED)
        rows[block] = row_new
        rsum[...] = rsum[...] + row_new
        inv = 1.0 / row_new
        for t, total in enumerate((in2_e, in2_h)):
            for core in range(2):
                acc = t_acc[t, core]
                for i in range(2):
                    g = total[2 * q + i, core]
                    acc = acc + (g * g) * inv[2 * t + i:2 * t + i + 1, :]
                t_acc[t, core] = acc

    def scale_rows(block, get):
        factor = lax.rsqrt(rows[block])
        base = pl.multiple_of(block * (2 * LANES), 2 * LANES)
        for t, stage in enumerate((stage_e, stage_h)):
            for i in range(2):
                stage[:, pl.ds(base + i * LANES, LANES)] = get(t, i) * factor[2 * t + i:2 * t + i + 1, :]

    def scale_own(q):
        totals = (in2_e, in2_h)
        scale_rows(c * PAIRS + q, lambda t, i: totals[t][2 * q + i, c])

    def scale_peer(q):
        arrived(rows.at[oc * PAIRS + q], fw_r.at[q % RING])
        arrived(peer.at[q], swap_r.at[q % RING])
        scale_rows(oc * PAIRS + q, lambda t, i: peer[q, t, i])

    def param_sq(k):
        size = ROWS // CHUNKS * 2
        at = pl.ds(pl.multiple_of(k * size, size), size)
        for t, par in enumerate((par_e, par_h)):
            v = par[:, at]
            v = jnp.sum(v * v, axis=0, keepdims=True)
            for i in range(size // LANES):
                psum[t:t + 1, :] = psum[t:t + 1, :] + v[:, i * LANES:(i + 1) * LANES]

    for q in range(2):
        cols = pl.ds(pl.multiple_of((oy if q == 0 else y) * half_of, LANES), half_of)
        arrived(both_e.at[:, 0:LANES, cols], s0e_r.at[q])
        flip_e(0, oy if q == 0 else y)
        if q == 0:
            one_e(0).start()
        part = ox if q == 0 else x
        arrived(both_h.at[:, 0, :, part], s0h_r.at[q])
        add_h(0, part)
        if q == 0:
            one_h(0).start()
    @pl.loop(0, CHUNKS)
    def _(k):
        for i in range(1, len(GROUPS)):
            first, count = GROUPS[i]

            @pl.when(k + 1 == first)
            def _():
                at = slice(first * LANES, (first + count) * LANES)
                arrived(both_e.at[:, at, :], s0e_r.at[i + 1])
                arrived(both_h.at[:, first:first + count], s0h_r.at[i + 1])

        @pl.when(k + 1 < CHUNKS)
        def _():
            combine_cores(k + 1)

        first_sum(k)
        pair = k // 2

        @pl.when(k == 1)
        def _():
            pl.semaphore_wait(token.at[0], z_count)
            along_z(lambda peer_id: pl.semaphore_signal(token.at[1], inc=1, device_id=peer_id, device_id_type=MESH))

        @pl.when(k == 2)
        def _():
            pl.semaphore_wait(token.at[1], z_count)

        @pl.when(k == 3)
        def _():
            arrived(par_e, in_sem.at[0])
            arrived(par_h, in_sem.at[1])
            arrived(old_rows, in_sem.at[2])

        @pl.when(k >= CHUNKS // 2)
        def _():
            param_sq(k - CHUNKS // 2)

        @pl.when((k >= 1) & (k % 2 == 1))
        def _():
            finish(k - 1, pair, 0)

        @pl.when((k >= 2) & (k % 2 == 0))
        def _():
            finish(k - 1, pair - 1, 1)
            publish(pair - 1)

        @pl.when((k >= 6) & (k % 2 == 0))
        def _():
            scale_peer(pair - 3)

        @pl.when((k >= 4) & (k % 2 == 0))
        def _():
            row_stats(pair - 2)
            row_fwd(pair - 2).start()
            scale_own(pair - 2)

    finish(CHUNKS - 1, PAIRS - 1, 1)
    publish(PAIRS - 1)
    row_stats(PAIRS - 2)
    row_fwd(PAIRS - 2).start()
    row_stats(PAIRS - 1)
    row_fwd(PAIRS - 1).start()

    lane = lax.broadcasted_iota(jnp.int32, (1, LANES), 1)
    diag = lax.broadcasted_iota(jnp.int32, (COLS, LANES), 0) == lax.broadcasted_iota(jnp.int32, (COLS, LANES), 1)

    def as_row(acc):
        col = jnp.sum(acc, axis=1, keepdims=True)
        return jnp.sum(jnp.where(diag, col, 0.0), axis=0, keepdims=True)

    def total_of(v):
        return jnp.sum(jnp.sum(v, axis=1, keepdims=True), axis=0, keepdims=True)

    for t in range(2):
        r_part = total_of(rsum[2 * t:2 * t + 2, :])
        p_part = jnp.sum(psum[t:t + 1, :], axis=1, keepdims=True)
        for core in range(2):
            row = as_row(col_acc[t, core])
            row = jnp.where(lane == COLS, r_part, jnp.where(lane == COLS + 1, p_part, row))
            m_own[core, 2 * t:2 * t + 1, :] = row
            m_own[core, 2 * t + 1:2 * t + 2, :] = as_row(t_acc[t, core])

    columns = [(dz, fc) for dz in range(4) for fc in range(2) if dz + fc]

    def column_msg(i):
        dz, fc = columns[i]
        slot = columns.index(((4 - dz) % 4, fc))
        return remote(m_own, m_in.at[slot], send.at[9], last_r.at[0], column_id(dz, fc))

    for i in range(len(columns)):
        column_msg(i).start()

    scale_own(PAIRS - 2)
    scale_own(PAIRS - 1)
    arrived(old_cols.at[:, c], in_sem.at[3])
    arrived(old_cols.at[:, oc], in_sem.at[4])
    arrived(m_in, last_r.at[0])

    total = m_own[...]
    for i in range(len(columns)):
        total = total + m_in[i]
    m_sum[...] = total
    message = jnp.zeros((1, LANES), jnp.float32)
    for t in range(2):
        cols = total[0, 2 * t:2 * t + 1, :]
        r_mean = jnp.sum(jnp.where(lane == COLS, cols, 0.0), axis=1, keepdims=True) / VOCAB
        p_col = jnp.sum(jnp.where(lane == COLS + 1, cols, 0.0), axis=1, keepdims=True)
        u_sq = jnp.zeros((1, 1), jnp.float32)
        for core in range(2):
            col_new = BETA_TWO * old_cols[t, core] + (1.0 - BETA_TWO) * (total[core, 2 * t:2 * t + 1, :COLS] / VOCAB)
            u_sq = u_sq + jnp.sum(total[core, 2 * t + 1:2 * t + 2, :COLS] * (r_mean / col_new), axis=1, keepdims=True)
        message = jnp.where(lane == 2 * t, u_sq, jnp.where(lane == 2 * t + 1, p_col, message))
    s_own[...] = message

    def scalar_msg(i, fc):
        return remote(s_own, s_in.at[i], send.at[10], last_r.at[1], plane_id(*PLANE[i], fc))

    @pl.when(c == 1)
    def _():
        for fc in (1, 0):
            for i in (2, 0, 1):
                scalar_msg(i, fc).start()

    factor_cols = []
    for t, c_out in enumerate((emb_cols_out, head_cols_out)):
        cols = m_sum[c, 2 * t:2 * t + 1, :]
        r_mean = jnp.sum(jnp.where(lane == COLS, cols, 0.0), axis=1, keepdims=True) / VOCAB
        col_new = BETA_TWO * old_cols[t, c] + (1.0 - BETA_TWO) * (cols[:, :COLS] / VOCAB)
        c_out[...] = col_new
        factor = lax.rsqrt(col_new) * jnp.sqrt(r_mean)
        factor_cols.append(jnp.sum(jnp.where(diag[:, :COLS], factor, 0.0), axis=1, keepdims=True))

    @pl.loop(PAIRS - 3, PAIRS)
    def _(q):
        scale_peer(q)

    emb_rows_out[...] = rows[:, :2, :]
    head_rows_out[...] = rows[:, 2:, :]
    arrived(both_e.at[0], send.at[0])
    arrived(both_h.at[0], send.at[1])
    arrived(in1_e, send.at[2])
    arrived(in1_h, send.at[3])
    arrived(in2_e, send.at[4])
    arrived(in2_h, send.at[5])
    arrived(peer, send.at[6])
    arrived(rp_in, send.at[7])
    arrived(rows.at[0:PAIRS], send.at[8])
    arrived(m_in, send.at[9])
    arrived(old_cols.at[:, c], send.at[11])
    arrived(s_in, last_r.at[1])
    message = s_own[...]
    for i in range(3):
        message = message + s_in[i]
    count = float(VOCAB * EMBED)
    for t in range(2):
        u_sq = jnp.sum(jnp.where(lane == 2 * t, message, 0.0), axis=1, keepdims=True)
        p_sq = jnp.sum(jnp.where(lane == 2 * t + 1, message, 0.0), axis=1, keepdims=True)
        u_rms = jnp.sqrt(u_sq / count)
        p_rms = jnp.sqrt(p_sq / count)
        step = LEARN_RATE * jnp.maximum(SCALE_FLOOR, p_rms) / jnp.maximum(1.0, u_rms / CLIP_LIMIT)
        scale_out[t] = jnp.broadcast_to(factor_cols[t] * step, (COLS, LANES))

    @pl.when(c == 1)
    def _():
        for fc in range(2):
            arrived(s_in, send.at[10])


def update_kernel(emb_g, head_g, emb_p, head_p, emb_rows, head_rows, emb_cols, head_cols, scale,
                  emb_new, head_new, emb_rows_new, head_rows_new, emb_cols_new, head_cols_new, emb_half, head_half,
                  new_buf, half_buf, small_sem, big_sem):
    small = [pltpu.make_async_copy(src, dst, small_sem.at[i]) for i, (src, dst) in enumerate(
        ((emb_rows, emb_rows_new), (head_rows, head_rows_new), (emb_cols, emb_cols_new), (head_cols, head_cols_new)))]
    for cp in small:
        cp.start()
    size = COLS // PARTS
    for i in range(PARTS):
        part = slice(i * size, (i + 1) * size)
        for t, (p, g, new, half) in enumerate(((emb_p, emb_g, emb_new, emb_half), (head_p, head_g, head_new, head_half))):
            value = p[part, :] - g[part, :] * scale[t, part, 0:1]
            new_buf[t, part, :] = value
            half_buf[t, part, :] = value.astype(jnp.bfloat16)
            pltpu.make_async_copy(new_buf.at[t, part, :], new.at[part, :], big_sem.at[0]).start()
            pltpu.make_async_copy(half_buf.at[t, part, :], half.at[part, :], big_sem.at[1]).start()
    for cp in small:
        cp.wait()
    pltpu.make_async_copy(new_buf, new_buf, big_sem.at[0]).wait()
    pltpu.make_async_copy(half_buf, half_buf, big_sem.at[1]).wait()


def local_step(emb_p, head_p, emb_g, head_g, emb_r, emb_c, head_r, head_c):
    f32 = jnp.float32
    n = CHUNKS
    dma = pltpu.SemaphoreType.DMA
    hbm = pl.BlockSpec(memory_space=pltpu.HBM)
    vmem = pl.BlockSpec(memory_space=pltpu.VMEM)
    rows_shape = (BLOCKS, 2, LANES)
    table = jax.ShapeDtypeStruct((COLS, ROWS), f32)
    half = jax.ShapeDtypeStruct((COLS, ROWS), jnp.bfloat16)
    emb_p = emb_p.T
    shapes = [(2, ROWS // 2, EMBED), (n, 2, 2, 2, COLS, LANES), (2, n, 2, 2, 2, COLS, LANES)]
    shapes += [(n, 2, 2, COLS, LANES)] * 2 + [(n, 2, COLS, LANES)] * 2 + [(PAIRS, 2, 2, COLS, LANES)]
    shapes += [(BLOCKS, 4, LANES), (2, *rows_shape), (2, 2, 1, COLS)]
    shapes += [(PAIRS, 4, LANES), (PAIRS, 3, 4, LANES)]
    shapes += [(2, 2, COLS, LANES)] * 2 + [(4, LANES), (2, LANES)]
    shapes += [(2, 4, LANES), (7, 2, 4, LANES), (2, 4, LANES), (1, LANES), (3, 1, LANES)]
    scratch = [pltpu.VMEM(shape, f32) for shape in shapes]
    scratch += [dma((len(GROUPS) + 1,))] * 2 + [dma((RING,))] * 7
    scratch += [dma((12,)), dma((2,)), dma((5,)), pltpu.SemaphoreType.REGULAR((2,))]
    kept = [pltpu.VMEM((COLS, ROWS), f32)] * 4 + [pltpu.VMEM(rows_shape, f32)] * 2 + [pltpu.VMEM((1, COLS), f32)] * 2
    kept.append(pltpu.VMEM((2, COLS, LANES), f32))
    state = pl.pallas_call(
        exchange_kernel,
        out_shape=tuple(kept),
        in_specs=[hbm] * 8,
        out_specs=(vmem,) * 9,
        scratch_shapes=scratch,
        compiler_params=pltpu.CompilerParams(collective_id=0, has_side_effects=True, vmem_limit_bytes=60_000_000),
        name="exchange",
    )(emb_g.reshape(ROWS, EMBED), head_g.reshape(2, 2, 2, COLS, ROWS), emb_p, head_p,
      emb_r.reshape(rows_shape), head_r.reshape(rows_shape), emb_c.reshape(1, COLS), head_c.reshape(1, COLS))

    outs = pl.pallas_call(
        update_kernel,
        out_shape=(table, table, jax.ShapeDtypeStruct(rows_shape, f32), jax.ShapeDtypeStruct(rows_shape, f32),
                   jax.ShapeDtypeStruct((1, COLS), f32), jax.ShapeDtypeStruct((1, COLS), f32), half, half),
        in_specs=[vmem] * 9,
        out_specs=(hbm,) * 8,
        scratch_shapes=[pltpu.VMEM((2, COLS, ROWS), f32), pltpu.VMEM((2, COLS, ROWS), jnp.bfloat16),
                        dma((4,)), dma((2,))],
        compiler_params=pltpu.CompilerParams(vmem_limit_bytes=16 * 2 ** 20),
        name="update",
    )(*state)
    emb_new, head_new, emb_rn, head_rn, emb_cn, head_cn, emb_half, head_half = outs
    return (emb_new.T, head_new, emb_rn.reshape(ROWS), emb_cn.reshape(COLS), head_rn.reshape(ROWS),
            head_cn.reshape(COLS), emb_half.T, head_half)


def solution(mesh):
    arg_specs = (P("model", "data"), P("data", "model"), P("data", "model", None), P("data", None, "model"),
                 P("model"), P("data"), P("model"), P("data"))
    result_specs = (P("model", "data"), P("data", "model"), P("model"), P("data"), P("model"), P("data"),
                    P("model", "data"), P("data", "model"))
    mapped = jax.shard_map(local_step, mesh=mesh, in_specs=arg_specs, out_specs=result_specs, check_vma=False)

    def update_tables(emb_param, head_param, emb_grad, head_grad, emb_row, emb_col, head_row, head_col):
        return mapped(emb_param, head_param, emb_grad, head_grad, emb_row, emb_col, head_row, head_col)

    return update_tables
```

```python
import functools

import jax
import jax.numpy as jnp
from jax import lax
from jax.experimental import pallas as pl
from jax.experimental.pallas import tpu as pltpu
from jax.sharding import PartitionSpec as P

TRAIN_STEP = 10
DECAY_EXP = 0.8
EPS_ONE = 1e-30
CLIP_LIMIT = 1.0
SCALE_FLOOR = 1e-3
LEARN_RATE = float(TRAIN_STEP) ** -0.5
BETA_TWO = 1.0 - float(TRAIN_STEP) ** -DECAY_EXP

VOCAB = 16384
EMBED = 768
ROWS = VOCAB // 4
COLS = EMBED // 8
LANES = 128
CHUNKS = ROWS // 2 // LANES
GROUPS = ((0, 1), (1, 1), (2, 2), (4, 12))
PAIRS = CHUNKS // 2
BLOCKS = 2 * PAIRS
AHEAD = 2
DEEP = 6
RING = 4
PARTS = 3
MESH = pl.DeviceIdType.MESH
PLANE = ((0, 1), (1, 0), (1, 1))


def exchange_kernel(emb_ref, head_ref, emb_p_ref, head_p_ref, emb_r_ref, head_r_ref, emb_c_ref, head_c_ref,
                    stage_e, stage_h, par_e, par_h, emb_rows_out, head_rows_out, emb_cols_out, head_cols_out, scale_out,
                    both_e, sum_e, both_h, in1_e, in1_h, in2_e, in2_h, peer,
                    rows, old_rows, old_cols, rp_own, rp_in, col_acc, t_acc, rsum, psum, m_own, m_in, m_sum, s_own, s_in,
                    s0e_r, s0h_r, s1e_r, s1h_r, s2e_r, s2h_r, swap_r, rp_r, fw_r, send, last_r, in_sem, token):
    model = lax.axis_index("model")
    data = lax.axis_index("data")
    c = data % 2
    x = (data // 2) % 2
    y = data // 4
    oc, ox, oy = 1 - c, 1 - x, 1 - y

    def plane_id(fy, fx, fc):
        step = fy * (4 - 8 * y) + fx * (2 - 4 * x) + fc * (1 - 2 * c)
        return (model, data + step)

    def column_id(dz, fc):
        return ((model + dz) % 4, data + fc * (1 - 2 * c))

    core_peer, x_peer, y_peer = plane_id(0, 0, 1), plane_id(0, 1, 0), plane_id(1, 0, 0)

    def remote(src, dst, send_sem, recv_sem, peer_id):
        return pltpu.make_async_remote_copy(src_ref=src, dst_ref=dst, send_sem=send_sem, recv_sem=recv_sem,
                                            device_id=peer_id, device_id_type=MESH)

    def arrived(ref, sem):
        pltpu.make_async_copy(ref, ref, sem).wait()

    def vocab_at(core, first, count):
        return pl.ds(pl.multiple_of(core * (ROWS // 2) + first * LANES, LANES), count * LANES)

    half_of = 4 * COLS

    def first_e(q):
        cols = pl.ds(pl.multiple_of((oy if q == 0 else y) * half_of, LANES), half_of)
        return (pltpu.make_async_copy(emb_ref.at[vocab_at(c, 0, 1), cols], both_e.at[0, 0:LANES, cols], s0e_r.at[q]),
                remote(emb_ref.at[vocab_at(oc, 0, 1), cols], both_e.at[1, 0:LANES, cols], send.at[0], s0e_r.at[q], core_peer))

    def first_h(q):
        part = ox if q == 0 else x
        return (pltpu.make_async_copy(head_ref.at[:, part, :, :, vocab_at(c, 0, 1)], both_h.at[0, 0, :, part], s0h_r.at[q]),
                remote(head_ref.at[:, part, :, :, vocab_at(oc, 0, 1)], both_h.at[1, 0, :, part], send.at[1], s0h_r.at[q], core_peer))

    def group_e(i):
        first, count = GROUPS[i]
        at = slice(first * LANES, (first + count) * LANES)
        return (pltpu.make_async_copy(emb_ref.at[vocab_at(c, first, count), :], both_e.at[0, at, :], s0e_r.at[i + 1]),
                remote(emb_ref.at[vocab_at(oc, first, count), :], both_e.at[1, at, :], send.at[0], s0e_r.at[i + 1], core_peer))

    def group_h(i):
        first, count = GROUPS[i]
        pairs = []
        for j in range(first, first + count):
            pairs.append((pltpu.make_async_copy(head_ref.at[:, :, :, :, vocab_at(c, j, 1)], both_h.at[0, j], s0h_r.at[i + 1]),
                          remote(head_ref.at[:, :, :, :, vocab_at(oc, j, 1)], both_h.at[1, j], send.at[1], s0h_r.at[i + 1],
                                 core_peer)))
        return pairs

    def one_e(k):
        return remote(sum_e.at[k, oy], in1_e.at[k], send.at[2], s1e_r.at[k % DEEP], y_peer)

    def one_h(k):
        return remote(both_h.at[0, k, :, ox], in1_h.at[k], send.at[3], s1h_r.at[k % DEEP], x_peer)

    def two_e(k):
        return remote(in1_e.at[k, ox], in2_e.at[k], send.at[4], s2e_r.at[k % RING], x_peer)

    def two_h(k):
        return remote(in1_h.at[k, oy], in2_h.at[k], send.at[5], s2h_r.at[k % RING], y_peer)

    def swap(q):
        return [remote(total.at[pl.ds(2 * q, 2), oc], peer.at[q, t], send.at[6], swap_r.at[q % RING], core_peer)
                for t, total in enumerate((in2_e, in2_h))]

    def row_msg(q, i):
        fy, fx = PLANE[i]
        return remote(rp_own.at[q], rp_in.at[q, i], send.at[7], rp_r.at[q % RING], plane_id(fy, fx, 0))

    def row_fwd(q):
        return remote(rows.at[c * PAIRS + q], rows.at[c * PAIRS + q], send.at[8], fw_r.at[q % RING], core_peer)

    small_loads = [pltpu.make_async_copy(src, dst, in_sem.at[i]) for i, (src, dst) in (
        (0, (emb_p_ref, par_e)), (1, (head_p_ref, par_h)), (2, (emb_r_ref, old_rows.at[0])), (2, (head_r_ref, old_rows.at[1])),
        (3, (emb_c_ref, old_cols.at[0, c])), (3, (head_c_ref, old_cols.at[1, c])))]
    old_cols_out = [remote(src, old_cols.at[t, c], send.at[11], in_sem.at[4], core_peer)
                    for t, src in enumerate((emb_c_ref, head_c_ref))]

    barrier = pltpu.get_barrier_semaphore()
    above, below = column_id(1, 0), column_id(3, 0)
    for peer_id in (core_peer, x_peer, y_peer):
        pl.semaphore_signal(barrier, inc=1, device_id=peer_id, device_id_type=MESH)

    z_count = 1 + model * (3 - model) // 2

    def along_z(act):
        @pl.when(model < 3)
        def _():
            act(above)

        @pl.when(model > 0)
        def _():
            act(below)

    along_z(lambda peer_id: pl.semaphore_signal(barrier, inc=1, device_id=peer_id, device_id_type=MESH))
    for q in range(2):
        first_e(q)[0].start()
        first_h(q)[0].start()
    for i in range(1, len(GROUPS)):
        group_e(i)[0].start()
        for cp, _ in group_h(i):
            cp.start()
    pl.semaphore_wait(barrier, 3 + z_count)

    for q in range(2):
        first_e(q)[1].start()
        first_h(q)[1].start()
    for cp in old_cols_out:
        cp.start()
    for i in range(1, len(GROUPS)):
        group_e(i)[1].start()
        for _, cp in group_h(i):
            cp.start()
    for cp in small_loads:
        cp.start()
    along_z(lambda peer_id: pl.semaphore_signal(token.at[0], inc=1, device_id=peer_id, device_id_type=MESH))

    col_acc[...] = jnp.zeros_like(col_acc)
    t_acc[...] = jnp.zeros_like(t_acc)
    rsum[...] = jnp.zeros_like(rsum)
    psum[...] = jnp.zeros_like(psum)

    def flip_e(k, half):
        at = pl.ds(pl.multiple_of(k * LANES, LANES), LANES)
        for j in range(half_of // LANES):
            cols = pl.ds(pl.multiple_of(half * half_of + j * LANES, LANES), LANES)
            strip = (both_e[0, at, cols] + both_e[1, at, cols]).T
            done = 0
            while done < LANES:
                block, row = divmod(LANES * j + done, COLS)
                size = min(LANES - done, COLS - row)
                sum_e[k, half, block // 2, block % 2, row:row + size, :] = strip[done:done + size, :]
                done += size

    def add_h(k, part):
        for a in range(2):
            for b in range(2):
                both_h[0, k, a, part, b] = both_h[0, k, a, part, b] + both_h[1, k, a, part, b]

    def combine_cores(k):
        flip_e(k, oy)
        one_e(k).start()
        add_h(k, ox)
        one_h(k).start()
        flip_e(k, y)
        add_h(k, x)

    def first_sum(k):
        one_e(k).wait_recv()
        in1_e[k, ox] = in1_e[k, ox] + sum_e[k, y, ox]
        two_e(k).start()
        in1_e[k, x] = in1_e[k, x] + sum_e[k, y, x]
        one_h(k).wait_recv()
        in1_h[k, oy] = in1_h[k, oy] + both_h[0, k, oy, x]
        two_h(k).start()
        in1_h[k, y] = in1_h[k, y] + both_h[0, k, y, x]

    def finish(k, q, i):
        two_e(k).wait_recv()
        for core in range(2):
            in2_e[k, core] = in2_e[k, core] + in1_e[k, x, core]
        two_h(k).wait_recv()
        for core in range(2):
            in2_h[k, core] = in2_h[k, core] + in1_h[k, y, core]
        for t, total in enumerate((in2_e, in2_h)):
            row_part = jnp.zeros((1, LANES), jnp.float32)
            for core in range(2):
                g = total[k, core]
                sq = g * g + EPS_ONE
                col_acc[t, core] = col_acc[t, core] + sq
                row_part = row_part + jnp.sum(sq, axis=0, keepdims=True)
            rp_own[q, 2 * t + i:2 * t + i + 1, :] = row_part

    def send_rows(q):
        for i in (2, 1, 0):
            row_msg(q, i).start()

    def send_swap(q):
        for cp in swap(q):
            cp.start()

    def new_rows(q):
        arrived(rp_in.at[q], rp_r.at[q % RING])
        block = c * PAIRS + q
        row_sq = (rp_own[q] + rp_in[q, 0]) + (rp_in[q, 1] + rp_in[q, 2])
        old = jnp.concatenate([old_rows[0, block], old_rows[1, block]], axis=0)
        row_new = BETA_TWO * old + (1.0 - BETA_TWO) * (row_sq / EMBED)
        rows[block] = row_new
        return row_new

    def row_stats(q):
        row_new = new_rows(q)
        rsum[...] = rsum[...] + row_new
        inv = 1.0 / row_new
        for t, total in enumerate((in2_e, in2_h)):
            for core in range(2):
                acc = t_acc[t, core]
                for i in range(2):
                    g = total[2 * q + i, core]
                    acc = acc + (g * g) * inv[2 * t + i:2 * t + i + 1, :]
                t_acc[t, core] = acc

    def scale_rows(block, get):
        factor = lax.rsqrt(rows[block])
        base = pl.multiple_of(block * (2 * LANES), 2 * LANES)
        for t, stage in enumerate((stage_e, stage_h)):
            for i in range(2):
                stage[:, pl.ds(base + i * LANES, LANES)] = get(t, i) * factor[2 * t + i:2 * t + i + 1, :]

    def scale_own(q):
        totals = (in2_e, in2_h)
        scale_rows(c * PAIRS + q, lambda t, i: totals[t][2 * q + i, c])

    def scale_peer(q):
        arrived(rows.at[oc * PAIRS + q], fw_r.at[q % RING])
        arrived(peer.at[q], swap_r.at[q % RING])
        scale_rows(oc * PAIRS + q, lambda t, i: peer[q, t, i])

    def param_sq(k):
        size = ROWS // CHUNKS * 2
        at = pl.ds(pl.multiple_of(k * size, size), size)
        for t, par in enumerate((par_e, par_h)):
            v = par[:, at]
            v = jnp.sum(v * v, axis=0, keepdims=True)
            for i in range(size // LANES):
                psum[t:t + 1, :] = psum[t:t + 1, :] + v[:, i * LANES:(i + 1) * LANES]

    for q in range(2):
        cols = pl.ds(pl.multiple_of((oy if q == 0 else y) * half_of, LANES), half_of)
        arrived(both_e.at[:, 0:LANES, cols], s0e_r.at[q])
        flip_e(0, oy if q == 0 else y)
        if q == 0:
            one_e(0).start()
        part = ox if q == 0 else x
        arrived(both_h.at[:, 0, :, part], s0h_r.at[q])
        add_h(0, part)
        if q == 0:
            one_h(0).start()
    def group_arrived(i):
        first, count = GROUPS[i]
        arrived(both_e.at[:, first * LANES:(first + count) * LANES, :], s0e_r.at[i + 1])
        arrived(both_h.at[:, first:first + count], s0h_r.at[i + 1])

    group_arrived(1)
    combine_cores(1)

    @pl.loop(0, CHUNKS)
    def _(k):
        for i in range(2, len(GROUPS)):
            @pl.when(k + AHEAD == GROUPS[i][0])
            def _():
                group_arrived(i)

        @pl.when(k + AHEAD < CHUNKS)
        def _():
            combine_cores(k + AHEAD)

        first_sum(k)
        pair = k // 2

        @pl.when(k == 1)
        def _():
            pl.semaphore_wait(token.at[0], z_count)
            along_z(lambda peer_id: pl.semaphore_signal(token.at[1], inc=1, device_id=peer_id, device_id_type=MESH))

        @pl.when(k == 2)
        def _():
            pl.semaphore_wait(token.at[1], z_count)

        @pl.when(k == 3)
        def _():
            arrived(par_e, in_sem.at[0])
            arrived(par_h, in_sem.at[1])
            arrived(old_rows, in_sem.at[2])

        @pl.when(k >= CHUNKS // 2)
        def _():
            param_sq(k - CHUNKS // 2)

        @pl.when((k >= 1) & (k % 2 == 1))
        def _():
            finish(k - 1, pair, 0)

        @pl.when((k >= 2) & (k % 2 == 0))
        def _():
            finish(k - 1, pair - 1, 1)
            send_rows(pair - 1)
            send_swap(pair - 1)

        @pl.when((k >= 6) & (k % 2 == 0))
        def _():
            scale_peer(pair - 3)

        @pl.when((k >= 4) & (k % 2 == 0))
        def _():
            row_stats(pair - 2)
            row_fwd(pair - 2).start()
            scale_own(pair - 2)

    lane = lax.broadcasted_iota(jnp.int32, (1, LANES), 1)
    diag = lax.broadcasted_iota(jnp.int32, (COLS, LANES), 0) == lax.broadcasted_iota(jnp.int32, (COLS, LANES), 1)

    def as_row(acc):
        col = jnp.sum(acc, axis=1, keepdims=True)
        return jnp.sum(jnp.where(diag, col, 0.0), axis=0, keepdims=True)

    def total_of(v):
        return jnp.sum(jnp.sum(v, axis=1, keepdims=True), axis=0, keepdims=True)

    row_stats(PAIRS - 2)
    row_fwd(PAIRS - 2).start()
    r_parts = [total_of(rsum[2 * t:2 * t + 2, :]) for t in range(2)]
    p_parts = [jnp.sum(psum[t:t + 1, :], axis=1, keepdims=True) for t in range(2)]
    for t in range(2):
        for core in range(2):
            m_own[core, 2 * t + 1:2 * t + 2, :] = as_row(t_acc[t, core])
    scale_own(PAIRS - 2)

    finish(CHUNKS - 1, PAIRS - 1, 1)
    send_rows(PAIRS - 1)
    for t in range(2):
        for core in range(2):
            row = as_row(col_acc[t, core])
            m_own[core, 2 * t:2 * t + 1, :] = jnp.where(lane == COLS, r_parts[t], jnp.where(lane == COLS + 1, p_parts[t], row))

    columns = [(dz, fc) for dz in range(4) for fc in range(2) if dz + fc]

    def column_msg(i):
        dz, fc = columns[i]
        slot = columns.index(((4 - dz) % 4, fc))
        return remote(m_own, m_in.at[slot], send.at[9], last_r.at[0], column_id(dz, fc))

    for i in (3, 4, 1, 2, 5, 6, 0):
        column_msg(i).start()
    send_swap(PAIRS - 1)

    row_new = new_rows(PAIRS - 1)
    row_fwd(PAIRS - 1).start()
    inv = 1.0 / row_new
    t_last, r_last = [], []
    for t, sums in enumerate((in2_e, in2_h)):
        r_last.append(total_of(row_new[2 * t:2 * t + 2, :]))
        for core in range(2):
            acc = jnp.zeros((COLS, LANES), jnp.float32)
            for i in range(2):
                g = sums[2 * (PAIRS - 1) + i, core]
                acc = acc + (g * g) * inv[2 * t + i:2 * t + i + 1, :]
            t_last.append(as_row(acc))
    scale_own(PAIRS - 1)
    arrived(old_cols.at[:, c], in_sem.at[3])
    arrived(old_cols.at[:, oc], in_sem.at[4])
    arrived(m_in, last_r.at[0])

    total = m_own[...]
    for i in range(len(columns)):
        total = total + m_in[i]
    m_sum[...] = total
    message = jnp.zeros((1, LANES), jnp.float32)
    r_firsts = []
    for t in range(2):
        cols = total[0, 2 * t:2 * t + 1, :]
        r_first = jnp.sum(jnp.where(lane == COLS, cols, 0.0), axis=1, keepdims=True) / VOCAB
        p_col = jnp.sum(jnp.where(lane == COLS + 1, cols, 0.0), axis=1, keepdims=True)
        u_sq = jnp.zeros((1, COLS), jnp.float32)
        for core in range(2):
            col_new = BETA_TWO * old_cols[t, core] + (1.0 - BETA_TWO) * (total[core, 2 * t:2 * t + 1, :COLS] / VOCAB)
            t_sum = 0.125 * total[core, 2 * t + 1:2 * t + 2, :COLS] + t_last[2 * t + core][:, :COLS]
            u_sq = u_sq + t_sum * (r_first / col_new)
        u_sq = jnp.sum(u_sq, axis=1, keepdims=True)
        message = jnp.where(lane == 3 * t, u_sq, jnp.where(lane == 3 * t + 1, 0.125 * p_col, message))
        message = jnp.where(lane == 3 * t + 2, 0.03125 * r_first + 0.25 * r_last[t] / VOCAB, message)
        r_firsts.append(r_first)
    s_own[...] = message

    others = [(dz, fy, fx, fc) for dz in range(4) for fy in range(2) for fx in range(2) for fc in range(2) if dz + fy + fx + fc]

    def scalar_msg(i):
        dz, fy, fx, fc = others[i]
        slot = others.index(((4 - dz) % 4, fy, fx, fc))
        return remote(s_own, s_in.at[slot], send.at[10], last_r.at[1], ((model + dz) % 4, plane_id(fy, fx, fc)[1]))

    for i in sorted(range(len(others)), key=lambda i: -sum(others[i][1:3])):
        scalar_msg(i).start()

    factor_cols = []
    for t, c_out in enumerate((emb_cols_out, head_cols_out)):
        cols = m_sum[c, 2 * t:2 * t + 1, :]
        col_new = BETA_TWO * old_cols[t, c] + (1.0 - BETA_TWO) * (cols[:, :COLS] / VOCAB)
        c_out[...] = col_new
        factor_cols.append(jnp.sum(jnp.where(diag[:, :COLS], lax.rsqrt(col_new), 0.0), axis=1, keepdims=True))

    @pl.loop(PAIRS - 3, PAIRS)
    def _(q):
        scale_peer(q)

    emb_rows_out[...] = rows[:, :2, :]
    head_rows_out[...] = rows[:, 2:, :]
    arrived(both_e.at[0], send.at[0])
    arrived(both_h.at[0], send.at[1])
    arrived(in1_e, send.at[2])
    arrived(in1_h, send.at[3])
    arrived(in2_e, send.at[4])
    arrived(in2_h, send.at[5])
    arrived(peer, send.at[6])
    arrived(rp_in, send.at[7])
    arrived(rows.at[0:PAIRS], send.at[8])
    arrived(m_in, send.at[9])
    arrived(old_cols.at[:, c], send.at[11])
    arrived(s_in, last_r.at[1])
    message = s_own[...] + jnp.sum(s_in[...], axis=0)
    count = float(VOCAB * EMBED)
    for t in range(2):
        u_sq, p_sq, r_mean = [jnp.sum(jnp.where(lane == 3 * t + i, message, 0.0), axis=1, keepdims=True) for i in range(3)]
        u_rms = jnp.sqrt(u_sq * (r_mean / r_firsts[t]) / count)
        p_rms = jnp.sqrt(p_sq / count)
        step = LEARN_RATE * jnp.maximum(SCALE_FLOOR, p_rms) / jnp.maximum(1.0, u_rms / CLIP_LIMIT)
        scale_out[t] = jnp.broadcast_to(factor_cols[t] * (step * jnp.sqrt(r_mean)), (COLS, LANES))
    arrived(s_in, send.at[10])


def update_kernel(emb_g, head_g, emb_p, head_p, emb_rows, head_rows, emb_cols, head_cols, scale,
                  emb_new, head_new, emb_rows_new, head_rows_new, emb_cols_new, head_cols_new, emb_half, head_half,
                  new_buf, half_buf, small_sem, big_sem):
    small = [pltpu.make_async_copy(src, dst, small_sem.at[i]) for i, (src, dst) in enumerate(
        ((emb_rows, emb_rows_new), (head_rows, head_rows_new), (emb_cols, emb_cols_new), (head_cols, head_cols_new)))]
    for cp in small:
        cp.start()
    size = COLS // PARTS
    for i in range(PARTS):
        part = slice(i * size, (i + 1) * size)
        for t, (p, g, new, half) in enumerate(((emb_p, emb_g, emb_new, emb_half), (head_p, head_g, head_new, head_half))):
            value = p[part, :] - g[part, :] * scale[t, part, 0:1]
            new_buf[t, part, :] = value
            half_buf[t, part, :] = value.astype(jnp.bfloat16)
            pltpu.make_async_copy(new_buf.at[t, part, :], new.at[part, :], big_sem.at[0]).start()
            pltpu.make_async_copy(half_buf.at[t, part, :], half.at[part, :], big_sem.at[1]).start()
    for cp in small:
        cp.wait()
    pltpu.make_async_copy(new_buf, new_buf, big_sem.at[0]).wait()
    pltpu.make_async_copy(half_buf, half_buf, big_sem.at[1]).wait()


def local_step(emb_p, head_p, emb_g, head_g, emb_r, emb_c, head_r, head_c):
    f32 = jnp.float32
    n = CHUNKS
    dma = pltpu.SemaphoreType.DMA
    hbm = pl.BlockSpec(memory_space=pltpu.HBM)
    vmem = pl.BlockSpec(memory_space=pltpu.VMEM)
    rows_shape = (BLOCKS, 2, LANES)
    table = jax.ShapeDtypeStruct((COLS, ROWS), f32)
    half = jax.ShapeDtypeStruct((COLS, ROWS), jnp.bfloat16)
    emb_p = emb_p.T
    shapes = [(2, ROWS // 2, EMBED), (n, 2, 2, 2, COLS, LANES), (2, n, 2, 2, 2, COLS, LANES)]
    shapes += [(n, 2, 2, COLS, LANES)] * 2 + [(n, 2, COLS, LANES)] * 2 + [(PAIRS, 2, 2, COLS, LANES)]
    shapes += [(BLOCKS, 4, LANES), (2, *rows_shape), (2, 2, 1, COLS)]
    shapes += [(PAIRS, 4, LANES), (PAIRS, 3, 4, LANES)]
    shapes += [(2, 2, COLS, LANES)] * 2 + [(4, LANES), (2, LANES)]
    shapes += [(2, 4, LANES), (7, 2, 4, LANES), (2, 4, LANES), (1, LANES), (31, 1, LANES)]
    scratch = [pltpu.VMEM(shape, f32) for shape in shapes]
    scratch += [dma((len(GROUPS) + 1,))] * 2 + [dma((DEEP,))] * 2 + [dma((RING,))] * 5
    scratch += [dma((12,)), dma((2,)), dma((5,)), pltpu.SemaphoreType.REGULAR((2,))]
    kept = [pltpu.VMEM((COLS, ROWS), f32)] * 4 + [pltpu.VMEM(rows_shape, f32)] * 2 + [pltpu.VMEM((1, COLS), f32)] * 2
    kept.append(pltpu.VMEM((2, COLS, LANES), f32))
    state = pl.pallas_call(
        exchange_kernel,
        out_shape=tuple(kept),
        in_specs=[hbm] * 8,
        out_specs=(vmem,) * 9,
        scratch_shapes=scratch,
        compiler_params=pltpu.CompilerParams(collective_id=0, has_side_effects=True, vmem_limit_bytes=60_000_000),
        name="exchange",
    )(emb_g.reshape(ROWS, EMBED), head_g.reshape(2, 2, 2, COLS, ROWS), emb_p, head_p,
      emb_r.reshape(rows_shape), head_r.reshape(rows_shape), emb_c.reshape(1, COLS), head_c.reshape(1, COLS))

    outs = pl.pallas_call(
        update_kernel,
        out_shape=(table, table, jax.ShapeDtypeStruct(rows_shape, f32), jax.ShapeDtypeStruct(rows_shape, f32),
                   jax.ShapeDtypeStruct((1, COLS), f32), jax.ShapeDtypeStruct((1, COLS), f32), half, half),
        in_specs=[vmem] * 9,
        out_specs=(hbm,) * 8,
        scratch_shapes=[pltpu.VMEM((2, COLS, ROWS), f32), pltpu.VMEM((2, COLS, ROWS), jnp.bfloat16),
                        dma((4,)), dma((2,))],
        compiler_params=pltpu.CompilerParams(vmem_limit_bytes=16 * 2 ** 20),
        name="update",
    )(*state)
    emb_new, head_new, emb_rn, head_rn, emb_cn, head_cn, emb_half, head_half = outs
    return (emb_new.T, head_new, emb_rn.reshape(ROWS), emb_cn.reshape(COLS), head_rn.reshape(ROWS),
            head_cn.reshape(COLS), emb_half.T, head_half)


def solution(mesh):
    arg_specs = (P("model", "data"), P("data", "model"), P("data", "model", None), P("data", None, "model"),
                 P("model"), P("data"), P("model"), P("data"))
    result_specs = (P("model", "data"), P("data", "model"), P("model"), P("data"), P("model"), P("data"),
                    P("model", "data"), P("data", "model"))
    mapped = jax.shard_map(local_step, mesh=mesh, in_specs=arg_specs, out_specs=result_specs, check_vma=False)

    def update_tables(emb_param, head_param, emb_grad, head_grad, emb_row, emb_col, head_row, head_col):
        return mapped(emb_param, head_param, emb_grad, head_grad, emb_row, emb_col, head_row, head_col)

    return update_tables
```

```python
import functools

import jax
import jax.numpy as jnp
from jax import lax
from jax.experimental import pallas as pl
from jax.experimental.pallas import tpu as pltpu
from jax.sharding import PartitionSpec as P

TRAIN_STEP = 10
DECAY_EXP = 0.8
EPS_ONE = 1e-30
CLIP_LIMIT = 1.0
SCALE_FLOOR = 1e-3
LEARN_RATE = float(TRAIN_STEP) ** -0.5
BETA_TWO = 1.0 - float(TRAIN_STEP) ** -DECAY_EXP

VOCAB = 16384
EMBED = 768
ROWS = VOCAB // 4
COLS = EMBED // 8
LANES = 128
CHUNKS = ROWS // 2 // LANES
GROUPS = ((0, 1), (1, 1), (2, 2), (4, 12))
PAIRS = CHUNKS // 2
BLOCKS = 2 * PAIRS
AHEAD = 2
RING = 6
SHORT = 4
PARTS = 3
MESH = pl.DeviceIdType.MESH
PLANE = ((0, 1), (1, 0), (1, 1))


def exchange_kernel(emb_ref, head_ref, emb_p_ref, head_p_ref, emb_r_ref, head_r_ref, emb_c_ref, head_c_ref,
                    stage_e, stage_h, par_e, par_h, emb_rows_out, head_rows_out, emb_cols_out, head_cols_out, scale_out,
                    both_e, sum_e, both_h, in1, in2, peer,
                    rows, old_rows, old_cols, rp_own, rp_in, col_acc, t_acc, rsum, psum, m_own, m_in, m_sum, s_own, s_in,
                    s0e_r, s0h_r, s1_r, s2_r, swap_r, rp_r, fw_r, send, last_r, in_sem, token):
    model = lax.axis_index("model")
    data = lax.axis_index("data")
    c = data % 2
    x = (data // 2) % 2
    y = data // 4
    oc, ox, oy = 1 - c, 1 - x, 1 - y

    def plane_id(fy, fx, fc):
        step = fy * (4 - 8 * y) + fx * (2 - 4 * x) + fc * (1 - 2 * c)
        return (model, data + step)

    def column_id(dz, fc):
        return ((model + dz) % 4, data + fc * (1 - 2 * c))

    core_peer, x_peer, y_peer = plane_id(0, 0, 1), plane_id(0, 1, 0), plane_id(1, 0, 0)

    def remote(src, dst, send_sem, recv_sem, peer_id):
        return pltpu.make_async_remote_copy(src_ref=src, dst_ref=dst, send_sem=send_sem, recv_sem=recv_sem,
                                            device_id=peer_id, device_id_type=MESH)

    def arrived(ref, sem):
        pltpu.make_async_copy(ref, ref, sem).wait()

    def vocab_at(core, first, count):
        return pl.ds(pl.multiple_of(core * (ROWS // 2) + first * LANES, LANES), count * LANES)

    half_of = 4 * COLS

    def first_e(q):
        cols = pl.ds(pl.multiple_of((oy if q == 0 else y) * half_of, LANES), half_of)
        return (pltpu.make_async_copy(emb_ref.at[vocab_at(c, 0, 1), cols], both_e.at[0, 0:LANES, cols], s0e_r.at[q]),
                remote(emb_ref.at[vocab_at(oc, 0, 1), cols], both_e.at[1, 0:LANES, cols], send.at[0], s0e_r.at[q], core_peer))

    def first_h(q):
        part = ox if q == 0 else x
        return (pltpu.make_async_copy(head_ref.at[:, part, :, :, vocab_at(c, 0, 1)], both_h.at[0, 0, :, part], s0h_r.at[q]),
                remote(head_ref.at[:, part, :, :, vocab_at(oc, 0, 1)], both_h.at[1, 0, :, part], send.at[1], s0h_r.at[q], core_peer))

    def group_e(i):
        first, count = GROUPS[i]
        at = slice(first * LANES, (first + count) * LANES)
        return (pltpu.make_async_copy(emb_ref.at[vocab_at(c, first, count), :], both_e.at[0, at, :], s0e_r.at[i + 1]),
                remote(emb_ref.at[vocab_at(oc, first, count), :], both_e.at[1, at, :], send.at[0], s0e_r.at[i + 1], core_peer))

    def group_h(i):
        first, count = GROUPS[i]
        pairs = []
        for j in range(first, first + count):
            pairs.append((pltpu.make_async_copy(head_ref.at[:, :, :, :, vocab_at(c, j, 1)], both_h.at[0, j], s0h_r.at[i + 1]),
                          remote(head_ref.at[:, :, :, :, vocab_at(oc, j, 1)], both_h.at[1, j], send.at[1], s0h_r.at[i + 1],
                                 core_peer)))
        return pairs

    def one_e(k):
        return remote(sum_e.at[k, oy], in1.at[k, 0], send.at[2], s1_r.at[k % RING], y_peer)

    def one_h(k):
        return remote(both_h.at[0, k, :, ox], in1.at[k, 1], send.at[2], s1_r.at[k % RING], x_peer)

    def two_e(k):
        return remote(in1.at[k, 0, ox], in2.at[k, 0], send.at[3], s2_r.at[k % RING], x_peer)

    def two_h(k):
        return remote(in1.at[k, 1, oy], in2.at[k, 1], send.at[3], s2_r.at[k % RING], y_peer)

    def swap(q):
        return [remote(in2.at[pl.ds(2 * q, 2), t, oc], peer.at[q, t], send.at[4], swap_r.at[q % SHORT], core_peer)
                for t in range(2)]

    def row_msg(q, i):
        fy, fx = PLANE[i]
        return remote(rp_own.at[q], rp_in.at[q, i], send.at[5], rp_r.at[q % SHORT], plane_id(fy, fx, 0))

    def row_fwd(q):
        return remote(rows.at[c * PAIRS + q], rows.at[c * PAIRS + q], send.at[6], fw_r.at[q % SHORT], core_peer)

    small_loads = [pltpu.make_async_copy(src, dst, in_sem.at[i]) for i, (src, dst) in (
        (0, (emb_p_ref, par_e)), (1, (head_p_ref, par_h)), (2, (emb_r_ref, old_rows.at[0])), (2, (head_r_ref, old_rows.at[1])),
        (3, (emb_c_ref, old_cols.at[0, c])), (3, (head_c_ref, old_cols.at[1, c])))]
    old_cols_out = [remote(src, old_cols.at[t, c], send.at[8], in_sem.at[4], core_peer)
                    for t, src in enumerate((emb_c_ref, head_c_ref))]

    barrier = pltpu.get_barrier_semaphore()
    above, below = column_id(1, 0), column_id(3, 0)
    for peer_id in (core_peer, x_peer, y_peer):
        pl.semaphore_signal(barrier, inc=1, device_id=peer_id, device_id_type=MESH)

    z_count = 1 + model * (3 - model) // 2

    def along_z(act):
        @pl.when(model < 3)
        def _():
            act(above)

        @pl.when(model > 0)
        def _():
            act(below)

    along_z(lambda peer_id: pl.semaphore_signal(barrier, inc=1, device_id=peer_id, device_id_type=MESH))
    for q in range(2):
        first_e(q)[0].start()
        first_h(q)[0].start()
    for i in range(1, len(GROUPS)):
        group_e(i)[0].start()
        for cp, _ in group_h(i):
            cp.start()
    pl.semaphore_wait(barrier, 3 + z_count)

    for q in range(2):
        first_e(q)[1].start()
        first_h(q)[1].start()
    for cp in old_cols_out:
        cp.start()
    for i in range(1, len(GROUPS)):
        group_e(i)[1].start()
        for _, cp in group_h(i):
            cp.start()
    for cp in small_loads:
        cp.start()
    along_z(lambda peer_id: pl.semaphore_signal(token.at[0], inc=1, device_id=peer_id, device_id_type=MESH))

    col_acc[...] = jnp.zeros_like(col_acc)
    t_acc[...] = jnp.zeros_like(t_acc)
    rsum[...] = jnp.zeros_like(rsum)
    psum[...] = jnp.zeros_like(psum)

    def flip_e(k, half):
        at = pl.ds(pl.multiple_of(k * LANES, LANES), LANES)
        for j in range(half_of // LANES):
            cols = pl.ds(pl.multiple_of(half * half_of + j * LANES, LANES), LANES)
            strip = (both_e[0, at, cols] + both_e[1, at, cols]).T
            done = 0
            while done < LANES:
                block, row = divmod(LANES * j + done, COLS)
                size = min(LANES - done, COLS - row)
                sum_e[k, half, block // 2, block % 2, row:row + size, :] = strip[done:done + size, :]
                done += size

    def add_h(k, part):
        for a in range(2):
            for b in range(2):
                both_h[0, k, a, part, b] = both_h[0, k, a, part, b] + both_h[1, k, a, part, b]

    def combine_cores(k):
        flip_e(k, oy)
        one_e(k).start()
        add_h(k, ox)
        one_h(k).start()
        flip_e(k, y)
        add_h(k, x)

    def first_sum(k):
        arrived(in1.at[k], s1_r.at[k % RING])
        in1[k, 0, ox] = in1[k, 0, ox] + sum_e[k, y, ox]
        two_e(k).start()
        in1[k, 1, oy] = in1[k, 1, oy] + both_h[0, k, oy, x]
        two_h(k).start()
        in1[k, 0, x] = in1[k, 0, x] + sum_e[k, y, x]
        in1[k, 1, y] = in1[k, 1, y] + both_h[0, k, y, x]

    def finish(k, q, i):
        arrived(in2.at[k], s2_r.at[k % RING])
        for t, mine in enumerate((x, y)):
            for core in range(2):
                in2[k, t, core] = in2[k, t, core] + in1[k, t, mine, core]
        for t in range(2):
            row_part = jnp.zeros((1, LANES), jnp.float32)
            for core in range(2):
                g = in2[k, t, core]
                sq = g * g + EPS_ONE
                col_acc[t, core] = col_acc[t, core] + sq
                row_part = row_part + jnp.sum(sq, axis=0, keepdims=True)
            rp_own[q, 2 * t + i:2 * t + i + 1, :] = row_part

    def send_rows(q):
        for i in (2, 1, 0):
            row_msg(q, i).start()

    def send_swap(q):
        for cp in swap(q):
            cp.start()

    def new_rows(q):
        arrived(rp_in.at[q], rp_r.at[q % SHORT])
        block = c * PAIRS + q
        row_sq = (rp_own[q] + rp_in[q, 0]) + (rp_in[q, 1] + rp_in[q, 2])
        old = jnp.concatenate([old_rows[0, block], old_rows[1, block]], axis=0)
        row_new = BETA_TWO * old + (1.0 - BETA_TWO) * (row_sq / EMBED)
        rows[block] = row_new
        return row_new

    def row_stats(q):
        row_new = new_rows(q)
        rsum[...] = rsum[...] + row_new
        inv = 1.0 / row_new
        for t in range(2):
            for core in range(2):
                acc = t_acc[t, core]
                for i in range(2):
                    g = in2[2 * q + i, t, core]
                    acc = acc + (g * g) * inv[2 * t + i:2 * t + i + 1, :]
                t_acc[t, core] = acc

    def scale_rows(block, get):
        factor = lax.rsqrt(rows[block])
        base = pl.multiple_of(block * (2 * LANES), 2 * LANES)
        for t, stage in enumerate((stage_e, stage_h)):
            for i in range(2):
                stage[:, pl.ds(base + i * LANES, LANES)] = get(t, i) * factor[2 * t + i:2 * t + i + 1, :]

    def scale_own(q):
        scale_rows(c * PAIRS + q, lambda t, i: in2[2 * q + i, t, c])

    def scale_peer(q):
        arrived(rows.at[oc * PAIRS + q], fw_r.at[q % SHORT])
        arrived(peer.at[q], swap_r.at[q % SHORT])
        scale_rows(oc * PAIRS + q, lambda t, i: peer[q, t, i])

    def param_sq(k):
        size = ROWS // CHUNKS * 2
        at = pl.ds(pl.multiple_of(k * size, size), size)
        for t, par in enumerate((par_e, par_h)):
            v = par[:, at]
            v = jnp.sum(v * v, axis=0, keepdims=True)
            for i in range(size // LANES):
                psum[t:t + 1, :] = psum[t:t + 1, :] + v[:, i * LANES:(i + 1) * LANES]

    for q in range(2):
        cols = pl.ds(pl.multiple_of((oy if q == 0 else y) * half_of, LANES), half_of)
        arrived(both_e.at[:, 0:LANES, cols], s0e_r.at[q])
        flip_e(0, oy if q == 0 else y)
        if q == 0:
            @pl.when(c == 0)
            def _():
                one_e(0).start()

        part = ox if q == 0 else x
        arrived(both_h.at[:, 0, :, part], s0h_r.at[q])
        add_h(0, part)
        if q == 0:
            @pl.when(c == 0)
            def _():
                one_h(0).start()

    def group_arrived(i):
        first, count = GROUPS[i]
        arrived(both_e.at[:, first * LANES:(first + count) * LANES, :], s0e_r.at[i + 1])
        arrived(both_h.at[:, first:first + count], s0h_r.at[i + 1])

    group_arrived(1)

    @pl.when(c == 1)
    def _():
        one_e(0).start()
        one_h(0).start()

    combine_cores(1)

    @pl.loop(0, CHUNKS)
    def _(k):
        for i in range(2, len(GROUPS)):
            @pl.when(k + AHEAD == GROUPS[i][0])
            def _():
                group_arrived(i)

        @pl.when(k + AHEAD < CHUNKS)
        def _():
            combine_cores(k + AHEAD)

        first_sum(k)
        pair = k // 2

        @pl.when(k == 1)
        def _():
            pl.semaphore_wait(token.at[0], z_count)
            along_z(lambda peer_id: pl.semaphore_signal(token.at[1], inc=1, device_id=peer_id, device_id_type=MESH))

        @pl.when(k == 2)
        def _():
            pl.semaphore_wait(token.at[1], z_count)

        @pl.when(k == 3)
        def _():
            arrived(par_e, in_sem.at[0])
            arrived(par_h, in_sem.at[1])
            arrived(old_rows, in_sem.at[2])

        @pl.when(k >= CHUNKS // 2)
        def _():
            param_sq(k - CHUNKS // 2)

        @pl.when((k >= 2) & (k % 2 == 0))
        def _():
            finish(k - 2, pair - 1, 0)

        @pl.when((k >= 3) & (k % 2 == 1))
        def _():
            finish(k - 2, pair - 1, 1)
            send_rows(pair - 1)
            send_swap(pair - 1)

        @pl.when((k >= 7) & (k % 2 == 1))
        def _():
            scale_peer(pair - 3)

        @pl.when((k >= 5) & (k % 2 == 1))
        def _():
            row_stats(pair - 2)
            row_fwd(pair - 2).start()
            scale_own(pair - 2)

    lane = lax.broadcasted_iota(jnp.int32, (1, LANES), 1)
    diag = lax.broadcasted_iota(jnp.int32, (COLS, LANES), 0) == lax.broadcasted_iota(jnp.int32, (COLS, LANES), 1)

    def as_row(acc):
        col = jnp.sum(acc, axis=1, keepdims=True)
        return jnp.sum(jnp.where(diag, col, 0.0), axis=0, keepdims=True)

    def total_of(v):
        return jnp.sum(jnp.sum(v, axis=0, keepdims=True), axis=1, keepdims=True)

    finish(CHUNKS - 2, PAIRS - 1, 0)
    row_stats(PAIRS - 2)
    row_fwd(PAIRS - 2).start()
    r_parts = [total_of(rsum[2 * t:2 * t + 2, :]) for t in range(2)]
    p_parts = [jnp.sum(psum[t:t + 1, :], axis=1, keepdims=True) for t in range(2)]
    for t in range(2):
        for core in range(2):
            m_own[core, 2 * t + 1:2 * t + 2, :] = as_row(t_acc[t, core])
    scale_own(PAIRS - 2)

    finish(CHUNKS - 1, PAIRS - 1, 1)
    send_rows(PAIRS - 1)
    for t in range(2):
        for core in range(2):
            row = as_row(col_acc[t, core])
            m_own[core, 2 * t:2 * t + 1, :] = jnp.where(lane == COLS, r_parts[t], jnp.where(lane == COLS + 1, p_parts[t], row))

    columns = [(dz, fc) for dz in range(4) for fc in range(2) if dz + fc]

    def column_msg(i):
        dz, fc = columns[i]
        slot = columns.index(((4 - dz) % 4, fc))
        return remote(m_own, m_in.at[slot], send.at[7], last_r.at[0], column_id(dz, fc))

    for i in (3, 4, 1, 2, 5, 6, 0):
        column_msg(i).start()
    send_swap(PAIRS - 1)

    arrived(old_cols.at[:, c], in_sem.at[3])
    arrived(old_cols.at[:, oc], in_sem.at[4])
    arrived(m_in, last_r.at[0])
    total = m_own[...]
    for i in range(len(columns)):
        total = total + m_in[i]
    m_sum[...] = total
    r_firsts, p_cols, u_firsts, weights = [], [], [], []
    for t in range(2):
        cols = total[0, 2 * t:2 * t + 1, :]
        r_first = jnp.sum(jnp.where(lane == COLS, cols, 0.0), axis=1, keepdims=True) / VOCAB
        u_first = jnp.zeros((1, COLS), jnp.float32)
        for core in range(2):
            col_new = BETA_TWO * old_cols[t, core] + (1.0 - BETA_TWO) * (total[core, 2 * t:2 * t + 1, :COLS] / VOCAB)
            weight = r_first / col_new
            u_first = u_first + total[core, 2 * t + 1:2 * t + 2, :COLS] * weight
            weights.append(jnp.sum(jnp.where(diag[:, :COLS], weight, 0.0), axis=1, keepdims=True))
        r_firsts.append(r_first)
        p_cols.append(jnp.sum(jnp.where(lane == COLS + 1, cols, 0.0), axis=1, keepdims=True))
        u_firsts.append(0.125 * jnp.sum(u_first, axis=1, keepdims=True))

    row_new = new_rows(PAIRS - 1)
    inv = 1.0 / row_new
    message = jnp.zeros((1, LANES), jnp.float32)
    for t in range(2):
        acc = jnp.zeros((COLS, LANES), jnp.float32)
        for core in range(2):
            for i in range(2):
                g = in2[2 * (PAIRS - 1) + i, t, core]
                acc = acc + (g * g) * inv[2 * t + i:2 * t + i + 1, :] * weights[2 * t + core]
        r_mean = 0.03125 * r_firsts[t] + 0.25 * total_of(row_new[2 * t:2 * t + 2, :]) / VOCAB
        for i, value in enumerate((u_firsts[t] + total_of(acc), 0.125 * p_cols[t], r_mean)):
            message = jnp.where(lane == 3 * t + i, value, message)
    s_own[...] = message

    others = [(dz, fy, fx, fc) for dz in range(4) for fy in range(2) for fx in range(2) for fc in range(2) if dz + fy + fx + fc]

    def scalar_msg(i):
        dz, fy, fx, fc = others[i]
        slot = others.index(((4 - dz) % 4, fy, fx, fc))
        return remote(s_own, s_in.at[slot], send.at[9], last_r.at[1], ((model + dz) % 4, plane_id(fy, fx, fc)[1]))

    for i in sorted(range(len(others)), key=lambda i: -sum(others[i][1:3])):
        scalar_msg(i).start()
    row_fwd(PAIRS - 1).start()
    scale_own(PAIRS - 1)

    factor_cols = []
    for t, c_out in enumerate((emb_cols_out, head_cols_out)):
        cols = m_sum[c, 2 * t:2 * t + 1, :]
        col_new = BETA_TWO * old_cols[t, c] + (1.0 - BETA_TWO) * (cols[:, :COLS] / VOCAB)
        c_out[...] = col_new
        factor_cols.append(jnp.sum(jnp.where(diag[:, :COLS], lax.rsqrt(col_new), 0.0), axis=1, keepdims=True))

    @pl.loop(PAIRS - 3, PAIRS)
    def _(q):
        scale_peer(q)

    emb_rows_out[...] = rows[:, :2, :]
    head_rows_out[...] = rows[:, 2:, :]
    arrived(both_e.at[0], send.at[0])
    arrived(both_h.at[0], send.at[1])
    arrived(in1, send.at[2])
    arrived(in2, send.at[3])
    arrived(peer, send.at[4])
    arrived(rp_in, send.at[5])
    arrived(rows.at[0:PAIRS], send.at[6])
    arrived(m_in, send.at[7])
    arrived(old_cols.at[:, c], send.at[8])
    arrived(s_in, last_r.at[1])
    message = s_own[...] + jnp.sum(s_in[...], axis=0)
    count = float(VOCAB * EMBED)
    for t in range(2):
        u_sq, p_sq, r_mean = [jnp.sum(jnp.where(lane == 3 * t + i, message, 0.0), axis=1, keepdims=True) for i in range(3)]
        u_rms = jnp.sqrt(u_sq * (r_mean / r_firsts[t]) / count)
        p_rms = jnp.sqrt(p_sq / count)
        step = LEARN_RATE * jnp.maximum(SCALE_FLOOR, p_rms) / jnp.maximum(1.0, u_rms / CLIP_LIMIT)
        scale_out[t] = jnp.broadcast_to(factor_cols[t] * (step * jnp.sqrt(r_mean)), (COLS, LANES))
    arrived(s_in, send.at[9])


def update_kernel(emb_g, head_g, emb_p, head_p, emb_rows, head_rows, emb_cols, head_cols, scale,
                  emb_new, head_new, emb_rows_new, head_rows_new, emb_cols_new, head_cols_new, emb_half, head_half,
                  new_buf, half_buf, small_sem, big_sem):
    small = [pltpu.make_async_copy(src, dst, small_sem.at[i]) for i, (src, dst) in enumerate(
        ((emb_rows, emb_rows_new), (head_rows, head_rows_new), (emb_cols, emb_cols_new), (head_cols, head_cols_new)))]
    for cp in small:
        cp.start()
    size = COLS // PARTS
    for i in range(PARTS):
        part = slice(i * size, (i + 1) * size)
        for t, (p, g, new, half) in enumerate(((emb_p, emb_g, emb_new, emb_half), (head_p, head_g, head_new, head_half))):
            value = p[part, :] - g[part, :] * scale[t, part, 0:1]
            new_buf[t, part, :] = value
            half_buf[t, part, :] = value.astype(jnp.bfloat16)
            pltpu.make_async_copy(new_buf.at[t, part, :], new.at[part, :], big_sem.at[0]).start()
            pltpu.make_async_copy(half_buf.at[t, part, :], half.at[part, :], big_sem.at[1]).start()
    for cp in small:
        cp.wait()
    pltpu.make_async_copy(new_buf, new_buf, big_sem.at[0]).wait()
    pltpu.make_async_copy(half_buf, half_buf, big_sem.at[1]).wait()


def local_step(emb_p, head_p, emb_g, head_g, emb_r, emb_c, head_r, head_c):
    f32 = jnp.float32
    n = CHUNKS
    dma = pltpu.SemaphoreType.DMA
    hbm = pl.BlockSpec(memory_space=pltpu.HBM)
    vmem = pl.BlockSpec(memory_space=pltpu.VMEM)
    rows_shape = (BLOCKS, 2, LANES)
    table = jax.ShapeDtypeStruct((COLS, ROWS), f32)
    half = jax.ShapeDtypeStruct((COLS, ROWS), jnp.bfloat16)
    emb_p = emb_p.T
    shapes = [(2, ROWS // 2, EMBED), (n, 2, 2, 2, COLS, LANES), (2, n, 2, 2, 2, COLS, LANES)]
    shapes += [(n, 2, 2, 2, COLS, LANES), (n, 2, 2, COLS, LANES), (PAIRS, 2, 2, COLS, LANES)]
    shapes += [(BLOCKS, 4, LANES), (2, *rows_shape), (2, 2, 1, COLS)]
    shapes += [(PAIRS, 4, LANES), (PAIRS, 3, 4, LANES)]
    shapes += [(2, 2, COLS, LANES)] * 2 + [(4, LANES), (2, LANES)]
    shapes += [(2, 4, LANES), (7, 2, 4, LANES), (2, 4, LANES), (1, LANES), (31, 1, LANES)]
    scratch = [pltpu.VMEM(shape, f32) for shape in shapes]
    scratch += [dma((len(GROUPS) + 1,))] * 2 + [dma((RING,))] * 2 + [dma((SHORT,))] * 3
    scratch += [dma((10,)), dma((2,)), dma((5,)), pltpu.SemaphoreType.REGULAR((2,))]
    kept = [pltpu.VMEM((COLS, ROWS), f32)] * 4 + [pltpu.VMEM(rows_shape, f32)] * 2 + [pltpu.VMEM((1, COLS), f32)] * 2
    kept.append(pltpu.VMEM((2, COLS, LANES), f32))
    state = pl.pallas_call(
        exchange_kernel,
        out_shape=tuple(kept),
        in_specs=[hbm] * 8,
        out_specs=(vmem,) * 9,
        scratch_shapes=scratch,
        compiler_params=pltpu.CompilerParams(collective_id=0, has_side_effects=True, vmem_limit_bytes=60_000_000),
        name="exchange",
    )(emb_g.reshape(ROWS, EMBED), head_g.reshape(2, 2, 2, COLS, ROWS), emb_p, head_p,
      emb_r.reshape(rows_shape), head_r.reshape(rows_shape), emb_c.reshape(1, COLS), head_c.reshape(1, COLS))

    outs = pl.pallas_call(
        update_kernel,
        out_shape=(table, table, jax.ShapeDtypeStruct(rows_shape, f32), jax.ShapeDtypeStruct(rows_shape, f32),
                   jax.ShapeDtypeStruct((1, COLS), f32), jax.ShapeDtypeStruct((1, COLS), f32), half, half),
        in_specs=[vmem] * 9,
        out_specs=(hbm,) * 8,
        scratch_shapes=[pltpu.VMEM((2, COLS, ROWS), f32), pltpu.VMEM((2, COLS, ROWS), jnp.bfloat16),
                        dma((4,)), dma((2,))],
        compiler_params=pltpu.CompilerParams(vmem_limit_bytes=16 * 2 ** 20),
        name="update",
    )(*state)
    emb_new, head_new, emb_rn, head_rn, emb_cn, head_cn, emb_half, head_half = outs
    return (emb_new.T, head_new, emb_rn.reshape(ROWS), emb_cn.reshape(COLS), head_rn.reshape(ROWS),
            head_cn.reshape(COLS), emb_half.T, head_half)


def solution(mesh):
    arg_specs = (P("model", "data"), P("data", "model"), P("data", "model", None), P("data", None, "model"),
                 P("model"), P("data"), P("model"), P("data"))
    result_specs = (P("model", "data"), P("data", "model"), P("model"), P("data"), P("model"), P("data"),
                    P("model", "data"), P("data", "model"))
    mapped = jax.shard_map(local_step, mesh=mesh, in_specs=arg_specs, out_specs=result_specs, check_vma=False)

    def update_tables(emb_param, head_param, emb_grad, head_grad, emb_row, emb_col, head_row, head_col):
        return mapped(emb_param, head_param, emb_grad, head_grad, emb_row, emb_col, head_row, head_col)

    return update_tables
```

```python
import functools

import jax
import jax.numpy as jnp
from jax import lax
from jax.experimental import pallas as pl
from jax.experimental.pallas import tpu as pltpu
from jax.sharding import PartitionSpec as P

TRAIN_STEP = 10
DECAY_EXP = 0.8
EPS_ONE = 1e-30
CLIP_LIMIT = 1.0
SCALE_FLOOR = 1e-3
LEARN_RATE = float(TRAIN_STEP) ** -0.5
BETA_TWO = 1.0 - float(TRAIN_STEP) ** -DECAY_EXP

VOCAB = 16384
EMBED = 768
ROWS = VOCAB // 4
COLS = EMBED // 8
LANES = 128
CHUNKS = ROWS // 2 // LANES
GROUPS = ((0, 1), (1, 1), (2, 2), (4, 12))
PAIRS = CHUNKS // 2
BLOCKS = 2 * PAIRS
AHEAD = 2
RING = 6
SHORT = 4
PARTS = 8
MESH = pl.DeviceIdType.MESH
PLANE = ((0, 1), (1, 0), (1, 1))


def exchange_kernel(emb_ref, head_ref, emb_p_ref, head_p_ref, emb_r_ref, head_r_ref, emb_c_ref, head_c_ref,
                    stage_e, stage_h, par_e, par_h, emb_rows_out, head_rows_out, emb_cols_out, head_cols_out, scale_out,
                    both_e, sum_e, both_h, in1, in2, peer,
                    rows, old_rows, old_cols, rp_own, rp_in, col_acc, t_acc, rsum, psum, m_own, m_in, m_sum, s_own, s_in,
                    s0e_r, s0h_r, s1_r, s2_r, swap_r, rp_r, fw_r, send, last_r, in_sem, token):
    model = lax.axis_index("model")
    data = lax.axis_index("data")
    c = data % 2
    x = (data // 2) % 2
    y = data // 4
    oc, ox, oy = 1 - c, 1 - x, 1 - y

    def plane_id(fy, fx, fc):
        step = fy * (4 - 8 * y) + fx * (2 - 4 * x) + fc * (1 - 2 * c)
        return (model, data + step)

    def column_id(dz, fc):
        return ((model + dz) % 4, data + fc * (1 - 2 * c))

    core_peer, x_peer, y_peer = plane_id(0, 0, 1), plane_id(0, 1, 0), plane_id(1, 0, 0)

    def remote(src, dst, send_sem, recv_sem, peer_id):
        return pltpu.make_async_remote_copy(src_ref=src, dst_ref=dst, send_sem=send_sem, recv_sem=recv_sem,
                                            device_id=peer_id, device_id_type=MESH)

    def arrived(ref, sem):
        pltpu.make_async_copy(ref, ref, sem).wait()

    def vocab_at(core, first, count):
        return pl.ds(pl.multiple_of(core * (ROWS // 2) + first * LANES, LANES), count * LANES)

    half_of = 4 * COLS

    def first_e(q):
        cols = pl.ds(pl.multiple_of((oy if q == 0 else y) * half_of, LANES), half_of)
        return (pltpu.make_async_copy(emb_ref.at[vocab_at(c, 0, 1), cols], both_e.at[0, 0:LANES, cols], s0e_r.at[q]),
                remote(emb_ref.at[vocab_at(oc, 0, 1), cols], both_e.at[1, 0:LANES, cols], send.at[0], s0e_r.at[q], core_peer))

    def first_h(q):
        part = ox if q == 0 else x
        return (pltpu.make_async_copy(head_ref.at[:, part, :, :, vocab_at(c, 0, 1)], both_h.at[0, 0, :, part], s0h_r.at[q]),
                remote(head_ref.at[:, part, :, :, vocab_at(oc, 0, 1)], both_h.at[1, 0, :, part], send.at[1], s0h_r.at[q], core_peer))

    def group_e(i):
        first, count = GROUPS[i]
        at = slice(first * LANES, (first + count) * LANES)
        return (pltpu.make_async_copy(emb_ref.at[vocab_at(c, first, count), :], both_e.at[0, at, :], s0e_r.at[i + 1]),
                remote(emb_ref.at[vocab_at(oc, first, count), :], both_e.at[1, at, :], send.at[0], s0e_r.at[i + 1], core_peer))

    def group_h(i):
        first, count = GROUPS[i]
        pairs = []
        for j in range(first, first + count):
            pairs.append((pltpu.make_async_copy(head_ref.at[:, :, :, :, vocab_at(c, j, 1)], both_h.at[0, j], s0h_r.at[i + 1]),
                          remote(head_ref.at[:, :, :, :, vocab_at(oc, j, 1)], both_h.at[1, j], send.at[1], s0h_r.at[i + 1],
                                 core_peer)))
        return pairs

    def one_e(k):
        return remote(sum_e.at[k, oy], in1.at[k, 0], send.at[2], s1_r.at[k % RING], y_peer)

    def one_h(k):
        return remote(both_h.at[0, k, :, ox], in1.at[k, 1], send.at[2], s1_r.at[k % RING], x_peer)

    def two_e(k):
        return remote(in1.at[k, 0, ox], in2.at[k, 0], send.at[3], s2_r.at[k % RING], x_peer)

    def two_h(k):
        return remote(in1.at[k, 1, oy], in2.at[k, 1], send.at[3], s2_r.at[k % RING], y_peer)

    def swap(q):
        return [remote(in2.at[pl.ds(2 * q, 2), t, oc], peer.at[q, t], send.at[4], swap_r.at[q % SHORT], core_peer)
                for t in range(2)]

    def row_msg(q, i):
        fy, fx = PLANE[i]
        return remote(rp_own.at[q], rp_in.at[q, i], send.at[5], rp_r.at[q % SHORT], plane_id(fy, fx, 0))

    def row_fwd(q):
        return remote(rows.at[c * PAIRS + q], rows.at[c * PAIRS + q], send.at[6], fw_r.at[q % SHORT], core_peer)

    small_loads = [pltpu.make_async_copy(src, dst, in_sem.at[i]) for i, (src, dst) in (
        (0, (emb_p_ref, par_e)), (1, (head_p_ref, par_h)), (2, (emb_r_ref, old_rows.at[0])), (2, (head_r_ref, old_rows.at[1])),
        (3, (emb_c_ref, old_cols.at[0, c])), (3, (head_c_ref, old_cols.at[1, c])))]
    old_cols_out = [remote(src, old_cols.at[t, c], send.at[8], in_sem.at[4], core_peer)
                    for t, src in enumerate((emb_c_ref, head_c_ref))]

    barrier = pltpu.get_barrier_semaphore()
    above, below = column_id(1, 0), column_id(3, 0)
    for peer_id in (core_peer, x_peer, y_peer):
        pl.semaphore_signal(barrier, inc=1, device_id=peer_id, device_id_type=MESH)

    z_count = 1 + model * (3 - model) // 2

    def along_z(act):
        @pl.when(model < 3)
        def _():
            act(above)

        @pl.when(model > 0)
        def _():
            act(below)

    along_z(lambda peer_id: pl.semaphore_signal(barrier, inc=1, device_id=peer_id, device_id_type=MESH))
    for q in range(2):
        first_e(q)[0].start()
        first_h(q)[0].start()
    for i in range(1, len(GROUPS)):
        group_e(i)[0].start()
        for cp, _ in group_h(i):
            cp.start()
    pl.semaphore_wait(barrier, 3 + z_count)

    for q in range(2):
        first_e(q)[1].start()
        first_h(q)[1].start()
    for cp in old_cols_out:
        cp.start()
    for i in range(1, len(GROUPS)):
        group_e(i)[1].start()
        for _, cp in group_h(i):
            cp.start()
    for cp in small_loads:
        cp.start()
    along_z(lambda peer_id: pl.semaphore_signal(token.at[0], inc=1, device_id=peer_id, device_id_type=MESH))

    col_acc[...] = jnp.zeros_like(col_acc)
    t_acc[...] = jnp.zeros_like(t_acc)
    rsum[...] = jnp.zeros_like(rsum)
    psum[...] = jnp.zeros_like(psum)

    def flip_e(k, half):
        at = pl.ds(pl.multiple_of(k * LANES, LANES), LANES)
        for j in range(half_of // LANES):
            cols = pl.ds(pl.multiple_of(half * half_of + j * LANES, LANES), LANES)
            strip = (both_e[0, at, cols] + both_e[1, at, cols]).T
            done = 0
            while done < LANES:
                block, row = divmod(LANES * j + done, COLS)
                size = min(LANES - done, COLS - row)
                sum_e[k, half, block // 2, block % 2, row:row + size, :] = strip[done:done + size, :]
                done += size

    def add_h(k, part):
        for a in range(2):
            for b in range(2):
                both_h[0, k, a, part, b] = both_h[0, k, a, part, b] + both_h[1, k, a, part, b]

    def combine_cores(k):
        flip_e(k, oy)
        one_e(k).start()
        add_h(k, ox)
        one_h(k).start()
        flip_e(k, y)
        add_h(k, x)

    def first_sum(k):
        arrived(in1.at[k], s1_r.at[k % RING])
        in1[k, 0, ox] = in1[k, 0, ox] + sum_e[k, y, ox]
        two_e(k).start()
        in1[k, 1, oy] = in1[k, 1, oy] + both_h[0, k, oy, x]
        two_h(k).start()
        in1[k, 0, x] = in1[k, 0, x] + sum_e[k, y, x]
        in1[k, 1, y] = in1[k, 1, y] + both_h[0, k, y, x]

    def finish(k, q, i):
        arrived(in2.at[k], s2_r.at[k % RING])
        for t, mine in enumerate((x, y)):
            for core in range(2):
                in2[k, t, core] = in2[k, t, core] + in1[k, t, mine, core]
        for t in range(2):
            row_part = jnp.zeros((1, LANES), jnp.float32)
            for core in range(2):
                g = in2[k, t, core]
                sq = g * g + EPS_ONE
                col_acc[t, core] = col_acc[t, core] + sq
                row_part = row_part + jnp.sum(sq, axis=0, keepdims=True)
            rp_own[q, 2 * t + i:2 * t + i + 1, :] = row_part

    def send_rows(q):
        for i in (2, 1, 0):
            row_msg(q, i).start()

    def send_swap(q):
        for cp in swap(q):
            cp.start()

    def new_rows(q):
        arrived(rp_in.at[q], rp_r.at[q % SHORT])
        block = c * PAIRS + q
        row_sq = (rp_own[q] + rp_in[q, 0]) + (rp_in[q, 1] + rp_in[q, 2])
        old = jnp.concatenate([old_rows[0, block], old_rows[1, block]], axis=0)
        row_new = BETA_TWO * old + (1.0 - BETA_TWO) * (row_sq / EMBED)
        rows[block] = row_new
        return row_new

    def row_stats(q):
        row_new = new_rows(q)
        rsum[...] = rsum[...] + row_new
        inv = 1.0 / row_new
        for t in range(2):
            for core in range(2):
                acc = t_acc[t, core]
                for i in range(2):
                    g = in2[2 * q + i, t, core]
                    acc = acc + (g * g) * inv[2 * t + i:2 * t + i + 1, :]
                t_acc[t, core] = acc

    def scale_rows(block, get):
        factor = lax.rsqrt(rows[block])
        base = pl.multiple_of(block * (2 * LANES), 2 * LANES)
        for t, stage in enumerate((stage_e, stage_h)):
            for i in range(2):
                stage[:, pl.ds(base + i * LANES, LANES)] = get(t, i) * factor[2 * t + i:2 * t + i + 1, :]

    def scale_own(q):
        scale_rows(c * PAIRS + q, lambda t, i: in2[2 * q + i, t, c])

    def scale_peer(q):
        arrived(rows.at[oc * PAIRS + q], fw_r.at[q % SHORT])
        arrived(peer.at[q], swap_r.at[q % SHORT])
        scale_rows(oc * PAIRS + q, lambda t, i: peer[q, t, i])

    def param_sq(k):
        size = ROWS // CHUNKS * 2
        at = pl.ds(pl.multiple_of(k * size, size), size)
        for t, par in enumerate((par_e, par_h)):
            v = par[:, at]
            v = jnp.sum(v * v, axis=0, keepdims=True)
            for i in range(size // LANES):
                psum[t:t + 1, :] = psum[t:t + 1, :] + v[:, i * LANES:(i + 1) * LANES]

    for q in range(2):
        cols = pl.ds(pl.multiple_of((oy if q == 0 else y) * half_of, LANES), half_of)
        arrived(both_e.at[:, 0:LANES, cols], s0e_r.at[q])
        flip_e(0, oy if q == 0 else y)
        if q == 0:
            @pl.when(c == 0)
            def _():
                one_e(0).start()

        part = ox if q == 0 else x
        arrived(both_h.at[:, 0, :, part], s0h_r.at[q])
        add_h(0, part)
        if q == 0:
            @pl.when(c == 0)
            def _():
                one_h(0).start()

    def group_arrived(i):
        first, count = GROUPS[i]
        arrived(both_e.at[:, first * LANES:(first + count) * LANES, :], s0e_r.at[i + 1])
        arrived(both_h.at[:, first:first + count], s0h_r.at[i + 1])

    group_arrived(1)

    @pl.when(c == 0)
    def _():
        combine_cores(1)

    group_arrived(2)

    @pl.when(c == 1)
    def _():
        one_e(0).start()
        one_h(0).start()
        combine_cores(1)


    @pl.loop(0, CHUNKS)
    def _(k):
        for i in range(3, len(GROUPS)):
            @pl.when(k + AHEAD == GROUPS[i][0])
            def _():
                group_arrived(i)

        @pl.when(k + AHEAD < CHUNKS)
        def _():
            combine_cores(k + AHEAD)

        first_sum(k)
        pair = k // 2

        @pl.when(k == 1)
        def _():
            pl.semaphore_wait(token.at[0], z_count)
            along_z(lambda peer_id: pl.semaphore_signal(token.at[1], inc=1, device_id=peer_id, device_id_type=MESH))

        @pl.when(k == 2)
        def _():
            pl.semaphore_wait(token.at[1], z_count)

        @pl.when(k == 3)
        def _():
            arrived(par_e, in_sem.at[0])
            arrived(par_h, in_sem.at[1])
            arrived(old_rows, in_sem.at[2])

        @pl.when(k >= CHUNKS // 2)
        def _():
            param_sq(k - CHUNKS // 2)

        @pl.when((k >= 2) & (k % 2 == 0))
        def _():
            finish(k - 2, pair - 1, 0)

        @pl.when((k >= 3) & (k % 2 == 1))
        def _():
            finish(k - 2, pair - 1, 1)
            send_rows(pair - 1)
            send_swap(pair - 1)

        @pl.when((k >= 7) & (k % 2 == 1))
        def _():
            scale_peer(pair - 3)

        @pl.when((k >= 5) & (k % 2 == 1))
        def _():
            row_stats(pair - 2)
            row_fwd(pair - 2).start()
            scale_own(pair - 2)

    lane = lax.broadcasted_iota(jnp.int32, (1, LANES), 1)
    diag = lax.broadcasted_iota(jnp.int32, (COLS, LANES), 0) == lax.broadcasted_iota(jnp.int32, (COLS, LANES), 1)

    def as_row(acc):
        col = jnp.sum(acc, axis=1, keepdims=True)
        return jnp.sum(jnp.where(diag, col, 0.0), axis=0, keepdims=True)

    def total_of(v):
        return jnp.sum(jnp.sum(v, axis=0, keepdims=True), axis=1, keepdims=True)

    r_parts = [total_of(rsum[2 * t:2 * t + 2, :]) for t in range(2)]
    p_parts = [jnp.sum(psum[t:t + 1, :], axis=1, keepdims=True) for t in range(2)]
    for t in range(2):
        for core in range(2):
            m_own[0, core, t:t + 1, :] = as_row(t_acc[t, core])

    def to_column(kind):
        for z in range(4):
            for fc in (1, 0):
                def send_it(z=z, fc=fc):
                    remote(m_own.at[kind], m_in.at[2 * model + c, kind], send.at[7], last_r.at[0], (z, data + fc * (1 - 2 * c))).start()

                if fc:
                    send_it()
                else:
                    pl.when(model != z)(send_it)

    to_column(0)
    finish(CHUNKS - 2, PAIRS - 1, 0)
    finish(CHUNKS - 1, PAIRS - 1, 1)
    send_rows(PAIRS - 1)
    for t in range(2):
        for core in range(2):
            row = as_row(col_acc[t, core])
            m_own[1, core, t:t + 1, :] = jnp.where(lane == COLS, r_parts[t], jnp.where(lane == COLS + 1, p_parts[t], row))
    to_column(1)
    m_in[2 * model + c] = m_own[...]
    send_swap(PAIRS - 1)

    arrived(old_cols.at[:, c], in_sem.at[3])
    arrived(old_cols.at[:, oc], in_sem.at[4])
    arrived(m_in.at[0:7], last_r.at[0])
    total = jnp.sum(m_in[...], axis=0)
    m_sum[...] = total
    r_firsts, p_cols, u_firsts, weights = [], [], [], []
    for t in range(2):
        cols = total[1, 0, t:t + 1, :]
        r_first = jnp.sum(jnp.where(lane == COLS, cols, 0.0), axis=1, keepdims=True) / VOCAB
        u_first = jnp.zeros((1, COLS), jnp.float32)
        for core in range(2):
            col_new = BETA_TWO * old_cols[t, core] + (1.0 - BETA_TWO) * (total[1, core, t:t + 1, :COLS] / VOCAB)
            weight = r_first / col_new
            u_first = u_first + total[0, core, t:t + 1, :COLS] * weight
            weights.append(jnp.sum(jnp.where(diag[:, :COLS], weight, 0.0), axis=1, keepdims=True))
        r_firsts.append(r_first)
        p_cols.append(jnp.sum(jnp.where(lane == COLS + 1, cols, 0.0), axis=1, keepdims=True))
        u_firsts.append(0.125 * jnp.sum(u_first, axis=1, keepdims=True))

    late = (PAIRS - 2, PAIRS - 1)
    row_new = [new_rows(q) for q in late]
    inv = [1.0 / r for r in row_new]
    message = jnp.zeros((1, LANES), jnp.float32)
    for t in range(2):
        acc = jnp.zeros((COLS, LANES), jnp.float32)
        for core in range(2):
            part = jnp.zeros((COLS, LANES), jnp.float32)
            for q, r in zip(late, inv):
                for i in range(2):
                    g = in2[2 * q + i, t, core]
                    part = part + (g * g) * r[2 * t + i:2 * t + i + 1, :]
            acc = acc + part * weights[2 * t + core]
        r_mean = 0.03125 * r_firsts[t] + 0.25 * total_of((row_new[0] + row_new[1])[2 * t:2 * t + 2, :]) / VOCAB
        for i, value in enumerate((u_firsts[t] + total_of(acc), 0.125 * p_cols[t], r_mean)):
            message = jnp.where(lane == 3 * t + i, value, message)
    s_own[...] = message

    me = 8 * model + data
    s_in[me] = message
    for z in range(4):
        for fy, fx, fc in ((1, 1, 1), (1, 1, 0), (0, 1, 1), (1, 0, 1), (0, 1, 0), (1, 0, 0), (0, 0, 1), (0, 0, 0)):
            def send_it(z=z, fy=fy, fx=fx, fc=fc):
                remote(s_own, s_in.at[me], send.at[9], last_r.at[1], (z, plane_id(fy, fx, fc)[1])).start()

            if fy + fx + fc:
                send_it()
            else:
                pl.when(model != z)(send_it)

    for q in late:
        row_fwd(q).start()
        scale_own(q)

    factor_cols = []
    for t, c_out in enumerate((emb_cols_out, head_cols_out)):
        cols = m_sum[1, c, t:t + 1, :]
        col_new = BETA_TWO * old_cols[t, c] + (1.0 - BETA_TWO) * (cols[:, :COLS] / VOCAB)
        c_out[...] = col_new
        factor_cols.append(jnp.sum(jnp.where(diag[:, :COLS], lax.rsqrt(col_new), 0.0), axis=1, keepdims=True))

    @pl.loop(PAIRS - 3, PAIRS)
    def _(q):
        scale_peer(q)

    emb_rows_out[...] = rows[:, :2, :]
    head_rows_out[...] = rows[:, 2:, :]
    arrived(both_e.at[0], send.at[0])
    arrived(both_h.at[0], send.at[1])
    arrived(in1, send.at[2])
    arrived(in2, send.at[3])
    arrived(peer, send.at[4])
    arrived(rp_in, send.at[5])
    arrived(rows.at[0:PAIRS], send.at[6])
    arrived(m_in.at[0:7], send.at[7])
    arrived(old_cols.at[:, c], send.at[8])
    arrived(s_in.at[0:31], last_r.at[1])
    message = jnp.sum(s_in[...], axis=0)
    count = float(VOCAB * EMBED)
    for t in range(2):
        u_sq, p_sq, r_mean = [jnp.sum(jnp.where(lane == 3 * t + i, message, 0.0), axis=1, keepdims=True) for i in range(3)]
        u_rms = jnp.sqrt(u_sq * (r_mean / r_firsts[t]) / count)
        p_rms = jnp.sqrt(p_sq / count)
        step = LEARN_RATE * jnp.maximum(SCALE_FLOOR, p_rms) / jnp.maximum(1.0, u_rms / CLIP_LIMIT)
        scale_out[t] = jnp.broadcast_to(factor_cols[t] * (step * jnp.sqrt(r_mean)), (COLS, LANES))
    arrived(s_in.at[0:31], send.at[9])


def update_kernel(emb_g, head_g, emb_p, head_p, emb_rows, head_rows, emb_cols, head_cols, scale,
                  emb_new, head_new, emb_rows_new, head_rows_new, emb_cols_new, head_cols_new, emb_half, head_half,
                  new_buf, half_buf, small_sem, big_sem):
    small = [pltpu.make_async_copy(src, dst, small_sem.at[i]) for i, (src, dst) in enumerate(
        ((emb_rows, emb_rows_new), (head_rows, head_rows_new), (emb_cols, emb_cols_new), (head_cols, head_cols_new)))]
    for cp in small:
        cp.start()
    size = ROWS // PARTS
    tables = ((emb_p, emb_g, emb_new, emb_half), (head_p, head_g, head_new, head_half))
    for i in range(PARTS):
        part = slice(i * size, (i + 1) * size)
        for t, (p, g, new, half) in enumerate(tables):
            value = p[:, part] - g[:, part] * scale[t, :, 0:1]
            new_buf[t, :, part] = value
            half_buf[t, :, part] = value.astype(jnp.bfloat16)
            pltpu.make_async_copy(new_buf.at[t, :, part], new.at[:, part], big_sem.at[0]).start()
            pltpu.make_async_copy(half_buf.at[t, :, part], half.at[:, part], big_sem.at[1]).start()
    for cp in small:
        cp.wait()
    pltpu.make_async_copy(new_buf, new_buf, big_sem.at[0]).wait()
    pltpu.make_async_copy(half_buf, half_buf, big_sem.at[1]).wait()


def local_step(emb_p, head_p, emb_g, head_g, emb_r, emb_c, head_r, head_c):
    f32 = jnp.float32
    n = CHUNKS
    dma = pltpu.SemaphoreType.DMA
    hbm = pl.BlockSpec(memory_space=pltpu.HBM)
    vmem = pl.BlockSpec(memory_space=pltpu.VMEM)
    rows_shape = (BLOCKS, 2, LANES)
    table = jax.ShapeDtypeStruct((COLS, ROWS), f32)
    half = jax.ShapeDtypeStruct((COLS, ROWS), jnp.bfloat16)
    emb_p = emb_p.T
    shapes = [(2, ROWS // 2, EMBED), (n, 2, 2, 2, COLS, LANES), (2, n, 2, 2, 2, COLS, LANES)]
    shapes += [(n, 2, 2, 2, COLS, LANES), (n, 2, 2, COLS, LANES), (PAIRS, 2, 2, COLS, LANES)]
    shapes += [(BLOCKS, 4, LANES), (2, *rows_shape), (2, 2, 1, COLS)]
    shapes += [(PAIRS, 4, LANES), (PAIRS, 3, 4, LANES)]
    shapes += [(2, 2, COLS, LANES)] * 2 + [(4, LANES), (2, LANES)]
    shapes += [(2, 2, 2, LANES), (8, 2, 2, 2, LANES), (2, 2, 2, LANES), (1, LANES), (32, 1, LANES)]
    scratch = [pltpu.VMEM(shape, f32) for shape in shapes]
    scratch += [dma((len(GROUPS) + 1,))] * 2 + [dma((RING,))] * 2 + [dma((SHORT,))] * 3
    scratch += [dma((10,)), dma((2,)), dma((5,)), pltpu.SemaphoreType.REGULAR((2,))]
    kept = [pltpu.VMEM((COLS, ROWS), f32)] * 4 + [pltpu.VMEM(rows_shape, f32)] * 2 + [pltpu.VMEM((1, COLS), f32)] * 2
    kept.append(pltpu.VMEM((2, COLS, LANES), f32))
    state = pl.pallas_call(
        exchange_kernel,
        out_shape=tuple(kept),
        in_specs=[hbm] * 8,
        out_specs=(vmem,) * 9,
        scratch_shapes=scratch,
        compiler_params=pltpu.CompilerParams(collective_id=0, has_side_effects=True, vmem_limit_bytes=60_000_000),
        name="exchange",
    )(emb_g.reshape(ROWS, EMBED), head_g.reshape(2, 2, 2, COLS, ROWS), emb_p, head_p,
      emb_r.reshape(rows_shape), head_r.reshape(rows_shape), emb_c.reshape(1, COLS), head_c.reshape(1, COLS))

    outs = pl.pallas_call(
        update_kernel,
        out_shape=(table, table, jax.ShapeDtypeStruct(rows_shape, f32), jax.ShapeDtypeStruct(rows_shape, f32),
                   jax.ShapeDtypeStruct((1, COLS), f32), jax.ShapeDtypeStruct((1, COLS), f32), half, half),
        in_specs=[vmem] * 9,
        out_specs=(hbm,) * 8,
        scratch_shapes=[pltpu.VMEM((2, COLS, ROWS), f32), pltpu.VMEM((2, COLS, ROWS), jnp.bfloat16),
                        dma((4,)), dma((2,))],
        compiler_params=pltpu.CompilerParams(vmem_limit_bytes=16 * 2 ** 20),
        name="update",
    )(*state)
    emb_new, head_new, emb_rn, head_rn, emb_cn, head_cn, emb_half, head_half = outs
    return (emb_new.T, head_new, emb_rn.reshape(ROWS), emb_cn.reshape(COLS), head_rn.reshape(ROWS),
            head_cn.reshape(COLS), emb_half.T, head_half)


def solution(mesh):
    arg_specs = (P("model", "data"), P("data", "model"), P("data", "model", None), P("data", None, "model"),
                 P("model"), P("data"), P("model"), P("data"))
    result_specs = (P("model", "data"), P("data", "model"), P("model"), P("data"), P("model"), P("data"),
                    P("model", "data"), P("data", "model"))
    mapped = jax.shard_map(local_step, mesh=mesh, in_specs=arg_specs, out_specs=result_specs, check_vma=False)

    def update_tables(emb_param, head_param, emb_grad, head_grad, emb_row, emb_col, head_row, head_col):
        return mapped(emb_param, head_param, emb_grad, head_grad, emb_row, emb_col, head_row, head_col)

    return update_tables
```

```python
import functools

import jax
import jax.numpy as jnp
from jax import lax
from jax.experimental import pallas as pl
from jax.experimental.pallas import tpu as pltpu
from jax.sharding import PartitionSpec as P

TRAIN_STEP = 10
DECAY_EXP = 0.8
EPS_ONE = 1e-30
CLIP_LIMIT = 1.0
SCALE_FLOOR = 1e-3
LEARN_RATE = float(TRAIN_STEP) ** -0.5
BETA_TWO = 1.0 - float(TRAIN_STEP) ** -DECAY_EXP

VOCAB = 16384
EMBED = 768
ROWS = VOCAB // 4
COLS = EMBED // 8
LANES = 128
CHUNKS = ROWS // 2 // LANES
GROUPS = ((0, 1), (1, 1), (2, 2), (4, 12))
PAIRS = CHUNKS // 2
BLOCKS = 2 * PAIRS
AHEAD = 2
RING = 6
SHORT = 4
PARTS = 8
MESH = pl.DeviceIdType.MESH
PLANE = ((0, 1), (1, 0), (1, 1))


def exchange_kernel(emb_ref, head_ref, emb_p_ref, head_p_ref, emb_r_ref, head_r_ref, emb_c_ref, head_c_ref,
                    stage_e, stage_h, par_e, par_h, emb_rows_out, head_rows_out, emb_cols_out, head_cols_out, scale_out,
                    both_e, sum_e, both_h, in1, in2, peer,
                    rows, old_rows, old_cols, rp_own, rp_in, col_acc, t_acc, rsum, psum, m_own, m_in, m_sum, s_own, s_in,
                    s0e_r, s0h_r, s1_r, s2_r, swap_r, rp_r, fw_r, send, last_r, in_sem, token):
    model = lax.axis_index("model")
    data = lax.axis_index("data")
    c = data % 2
    x = (data // 2) % 2
    y = data // 4
    oc, ox, oy = 1 - c, 1 - x, 1 - y

    def plane_id(fy, fx, fc):
        step = fy * (4 - 8 * y) + fx * (2 - 4 * x) + fc * (1 - 2 * c)
        return (model, data + step)

    def column_id(dz, fc):
        return ((model + dz) % 4, data + fc * (1 - 2 * c))

    core_peer, x_peer, y_peer = plane_id(0, 0, 1), plane_id(0, 1, 0), plane_id(1, 0, 0)

    def remote(src, dst, send_sem, recv_sem, peer_id):
        return pltpu.make_async_remote_copy(src_ref=src, dst_ref=dst, send_sem=send_sem, recv_sem=recv_sem,
                                            device_id=peer_id, device_id_type=MESH)

    def arrived(ref, sem):
        pltpu.make_async_copy(ref, ref, sem).wait()

    def vocab_at(core, first, count):
        return pl.ds(pl.multiple_of(core * (ROWS // 2) + first * LANES, LANES), count * LANES)

    half_of = 4 * COLS

    def first_e(q):
        cols = pl.ds(pl.multiple_of((oy if q == 0 else y) * half_of, LANES), half_of)
        return (pltpu.make_async_copy(emb_ref.at[vocab_at(c, 0, 1), cols], both_e.at[0, 0:LANES, cols], s0e_r.at[q]),
                remote(emb_ref.at[vocab_at(oc, 0, 1), cols], both_e.at[1, 0:LANES, cols], send.at[0], s0e_r.at[q], core_peer))

    def first_h(q):
        part = ox if q == 0 else x
        return (pltpu.make_async_copy(head_ref.at[:, part, :, :, vocab_at(c, 0, 1)], both_h.at[0, 0, :, part], s0h_r.at[q]),
                remote(head_ref.at[:, part, :, :, vocab_at(oc, 0, 1)], both_h.at[1, 0, :, part], send.at[1], s0h_r.at[q], core_peer))

    def group_e(i):
        first, count = GROUPS[i]
        at = slice(first * LANES, (first + count) * LANES)
        return (pltpu.make_async_copy(emb_ref.at[vocab_at(c, first, count), :], both_e.at[0, at, :], s0e_r.at[i + 1]),
                remote(emb_ref.at[vocab_at(oc, first, count), :], both_e.at[1, at, :], send.at[0], s0e_r.at[i + 1], core_peer))

    def group_h(i):
        first, count = GROUPS[i]
        pairs = []
        for j in range(first, first + count):
            pairs.append((pltpu.make_async_copy(head_ref.at[:, :, :, :, vocab_at(c, j, 1)], both_h.at[0, j], s0h_r.at[i + 1]),
                          remote(head_ref.at[:, :, :, :, vocab_at(oc, j, 1)], both_h.at[1, j], send.at[1], s0h_r.at[i + 1],
                                 core_peer)))
        return pairs

    def one_e(k):
        return remote(sum_e.at[k, oy], in1.at[k, 0], send.at[2], s1_r.at[k % RING], y_peer)

    def one_h(k):
        return remote(both_h.at[0, k, :, ox], in1.at[k, 1], send.at[2], s1_r.at[k % RING], x_peer)

    def two_e(k):
        return remote(in1.at[k, 0, ox], in2.at[k, 0], send.at[3], s2_r.at[k % RING], x_peer)

    def two_h(k):
        return remote(in1.at[k, 1, oy], in2.at[k, 1], send.at[3], s2_r.at[k % RING], y_peer)

    def swap(q):
        return [remote(in2.at[pl.ds(2 * q, 2), t, oc], peer.at[q, t], send.at[4], swap_r.at[q % SHORT], core_peer)
                for t in range(2)]

    def row_msg(q, i):
        fy, fx = PLANE[i]
        return remote(rp_own.at[q], rp_in.at[q, i], send.at[5], rp_r.at[q % SHORT], plane_id(fy, fx, 0))

    def row_fwd(q):
        return remote(rows.at[c * PAIRS + q], rows.at[c * PAIRS + q], send.at[6], fw_r.at[q % SHORT], core_peer)

    small_loads = [pltpu.make_async_copy(src, dst, in_sem.at[i]) for i, (src, dst) in (
        (0, (emb_p_ref, par_e)), (1, (head_p_ref, par_h)), (2, (emb_r_ref, old_rows.at[0])), (2, (head_r_ref, old_rows.at[1])),
        (3, (emb_c_ref, old_cols.at[0, c])), (3, (head_c_ref, old_cols.at[1, c])))]
    old_cols_out = [remote(src, old_cols.at[t, c], send.at[8], in_sem.at[4], core_peer)
                    for t, src in enumerate((emb_c_ref, head_c_ref))]

    barrier = pltpu.get_barrier_semaphore()
    above, below = column_id(1, 0), column_id(3, 0)
    for peer_id in (core_peer, x_peer, y_peer):
        pl.semaphore_signal(barrier, inc=1, device_id=peer_id, device_id_type=MESH)

    z_count = 1 + model * (3 - model) // 2

    def along_z(act):
        @pl.when(model < 3)
        def _():
            act(above)

        @pl.when(model > 0)
        def _():
            act(below)

    along_z(lambda peer_id: pl.semaphore_signal(barrier, inc=1, device_id=peer_id, device_id_type=MESH))
    for q in range(2):
        first_e(q)[0].start()
        first_h(q)[0].start()
    for i in range(1, len(GROUPS)):
        group_e(i)[0].start()
        for cp, _ in group_h(i):
            cp.start()
    pl.semaphore_wait(barrier, 3 + z_count)

    for q in range(2):
        first_e(q)[1].start()
        first_h(q)[1].start()
    for cp in old_cols_out:
        cp.start()
    for i in range(1, len(GROUPS)):
        group_e(i)[1].start()
        for _, cp in group_h(i):
            cp.start()
    for cp in small_loads:
        cp.start()
    along_z(lambda peer_id: pl.semaphore_signal(token.at[0], inc=1, device_id=peer_id, device_id_type=MESH))

    col_acc[...] = jnp.zeros_like(col_acc)
    t_acc[...] = jnp.zeros_like(t_acc)
    rsum[...] = jnp.zeros_like(rsum)
    psum[...] = jnp.zeros_like(psum)

    def flip_e(k, half):
        at = pl.ds(pl.multiple_of(k * LANES, LANES), LANES)
        for j in range(half_of // LANES):
            cols = pl.ds(pl.multiple_of(half * half_of + j * LANES, LANES), LANES)
            strip = (both_e[0, at, cols] + both_e[1, at, cols]).T
            done = 0
            while done < LANES:
                block, row = divmod(LANES * j + done, COLS)
                size = min(LANES - done, COLS - row)
                sum_e[k, half, block // 2, block % 2, row:row + size, :] = strip[done:done + size, :]
                done += size

    def add_h(k, part):
        for a in range(2):
            for b in range(2):
                both_h[0, k, a, part, b] = both_h[0, k, a, part, b] + both_h[1, k, a, part, b]

    def combine_cores(k):
        flip_e(k, oy)
        one_e(k).start()
        add_h(k, ox)
        one_h(k).start()
        flip_e(k, y)
        add_h(k, x)

    def first_sum(k):
        arrived(in1.at[k], s1_r.at[k % RING])
        in1[k, 0, ox] = in1[k, 0, ox] + sum_e[k, y, ox]
        two_e(k).start()
        in1[k, 1, oy] = in1[k, 1, oy] + both_h[0, k, oy, x]
        two_h(k).start()
        in1[k, 0, x] = in1[k, 0, x] + sum_e[k, y, x]
        in1[k, 1, y] = in1[k, 1, y] + both_h[0, k, y, x]

    def finish(k, q, i):
        arrived(in2.at[k], s2_r.at[k % RING])
        for t, mine in enumerate((x, y)):
            for core in range(2):
                in2[k, t, core] = in2[k, t, core] + in1[k, t, mine, core]
        for t in range(2):
            row_part = jnp.zeros((1, LANES), jnp.float32)
            for core in range(2):
                g = in2[k, t, core]
                sq = g * g + EPS_ONE
                col_acc[t, core] = col_acc[t, core] + sq
                row_part = row_part + jnp.sum(sq, axis=0, keepdims=True)
            rp_own[q, 2 * t + i:2 * t + i + 1, :] = row_part

    def send_rows(q):
        for i in (2, 1, 0):
            row_msg(q, i).start()

    def send_swap(q):
        for cp in swap(q):
            cp.start()

    def new_rows(q):
        arrived(rp_in.at[q], rp_r.at[q % SHORT])
        block = c * PAIRS + q
        row_sq = (rp_own[q] + rp_in[q, 0]) + (rp_in[q, 1] + rp_in[q, 2])
        old = jnp.concatenate([old_rows[0, block], old_rows[1, block]], axis=0)
        row_new = BETA_TWO * old + (1.0 - BETA_TWO) * (row_sq / EMBED)
        rows[block] = row_new
        return row_new

    def row_stats(q):
        row_new = new_rows(q)
        rsum[...] = rsum[...] + row_new
        inv = 1.0 / row_new
        for t in range(2):
            for core in range(2):
                acc = t_acc[t, core]
                for i in range(2):
                    g = in2[2 * q + i, t, core]
                    acc = acc + (g * g) * inv[2 * t + i:2 * t + i + 1, :]
                t_acc[t, core] = acc

    def scale_rows(block, get):
        factor = lax.rsqrt(rows[block])
        base = pl.multiple_of(block * (2 * LANES), 2 * LANES)
        for t, stage in enumerate((stage_e, stage_h)):
            for i in range(2):
                stage[:, pl.ds(base + i * LANES, LANES)] = get(t, i) * factor[2 * t + i:2 * t + i + 1, :]

    def scale_own(q):
        scale_rows(c * PAIRS + q, lambda t, i: in2[2 * q + i, t, c])

    def scale_peer(q):
        arrived(rows.at[oc * PAIRS + q], fw_r.at[q % SHORT])
        arrived(peer.at[q], swap_r.at[q % SHORT])
        scale_rows(oc * PAIRS + q, lambda t, i: peer[q, t, i])

    def param_sq(k):
        size = ROWS // CHUNKS * 2
        at = pl.ds(pl.multiple_of(k * size, size), size)
        for t, par in enumerate((par_e, par_h)):
            v = par[:, at]
            v = jnp.sum(v * v, axis=0, keepdims=True)
            for i in range(size // LANES):
                psum[t:t + 1, :] = psum[t:t + 1, :] + v[:, i * LANES:(i + 1) * LANES]

    for q in range(2):
        cols = pl.ds(pl.multiple_of((oy if q == 0 else y) * half_of, LANES), half_of)
        arrived(both_e.at[:, 0:LANES, cols], s0e_r.at[q])
        flip_e(0, oy if q == 0 else y)
        if q == 0:
            @pl.when(c == 0)
            def _():
                one_e(0).start()

        part = ox if q == 0 else x
        arrived(both_h.at[:, 0, :, part], s0h_r.at[q])
        add_h(0, part)
        if q == 0:
            @pl.when(c == 0)
            def _():
                one_h(0).start()

    def group_arrived(i):
        first, count = GROUPS[i]
        arrived(both_e.at[:, first * LANES:(first + count) * LANES, :], s0e_r.at[i + 1])
        arrived(both_h.at[:, first:first + count], s0h_r.at[i + 1])

    group_arrived(1)

    @pl.when(c == 0)
    def _():
        combine_cores(1)

    group_arrived(2)

    @pl.when(c == 1)
    def _():
        one_e(0).start()
        one_h(0).start()
        combine_cores(1)


    @pl.loop(0, CHUNKS)
    def _(k):
        for i in range(3, len(GROUPS)):
            @pl.when(k + AHEAD == GROUPS[i][0])
            def _():
                group_arrived(i)

        @pl.when(k + AHEAD < CHUNKS)
        def _():
            combine_cores(k + AHEAD)

        first_sum(k)
        pair = k // 2

        @pl.when(k == 1)
        def _():
            pl.semaphore_wait(token.at[0], z_count)
            along_z(lambda peer_id: pl.semaphore_signal(token.at[1], inc=1, device_id=peer_id, device_id_type=MESH))

        @pl.when(k == 2)
        def _():
            pl.semaphore_wait(token.at[1], z_count)

        @pl.when(k == 3)
        def _():
            arrived(par_e, in_sem.at[0])
            arrived(par_h, in_sem.at[1])
            arrived(old_rows, in_sem.at[2])

        @pl.when(k >= CHUNKS // 2)
        def _():
            param_sq(k - CHUNKS // 2)

        @pl.when((k >= 2) & (k % 2 == 0))
        def _():
            finish(k - 2, pair - 1, 0)

        @pl.when((k >= 3) & (k % 2 == 1))
        def _():
            finish(k - 2, pair - 1, 1)
            send_rows(pair - 1)
            send_swap(pair - 1)

        @pl.when((k >= 7) & (k % 2 == 1))
        def _():
            scale_peer(pair - 3)

        @pl.when((k >= 5) & (k % 2 == 1))
        def _():
            row_stats(pair - 2)
            row_fwd(pair - 2).start()
            scale_own(pair - 2)

    lane = lax.broadcasted_iota(jnp.int32, (1, LANES), 1)
    diag = lax.broadcasted_iota(jnp.int32, (COLS, LANES), 0) == lax.broadcasted_iota(jnp.int32, (COLS, LANES), 1)

    def as_row(acc):
        col = jnp.sum(acc, axis=1, keepdims=True)
        return jnp.sum(jnp.where(diag, col, 0.0), axis=0, keepdims=True)

    def total_of(v):
        return jnp.sum(jnp.sum(v, axis=0, keepdims=True), axis=1, keepdims=True)

    def to_column(kind):
        for z in range(4):
            for fc in (1, 0):
                def send_it(z=z, fc=fc):
                    remote(m_own.at[kind], m_in.at[2 * model + c, kind], send.at[7], last_r.at[0], (z, data + fc * (1 - 2 * c))).start()

                if fc:
                    send_it()
                else:
                    pl.when(model != z)(send_it)

    def send_weighted():
        for t in range(2):
            r_part = total_of(rsum[2 * t:2 * t + 2, :])
            p_part = jnp.sum(psum[t:t + 1, :], axis=1, keepdims=True)
            for core in range(2):
                row = as_row(t_acc[t, core])
                row = jnp.where(lane == COLS, r_part, jnp.where(lane == COLS + 1, p_part, row))
                m_own[0, core, t:t + 1, :] = row
        to_column(0)

    late = (PAIRS - 2, PAIRS - 1)

    pl.when(c == 1)(send_weighted)
    finish(CHUNKS - 2, PAIRS - 1, 0)
    finish(CHUNKS - 1, PAIRS - 1, 1)
    send_rows(PAIRS - 1)
    for t in range(2):
        for core in range(2):
            m_own[1, core, t:t + 1, :] = as_row(col_acc[t, core])
    to_column(1)
    send_swap(PAIRS - 1)

    @pl.when(c == 0)
    def _():
        for q in late:
            row_stats(q)
            row_fwd(q).start()
        send_weighted()

    m_in[2 * model + c] = m_own[...]
    arrived(old_cols.at[:, c], in_sem.at[3])
    arrived(old_cols.at[:, oc], in_sem.at[4])
    arrived(m_in.at[0:7], last_r.at[0])
    total = jnp.sum(m_in[...], axis=0)
    m_sum[...] = total
    firsts = total[0, 0]
    r_firsts = [jnp.sum(jnp.where(lane == COLS, firsts[t:t + 1, :], 0.0), axis=1, keepdims=True) / VOCAB for t in range(2)]
    chip = 4 * model + data // 2

    @pl.when(c == 1)
    def _():
        message = jnp.zeros((1, LANES), jnp.float32)
        u_firsts, weights = [], []
        for t in range(2):
            u_first = jnp.zeros((1, COLS), jnp.float32)
            for core in range(2):
                col_new = BETA_TWO * old_cols[t, core] + (1.0 - BETA_TWO) * (m_sum[1, core, t:t + 1, :COLS] / VOCAB)
                weight = r_firsts[t] / col_new
                u_first = u_first + m_sum[0, core, t:t + 1, :COLS] * weight
                weights.append(jnp.sum(jnp.where(diag[:, :COLS], weight, 0.0), axis=1, keepdims=True))
            u_firsts.append(0.25 * jnp.sum(u_first, axis=1, keepdims=True))
        row_new = [new_rows(q) for q in late]
        inv = [1.0 / r for r in row_new]
        for t in range(2):
            acc = jnp.zeros((COLS, LANES), jnp.float32)
            for core in range(2):
                part = jnp.zeros((COLS, LANES), jnp.float32)
                for q, r in zip(late, inv):
                    for i in range(2):
                        g = in2[2 * q + i, t, core]
                        part = part + (g * g) * r[2 * t + i:2 * t + i + 1, :]
                acc = acc + part * weights[2 * t + core]
            r_mean = 0.0625 * r_firsts[t] + 0.25 * total_of((row_new[0] + row_new[1])[2 * t:2 * t + 2, :]) / VOCAB
            p_col = 0.25 * jnp.sum(jnp.where(lane == COLS + 1, m_sum[0, 0, t:t + 1, :], 0.0), axis=1, keepdims=True)
            for i, value in enumerate((u_firsts[t] + total_of(acc), p_col, r_mean)):
                message = jnp.where(lane == 3 * t + i, value, message)
        s_own[...] = message
        s_in[chip] = message
        for z in range(4):
            for fy, fx, fc in ((1, 1, 1), (1, 1, 0), (0, 1, 1), (1, 0, 1), (0, 1, 0), (1, 0, 0), (0, 0, 1), (0, 0, 0)):
                def send_it(z=z, fy=fy, fx=fx, fc=fc):
                    remote(s_own, s_in.at[chip], send.at[9], last_r.at[1], (z, plane_id(fy, fx, fc)[1])).start()

                if fy + fx + fc:
                    send_it()
                else:
                    pl.when(model != z)(send_it)

        for q in late:
            row_fwd(q).start()

    for q in late:
        scale_own(q)

    factor_cols = []
    for t, c_out in enumerate((emb_cols_out, head_cols_out)):
        cols = m_sum[1, c, t:t + 1, :]
        col_new = BETA_TWO * old_cols[t, c] + (1.0 - BETA_TWO) * (cols[:, :COLS] / VOCAB)
        c_out[...] = col_new
        factor_cols.append(jnp.sum(jnp.where(diag[:, :COLS], lax.rsqrt(col_new), 0.0), axis=1, keepdims=True))

    @pl.loop(PAIRS - 3, PAIRS)
    def _(q):
        scale_peer(q)

    emb_rows_out[...] = rows[:, :2, :]
    head_rows_out[...] = rows[:, 2:, :]
    arrived(both_e.at[0], send.at[0])
    arrived(both_h.at[0], send.at[1])
    arrived(in1, send.at[2])
    arrived(in2, send.at[3])
    arrived(peer, send.at[4])
    arrived(rp_in, send.at[5])
    arrived(rows.at[0:PAIRS], send.at[6])
    arrived(m_in.at[0:7], send.at[7])
    arrived(old_cols.at[:, c], send.at[8])

    @pl.when(c == 0)
    def _():
        arrived(s_in.at[0:16], last_r.at[1])

    @pl.when(c == 1)
    def _():
        arrived(s_in.at[0:15], last_r.at[1])

    message = jnp.sum(s_in[0:16], axis=0)
    count = float(VOCAB * EMBED)
    for t in range(2):
        u_sq, p_sq, r_mean = [jnp.sum(jnp.where(lane == 3 * t + i, message, 0.0), axis=1, keepdims=True) for i in range(3)]
        u_rms = jnp.sqrt(u_sq * (r_mean / r_firsts[t]) / count)
        p_rms = jnp.sqrt(p_sq / count)
        step = LEARN_RATE * jnp.maximum(SCALE_FLOOR, p_rms) / jnp.maximum(1.0, u_rms / CLIP_LIMIT)
        scale_out[t] = jnp.broadcast_to(factor_cols[t] * (step * jnp.sqrt(r_mean)), (COLS, LANES))

    @pl.when(c == 1)
    def _():
        arrived(s_in.at[0:31], send.at[9])


def update_kernel(emb_g, head_g, emb_p, head_p, emb_rows, head_rows, emb_cols, head_cols, scale,
                  emb_new, head_new, emb_rows_new, head_rows_new, emb_cols_new, head_cols_new, emb_half, head_half,
                  new_buf, half_buf, small_sem, big_sem):
    small = [pltpu.make_async_copy(src, dst, small_sem.at[i]) for i, (src, dst) in enumerate(
        ((emb_rows, emb_rows_new), (head_rows, head_rows_new), (emb_cols, emb_cols_new), (head_cols, head_cols_new)))]
    for cp in small:
        cp.start()
    size = ROWS // PARTS
    tables = ((emb_p, emb_g, emb_new, emb_half), (head_p, head_g, head_new, head_half))
    for i in range(PARTS):
        part = slice(i * size, (i + 1) * size)
        for t, (p, g, new, half) in enumerate(tables):
            value = p[:, part] - g[:, part] * scale[t, :, 0:1]
            new_buf[t, :, part] = value
            half_buf[t, :, part] = value.astype(jnp.bfloat16)
            pltpu.make_async_copy(new_buf.at[t, :, part], new.at[:, part], big_sem.at[0]).start()
            pltpu.make_async_copy(half_buf.at[t, :, part], half.at[:, part], big_sem.at[1]).start()
    for cp in small:
        cp.wait()
    pltpu.make_async_copy(new_buf, new_buf, big_sem.at[0]).wait()
    pltpu.make_async_copy(half_buf, half_buf, big_sem.at[1]).wait()


def local_step(emb_p, head_p, emb_g, head_g, emb_r, emb_c, head_r, head_c):
    f32 = jnp.float32
    n = CHUNKS
    dma = pltpu.SemaphoreType.DMA
    hbm = pl.BlockSpec(memory_space=pltpu.HBM)
    vmem = pl.BlockSpec(memory_space=pltpu.VMEM)
    rows_shape = (BLOCKS, 2, LANES)
    table = jax.ShapeDtypeStruct((COLS, ROWS), f32)
    half = jax.ShapeDtypeStruct((COLS, ROWS), jnp.bfloat16)
    emb_p = emb_p.T
    shapes = [(2, ROWS // 2, EMBED), (n, 2, 2, 2, COLS, LANES), (2, n, 2, 2, 2, COLS, LANES)]
    shapes += [(n, 2, 2, 2, COLS, LANES), (n, 2, 2, COLS, LANES), (PAIRS, 2, 2, COLS, LANES)]
    shapes += [(BLOCKS, 4, LANES), (2, *rows_shape), (2, 2, 1, COLS)]
    shapes += [(PAIRS, 4, LANES), (PAIRS, 3, 4, LANES)]
    shapes += [(2, 2, COLS, LANES)] * 2 + [(4, LANES), (2, LANES)]
    shapes += [(2, 2, 2, LANES), (8, 2, 2, 2, LANES), (2, 2, 2, LANES), (1, LANES), (32, 1, LANES)]
    scratch = [pltpu.VMEM(shape, f32) for shape in shapes]
    scratch += [dma((len(GROUPS) + 1,))] * 2 + [dma((RING,))] * 2 + [dma((SHORT,))] * 3
    scratch += [dma((10,)), dma((2,)), dma((5,)), pltpu.SemaphoreType.REGULAR((2,))]
    kept = [pltpu.VMEM((COLS, ROWS), f32)] * 4 + [pltpu.VMEM(rows_shape, f32)] * 2 + [pltpu.VMEM((1, COLS), f32)] * 2
    kept.append(pltpu.VMEM((2, COLS, LANES), f32))
    state = pl.pallas_call(
        exchange_kernel,
        out_shape=tuple(kept),
        in_specs=[hbm] * 8,
        out_specs=(vmem,) * 9,
        scratch_shapes=scratch,
        compiler_params=pltpu.CompilerParams(collective_id=0, has_side_effects=True, vmem_limit_bytes=60_000_000),
        name="exchange",
    )(emb_g.reshape(ROWS, EMBED), head_g.reshape(2, 2, 2, COLS, ROWS), emb_p, head_p,
      emb_r.reshape(rows_shape), head_r.reshape(rows_shape), emb_c.reshape(1, COLS), head_c.reshape(1, COLS))

    outs = pl.pallas_call(
        update_kernel,
        out_shape=(table, table, jax.ShapeDtypeStruct(rows_shape, f32), jax.ShapeDtypeStruct(rows_shape, f32),
                   jax.ShapeDtypeStruct((1, COLS), f32), jax.ShapeDtypeStruct((1, COLS), f32), half, half),
        in_specs=[vmem] * 9,
        out_specs=(hbm,) * 8,
        scratch_shapes=[pltpu.VMEM((2, COLS, ROWS), f32), pltpu.VMEM((2, COLS, ROWS), jnp.bfloat16),
                        dma((4,)), dma((2,))],
        compiler_params=pltpu.CompilerParams(vmem_limit_bytes=16 * 2 ** 20),
        name="update",
    )(*state)
    emb_new, head_new, emb_rn, head_rn, emb_cn, head_cn, emb_half, head_half = outs
    return (emb_new.T, head_new, emb_rn.reshape(ROWS), emb_cn.reshape(COLS), head_rn.reshape(ROWS),
            head_cn.reshape(COLS), emb_half.T, head_half)


def solution(mesh):
    arg_specs = (P("model", "data"), P("data", "model"), P("data", "model", None), P("data", None, "model"),
                 P("model"), P("data"), P("model"), P("data"))
    result_specs = (P("model", "data"), P("data", "model"), P("model"), P("data"), P("model"), P("data"),
                    P("model", "data"), P("data", "model"))
    mapped = jax.shard_map(local_step, mesh=mesh, in_specs=arg_specs, out_specs=result_specs, check_vma=False)

    def update_tables(emb_param, head_param, emb_grad, head_grad, emb_row, emb_col, head_row, head_col):
        return mapped(emb_param, head_param, emb_grad, head_grad, emb_row, emb_col, head_row, head_col)

    return update_tables
```

```python
import functools

import jax
import jax.numpy as jnp
from jax import lax
from jax.experimental import pallas as pl
from jax.experimental.pallas import tpu as pltpu
from jax.sharding import PartitionSpec as P

TRAIN_STEP = 10
DECAY_EXP = 0.8
EPS_ONE = 1e-30
CLIP_LIMIT = 1.0
SCALE_FLOOR = 1e-3
LEARN_RATE = float(TRAIN_STEP) ** -0.5
BETA_TWO = 1.0 - float(TRAIN_STEP) ** -DECAY_EXP

VOCAB = 16384
EMBED = 768
ROWS = VOCAB // 4
COLS = EMBED // 8
LANES = 128
CHUNKS = ROWS // 2 // LANES
GROUPS = ((0, 1), (1, 1), (2, 2), (4, 12))
PAIRS = CHUNKS // 2
BLOCKS = 2 * PAIRS
AHEAD = 2
RING = 6
SHORT = 4
PARTS = 8
MESH = pl.DeviceIdType.MESH
PLANE = ((0, 1), (1, 0), (1, 1))


def exchange_kernel(emb_ref, head_ref, emb_p_ref, head_p_ref, emb_r_ref, head_r_ref, emb_c_ref, head_c_ref,
                    stage_e, stage_h, par_e, par_h, emb_rows_out, head_rows_out, emb_cols_out, head_cols_out, scale_out,
                    both_e, sum_e, both_h, in1, in2, peer,
                    rows, old_rows, old_cols, rp_own, rp_in, col_acc, t_acc, rsum, psum, m_own, m_in, m_sum, s_own, s_in,
                    s0e_r, s0h_r, s1_r, s2_r, swap_r, rp_r, fw_r, send, last_r, in_sem, token):
    model = lax.axis_index("model")
    data = lax.axis_index("data")
    c = data % 2
    x = (data // 2) % 2
    y = data // 4
    oc, ox, oy = 1 - c, 1 - x, 1 - y

    def plane_id(fy, fx, fc):
        step = fy * (4 - 8 * y) + fx * (2 - 4 * x) + fc * (1 - 2 * c)
        return (model, data + step)

    def column_id(dz, fc):
        return ((model + dz) % 4, data + fc * (1 - 2 * c))

    core_peer, x_peer, y_peer = plane_id(0, 0, 1), plane_id(0, 1, 0), plane_id(1, 0, 0)

    def remote(src, dst, send_sem, recv_sem, peer_id):
        return pltpu.make_async_remote_copy(src_ref=src, dst_ref=dst, send_sem=send_sem, recv_sem=recv_sem,
                                            device_id=peer_id, device_id_type=MESH)

    def arrived(ref, sem):
        pltpu.make_async_copy(ref, ref, sem).wait()

    def vocab_at(core, first, count):
        return pl.ds(pl.multiple_of(core * (ROWS // 2) + first * LANES, LANES), count * LANES)

    half_of = 4 * COLS

    def first_e(q):
        cols = pl.ds(pl.multiple_of((oy if q == 0 else y) * half_of, LANES), half_of)
        return (pltpu.make_async_copy(emb_ref.at[vocab_at(c, 0, 1), cols], both_e.at[0, 0:LANES, cols], s0e_r.at[q]),
                remote(emb_ref.at[vocab_at(oc, 0, 1), cols], both_e.at[1, 0:LANES, cols], send.at[0], s0e_r.at[q], core_peer))

    def first_h(q):
        part = ox if q == 0 else x
        return (pltpu.make_async_copy(head_ref.at[:, part, :, :, vocab_at(c, 0, 1)], both_h.at[0, 0, :, part], s0h_r.at[q]),
                remote(head_ref.at[:, part, :, :, vocab_at(oc, 0, 1)], both_h.at[1, 0, :, part], send.at[1], s0h_r.at[q], core_peer))

    def group_e(i):
        first, count = GROUPS[i]
        at = slice(first * LANES, (first + count) * LANES)
        return (pltpu.make_async_copy(emb_ref.at[vocab_at(c, first, count), :], both_e.at[0, at, :], s0e_r.at[i + 1]),
                remote(emb_ref.at[vocab_at(oc, first, count), :], both_e.at[1, at, :], send.at[0], s0e_r.at[i + 1], core_peer))

    def group_h(i):
        first, count = GROUPS[i]
        pairs = []
        for j in range(first, first + count):
            pairs.append((pltpu.make_async_copy(head_ref.at[:, :, :, :, vocab_at(c, j, 1)], both_h.at[0, j], s0h_r.at[i + 1]),
                          remote(head_ref.at[:, :, :, :, vocab_at(oc, j, 1)], both_h.at[1, j], send.at[1], s0h_r.at[i + 1],
                                 core_peer)))
        return pairs

    def one_e(k):
        return remote(sum_e.at[k, oy], in1.at[k, 0], send.at[2], s1_r.at[k % RING], y_peer)

    def one_h(k):
        return remote(both_h.at[0, k, :, ox], in1.at[k, 1], send.at[2], s1_r.at[k % RING], x_peer)

    def two_e(k):
        return remote(in1.at[k, 0, ox], in2.at[k, 0], send.at[3], s2_r.at[k % RING], x_peer)

    def two_h(k):
        return remote(in1.at[k, 1, oy], in2.at[k, 1], send.at[3], s2_r.at[k % RING], y_peer)

    def swap(q):
        return [remote(in2.at[pl.ds(2 * q, 2), t, oc], peer.at[q, t], send.at[4], swap_r.at[q % SHORT], core_peer)
                for t in range(2)]

    def row_msg(q, i):
        fy, fx = PLANE[i]
        return remote(rp_own.at[q], rp_in.at[q, i], send.at[5], rp_r.at[q % SHORT], plane_id(fy, fx, 0))

    def row_fwd(q):
        return remote(rows.at[c * PAIRS + q], rows.at[c * PAIRS + q], send.at[6], fw_r.at[q % SHORT], core_peer)

    small_loads = [pltpu.make_async_copy(src, dst, in_sem.at[i]) for i, (src, dst) in (
        (0, (emb_p_ref, par_e)), (1, (head_p_ref, par_h)), (2, (emb_r_ref, old_rows.at[0])), (2, (head_r_ref, old_rows.at[1])),
        (3, (emb_c_ref, old_cols.at[0, c])), (3, (head_c_ref, old_cols.at[1, c])))]
    old_cols_out = [remote(src, old_cols.at[t, c], send.at[8], in_sem.at[4], core_peer)
                    for t, src in enumerate((emb_c_ref, head_c_ref))]

    barrier = pltpu.get_barrier_semaphore()
    above, below = column_id(1, 0), column_id(3, 0)
    for peer_id in (core_peer, x_peer, y_peer):
        pl.semaphore_signal(barrier, inc=1, device_id=peer_id, device_id_type=MESH)

    z_count = 1 + model * (3 - model) // 2

    def along_z(act):
        @pl.when(model < 3)
        def _():
            act(above)

        @pl.when(model > 0)
        def _():
            act(below)

    along_z(lambda peer_id: pl.semaphore_signal(barrier, inc=1, device_id=peer_id, device_id_type=MESH))
    for q in range(2):
        first_e(q)[0].start()
        first_h(q)[0].start()
    for i in range(1, len(GROUPS)):
        group_e(i)[0].start()
        for cp, _ in group_h(i):
            cp.start()
    pl.semaphore_wait(barrier, 3 + z_count)

    for q in range(2):
        first_e(q)[1].start()
        first_h(q)[1].start()
    for cp in old_cols_out:
        cp.start()
    for i in range(1, len(GROUPS)):
        group_e(i)[1].start()
        for _, cp in group_h(i):
            cp.start()
    for cp in small_loads:
        cp.start()
    along_z(lambda peer_id: pl.semaphore_signal(token.at[0], inc=1, device_id=peer_id, device_id_type=MESH))

    col_acc[...] = jnp.zeros_like(col_acc)
    t_acc[...] = jnp.zeros_like(t_acc)
    rsum[...] = jnp.zeros_like(rsum)
    psum[...] = jnp.zeros_like(psum)

    def flip_e(k, half):
        at = pl.ds(pl.multiple_of(k * LANES, LANES), LANES)
        for j in range(half_of // LANES):
            cols = pl.ds(pl.multiple_of(half * half_of + j * LANES, LANES), LANES)
            strip = (both_e[0, at, cols] + both_e[1, at, cols]).T
            done = 0
            while done < LANES:
                block, row = divmod(LANES * j + done, COLS)
                size = min(LANES - done, COLS - row)
                sum_e[k, half, block // 2, block % 2, row:row + size, :] = strip[done:done + size, :]
                done += size

    def add_h(k, part):
        for a in range(2):
            for b in range(2):
                both_h[0, k, a, part, b] = both_h[0, k, a, part, b] + both_h[1, k, a, part, b]

    def combine_cores(k):
        flip_e(k, oy)
        one_e(k).start()
        add_h(k, ox)
        one_h(k).start()
        flip_e(k, y)
        add_h(k, x)

    def first_sum(k):
        arrived(in1.at[k], s1_r.at[k % RING])
        in1[k, 0, ox] = in1[k, 0, ox] + sum_e[k, y, ox]
        two_e(k).start()
        in1[k, 1, oy] = in1[k, 1, oy] + both_h[0, k, oy, x]
        two_h(k).start()
        in1[k, 0, x] = in1[k, 0, x] + sum_e[k, y, x]
        in1[k, 1, y] = in1[k, 1, y] + both_h[0, k, y, x]

    def finish(k, q, i):
        arrived(in2.at[k], s2_r.at[k % RING])
        for t, mine in enumerate((x, y)):
            for core in range(2):
                in2[k, t, core] = in2[k, t, core] + in1[k, t, mine, core]
        for t in range(2):
            row_part = jnp.zeros((1, LANES), jnp.float32)
            for core in range(2):
                g = in2[k, t, core]
                sq = g * g + EPS_ONE
                col_acc[t, core] = col_acc[t, core] + sq
                row_part = row_part + jnp.sum(sq, axis=0, keepdims=True)
            rp_own[q, 2 * t + i:2 * t + i + 1, :] = row_part

    def send_rows(q):
        for i in (2, 1, 0):
            row_msg(q, i).start()

    def send_swap(q):
        for cp in swap(q):
            cp.start()

    def new_rows(q):
        arrived(rp_in.at[q], rp_r.at[q % SHORT])
        block = c * PAIRS + q
        row_sq = (rp_own[q] + rp_in[q, 0]) + (rp_in[q, 1] + rp_in[q, 2])
        old = jnp.concatenate([old_rows[0, block], old_rows[1, block]], axis=0)
        row_new = BETA_TWO * old + (1.0 - BETA_TWO) * (row_sq / EMBED)
        rows[block] = row_new
        return row_new

    def row_stats(q):
        row_new = new_rows(q)
        rsum[...] = rsum[...] + row_new
        inv = 1.0 / row_new
        for t in range(2):
            for core in range(2):
                acc = t_acc[t, core]
                for i in range(2):
                    g = in2[2 * q + i, t, core]
                    acc = acc + (g * g) * inv[2 * t + i:2 * t + i + 1, :]
                t_acc[t, core] = acc

    def scale_rows(block, get):
        factor = lax.rsqrt(rows[block])
        base = pl.multiple_of(block * (2 * LANES), 2 * LANES)
        for t, stage in enumerate((stage_e, stage_h)):
            for i in range(2):
                stage[:, pl.ds(base + i * LANES, LANES)] = get(t, i) * factor[2 * t + i:2 * t + i + 1, :]

    def scale_own(q):
        scale_rows(c * PAIRS + q, lambda t, i: in2[2 * q + i, t, c])

    def scale_peer(q):
        arrived(rows.at[oc * PAIRS + q], fw_r.at[q % SHORT])
        arrived(peer.at[q], swap_r.at[q % SHORT])
        scale_rows(oc * PAIRS + q, lambda t, i: peer[q, t, i])

    def param_sq(k):
        size = ROWS // CHUNKS * 2
        at = pl.ds(pl.multiple_of(k * size, size), size)
        for t, par in enumerate((par_e, par_h)):
            v = par[:, at]
            v = jnp.sum(v * v, axis=0, keepdims=True)
            for i in range(size // LANES):
                psum[t:t + 1, :] = psum[t:t + 1, :] + v[:, i * LANES:(i + 1) * LANES]

    for q in range(2):
        cols = pl.ds(pl.multiple_of((oy if q == 0 else y) * half_of, LANES), half_of)
        arrived(both_e.at[:, 0:LANES, cols], s0e_r.at[q])
        flip_e(0, oy if q == 0 else y)
        if q == 0:
            @pl.when(c == 0)
            def _():
                one_e(0).start()

        part = ox if q == 0 else x
        arrived(both_h.at[:, 0, :, part], s0h_r.at[q])
        add_h(0, part)
        if q == 0:
            @pl.when(c == 0)
            def _():
                one_h(0).start()

    def group_arrived(i):
        first, count = GROUPS[i]
        arrived(both_e.at[:, first * LANES:(first + count) * LANES, :], s0e_r.at[i + 1])
        arrived(both_h.at[:, first:first + count], s0h_r.at[i + 1])

    group_arrived(1)

    @pl.when(c == 0)
    def _():
        combine_cores(1)

    group_arrived(2)

    @pl.when(c == 1)
    def _():
        one_e(0).start()
        one_h(0).start()
        combine_cores(1)


    @pl.loop(0, CHUNKS)
    def _(k):
        for i in range(3, len(GROUPS)):
            @pl.when(k + AHEAD == GROUPS[i][0])
            def _():
                group_arrived(i)

        @pl.when(k + AHEAD < CHUNKS)
        def _():
            combine_cores(k + AHEAD)

        first_sum(k)
        pair = k // 2

        @pl.when(k == 1)
        def _():
            pl.semaphore_wait(token.at[0], z_count)
            along_z(lambda peer_id: pl.semaphore_signal(token.at[1], inc=1, device_id=peer_id, device_id_type=MESH))

        @pl.when(k == 2)
        def _():
            pl.semaphore_wait(token.at[1], z_count)

        @pl.when(k == 3)
        def _():
            arrived(par_e, in_sem.at[0])
            arrived(par_h, in_sem.at[1])
            arrived(old_rows, in_sem.at[2])

        @pl.when(k >= CHUNKS // 2)
        def _():
            param_sq(k - CHUNKS // 2)

        @pl.when((k >= 2) & (k % 2 == 0))
        def _():
            finish(k - 2, pair - 1, 0)

        @pl.when((k >= 3) & (k % 2 == 1))
        def _():
            finish(k - 2, pair - 1, 1)
            send_rows(pair - 1)
            send_swap(pair - 1)

        @pl.when((k >= 7) & (k % 2 == 1))
        def _():
            scale_peer(pair - 3)

        @pl.when((k >= 5) & (k % 2 == 1))
        def _():
            row_stats(pair - 2)
            row_fwd(pair - 2).start()
            scale_own(pair - 2)

    lane = lax.broadcasted_iota(jnp.int32, (1, LANES), 1)
    diag = lax.broadcasted_iota(jnp.int32, (COLS, LANES), 0) == lax.broadcasted_iota(jnp.int32, (COLS, LANES), 1)

    def as_row(acc):
        col = jnp.sum(acc, axis=1, keepdims=True)
        return jnp.sum(jnp.where(diag, col, 0.0), axis=0, keepdims=True)

    def total_of(v):
        return jnp.sum(jnp.sum(v, axis=0, keepdims=True), axis=1, keepdims=True)

    def to_column(kind):
        for z in range(4):
            for fc in (1, 0):
                def send_it(z=z, fc=fc):
                    remote(m_own.at[kind], m_in.at[2 * model + c, kind], send.at[7], last_r.at[0], (z, data + fc * (1 - 2 * c))).start()

                if fc:
                    send_it()
                else:
                    pl.when(model != z)(send_it)

    def send_weighted():
        for t in range(2):
            r_part = total_of(rsum[2 * t:2 * t + 2, :])
            p_part = jnp.sum(psum[t:t + 1, :], axis=1, keepdims=True)
            for core in range(2):
                row = as_row(t_acc[t, core])
                row = jnp.where(lane == COLS, r_part, jnp.where(lane == COLS + 1, p_part, row))
                m_own[0, core, t:t + 1, :] = row
        to_column(0)

    late = (PAIRS - 2, PAIRS - 1)

    pl.when(c == 1)(send_weighted)
    finish(CHUNKS - 2, PAIRS - 1, 0)
    finish(CHUNKS - 1, PAIRS - 1, 1)
    send_rows(PAIRS - 1)
    for t in range(2):
        for core in range(2):
            m_own[1, core, t:t + 1, :] = as_row(col_acc[t, core])
    to_column(1)
    send_swap(PAIRS - 1)

    @pl.when(c == 0)
    def _():
        for q in late:
            row_stats(q)
            row_fwd(q).start()
        send_weighted()

    m_in[2 * model + c] = m_own[...]
    arrived(old_cols.at[:, c], in_sem.at[3])
    arrived(old_cols.at[:, oc], in_sem.at[4])
    arrived(m_in.at[0:7], last_r.at[0])
    m_sum[...] = jnp.sum(m_in[...], axis=0)
    chip = 4 * model + data // 2

    @pl.when(c == 1)
    def _():
        message = jnp.zeros((1, LANES), jnp.float32)
        u_firsts, weights = [], []
        for t in range(2):
            u_first = jnp.zeros((1, COLS), jnp.float32)
            for core in range(2):
                col_new = BETA_TWO * old_cols[t, core] + (1.0 - BETA_TWO) * (m_sum[1, core, t:t + 1, :COLS] / VOCAB)
                weight = 1.0 / col_new
                u_first = u_first + m_sum[0, core, t:t + 1, :COLS] * weight
                weights.append(jnp.sum(jnp.where(diag[:, :COLS], weight, 0.0), axis=1, keepdims=True))
            u_firsts.append(0.25 * jnp.sum(u_first, axis=1, keepdims=True))
        row_new = [new_rows(q) for q in late]
        inv = [1.0 / r for r in row_new]
        for t in range(2):
            acc = jnp.zeros((COLS, LANES), jnp.float32)
            for core in range(2):
                part = jnp.zeros((COLS, LANES), jnp.float32)
                for q, r in zip(late, inv):
                    for i in range(2):
                        g = in2[2 * q + i, t, core]
                        part = part + (g * g) * r[2 * t + i:2 * t + i + 1, :]
                acc = acc + part * weights[2 * t + core]
            r_early, p_col = [jnp.sum(jnp.where(lane == COLS + i, m_sum[0, 0, t:t + 1, :], 0.0), axis=1, keepdims=True) for i in range(2)]
            r_mean = (0.0625 * r_early + 0.25 * total_of((row_new[0] + row_new[1])[2 * t:2 * t + 2, :])) / VOCAB
            for i, value in enumerate((u_firsts[t] + total_of(acc), 0.25 * p_col, r_mean)):
                message = jnp.where(lane == 3 * t + i, value, message)
        s_own[...] = message
        s_in[chip] = message
        for z in range(4):
            for fy, fx, fc in ((1, 1, 1), (1, 1, 0), (0, 1, 1), (1, 0, 1), (0, 1, 0), (1, 0, 0), (0, 0, 1), (0, 0, 0)):
                def send_it(z=z, fy=fy, fx=fx, fc=fc):
                    remote(s_own, s_in.at[chip], send.at[9], last_r.at[1], (z, plane_id(fy, fx, fc)[1])).start()

                if fy + fx + fc:
                    send_it()
                else:
                    pl.when(model != z)(send_it)

        for q in late:
            row_fwd(q).start()

    for q in late:
        scale_own(q)

    factor_cols = []
    for t, c_out in enumerate((emb_cols_out, head_cols_out)):
        cols = m_sum[1, c, t:t + 1, :]
        col_new = BETA_TWO * old_cols[t, c] + (1.0 - BETA_TWO) * (cols[:, :COLS] / VOCAB)
        c_out[...] = col_new
        factor_cols.append(jnp.sum(jnp.where(diag[:, :COLS], lax.rsqrt(col_new), 0.0), axis=1, keepdims=True))

    @pl.loop(PAIRS - 3, PAIRS)
    def _(q):
        scale_peer(q)

    emb_rows_out[...] = rows[:, :2, :]
    head_rows_out[...] = rows[:, 2:, :]
    arrived(both_e.at[0], send.at[0])
    arrived(both_h.at[0], send.at[1])
    arrived(in1, send.at[2])
    arrived(in2, send.at[3])
    arrived(peer, send.at[4])
    arrived(rp_in, send.at[5])
    arrived(rows.at[0:PAIRS], send.at[6])
    arrived(m_in.at[0:7], send.at[7])
    arrived(old_cols.at[:, c], send.at[8])

    @pl.when(c == 0)
    def _():
        arrived(s_in.at[0:16], last_r.at[1])

    @pl.when(c == 1)
    def _():
        arrived(s_in.at[0:15], last_r.at[1])

    message = jnp.sum(s_in[0:16], axis=0)
    count = float(VOCAB * EMBED)
    for t in range(2):
        u_sq, p_sq, r_mean = [jnp.sum(jnp.where(lane == 3 * t + i, message, 0.0), axis=1, keepdims=True) for i in range(3)]
        u_rms = jnp.sqrt(u_sq * r_mean / count)
        p_rms = jnp.sqrt(p_sq / count)
        step = LEARN_RATE * jnp.maximum(SCALE_FLOOR, p_rms) / jnp.maximum(1.0, u_rms / CLIP_LIMIT)
        scale_out[t] = jnp.broadcast_to(factor_cols[t] * (step * jnp.sqrt(r_mean)), (COLS, LANES))

    @pl.when(c == 1)
    def _():
        arrived(s_in.at[0:31], send.at[9])


def update_kernel(emb_g, head_g, emb_p, head_p, emb_rows, head_rows, emb_cols, head_cols, scale,
                  emb_new, head_new, emb_rows_new, head_rows_new, emb_cols_new, head_cols_new, emb_half, head_half,
                  new_buf, half_buf, small_sem, big_sem):
    small = [pltpu.make_async_copy(src, dst, small_sem.at[i]) for i, (src, dst) in enumerate(
        ((emb_rows, emb_rows_new), (head_rows, head_rows_new), (emb_cols, emb_cols_new), (head_cols, head_cols_new)))]
    for cp in small:
        cp.start()
    size = ROWS // PARTS
    tables = ((emb_p, emb_g, emb_new, emb_half), (head_p, head_g, head_new, head_half))
    for i in range(PARTS):
        part = slice(i * size, (i + 1) * size)
        for t, (p, g, new, half) in enumerate(tables):
            value = p[:, part] - g[:, part] * scale[t, :, 0:1]
            new_buf[t, :, part] = value
            half_buf[t, :, part] = value.astype(jnp.bfloat16)
            pltpu.make_async_copy(new_buf.at[t, :, part], new.at[:, part], big_sem.at[0]).start()
            pltpu.make_async_copy(half_buf.at[t, :, part], half.at[:, part], big_sem.at[1]).start()
    for cp in small:
        cp.wait()
    pltpu.make_async_copy(new_buf, new_buf, big_sem.at[0]).wait()
    pltpu.make_async_copy(half_buf, half_buf, big_sem.at[1]).wait()


def local_step(emb_p, head_p, emb_g, head_g, emb_r, emb_c, head_r, head_c):
    f32 = jnp.float32
    n = CHUNKS
    dma = pltpu.SemaphoreType.DMA
    hbm = pl.BlockSpec(memory_space=pltpu.HBM)
    vmem = pl.BlockSpec(memory_space=pltpu.VMEM)
    rows_shape = (BLOCKS, 2, LANES)
    table = jax.ShapeDtypeStruct((COLS, ROWS), f32)
    half = jax.ShapeDtypeStruct((COLS, ROWS), jnp.bfloat16)
    emb_p = emb_p.T
    shapes = [(2, ROWS // 2, EMBED), (n, 2, 2, 2, COLS, LANES), (2, n, 2, 2, 2, COLS, LANES)]
    shapes += [(n, 2, 2, 2, COLS, LANES), (n, 2, 2, COLS, LANES), (PAIRS, 2, 2, COLS, LANES)]
    shapes += [(BLOCKS, 4, LANES), (2, *rows_shape), (2, 2, 1, COLS)]
    shapes += [(PAIRS, 4, LANES), (PAIRS, 3, 4, LANES)]
    shapes += [(2, 2, COLS, LANES)] * 2 + [(4, LANES), (2, LANES)]
    shapes += [(2, 2, 2, LANES), (8, 2, 2, 2, LANES), (2, 2, 2, LANES), (1, LANES), (32, 1, LANES)]
    scratch = [pltpu.VMEM(shape, f32) for shape in shapes]
    scratch += [dma((len(GROUPS) + 1,))] * 2 + [dma((RING,))] * 2 + [dma((SHORT,))] * 3
    scratch += [dma((10,)), dma((2,)), dma((5,)), pltpu.SemaphoreType.REGULAR((2,))]
    kept = [pltpu.VMEM((COLS, ROWS), f32)] * 4 + [pltpu.VMEM(rows_shape, f32)] * 2 + [pltpu.VMEM((1, COLS), f32)] * 2
    kept.append(pltpu.VMEM((2, COLS, LANES), f32))
    state = pl.pallas_call(
        exchange_kernel,
        out_shape=tuple(kept),
        in_specs=[hbm] * 8,
        out_specs=(vmem,) * 9,
        scratch_shapes=scratch,
        compiler_params=pltpu.CompilerParams(collective_id=0, has_side_effects=True, vmem_limit_bytes=60_000_000),
        name="exchange",
    )(emb_g.reshape(ROWS, EMBED), head_g.reshape(2, 2, 2, COLS, ROWS), emb_p, head_p,
      emb_r.reshape(rows_shape), head_r.reshape(rows_shape), emb_c.reshape(1, COLS), head_c.reshape(1, COLS))

    outs = pl.pallas_call(
        update_kernel,
        out_shape=(table, table, jax.ShapeDtypeStruct(rows_shape, f32), jax.ShapeDtypeStruct(rows_shape, f32),
                   jax.ShapeDtypeStruct((1, COLS), f32), jax.ShapeDtypeStruct((1, COLS), f32), half, half),
        in_specs=[vmem] * 9,
        out_specs=(hbm,) * 8,
        scratch_shapes=[pltpu.VMEM((2, COLS, ROWS), f32), pltpu.VMEM((2, COLS, ROWS), jnp.bfloat16),
                        dma((4,)), dma((2,))],
        compiler_params=pltpu.CompilerParams(vmem_limit_bytes=16 * 2 ** 20),
        name="update",
    )(*state)
    emb_new, head_new, emb_rn, head_rn, emb_cn, head_cn, emb_half, head_half = outs
    return (emb_new.T, head_new, emb_rn.reshape(ROWS), emb_cn.reshape(COLS), head_rn.reshape(ROWS),
            head_cn.reshape(COLS), emb_half.T, head_half)


def solution(mesh):
    arg_specs = (P("model", "data"), P("data", "model"), P("data", "model", None), P("data", None, "model"),
                 P("model"), P("data"), P("model"), P("data"))
    result_specs = (P("model", "data"), P("data", "model"), P("model"), P("data"), P("model"), P("data"),
                    P("model", "data"), P("data", "model"))
    mapped = jax.shard_map(local_step, mesh=mesh, in_specs=arg_specs, out_specs=result_specs, check_vma=False)

    def update_tables(emb_param, head_param, emb_grad, head_grad, emb_row, emb_col, head_row, head_col):
        return mapped(emb_param, head_param, emb_grad, head_grad, emb_row, emb_col, head_row, head_col)

    return update_tables
```

```python
import functools

import jax
import jax.numpy as jnp
from jax import lax
from jax.experimental import pallas as pl
from jax.experimental.pallas import tpu as pltpu
from jax.sharding import PartitionSpec as P

TRAIN_STEP = 10
DECAY_EXP = 0.8
EPS_ONE = 1e-30
CLIP_LIMIT = 1.0
SCALE_FLOOR = 1e-3
LEARN_RATE = float(TRAIN_STEP) ** -0.5
BETA_TWO = 1.0 - float(TRAIN_STEP) ** -DECAY_EXP

VOCAB = 16384
EMBED = 768
ROWS = VOCAB // 4
COLS = EMBED // 8
LANES = 128
CHUNKS = ROWS // 2 // LANES
GROUPS = ((0, 1), (1, 1), (2, 2), (4, 12))
PAIRS = CHUNKS // 2
BLOCKS = 2 * PAIRS
AHEAD = 2
RING = 6
SHORT = 4
SWAPS = 5
RELAY = 5
PARTS = 16
MESH = pl.DeviceIdType.MESH
PLANE = ((0, 1), (1, 0), (1, 1))


def exchange_kernel(emb_ref, head_ref, emb_p_ref, head_p_ref, emb_r_ref, head_r_ref, emb_c_ref, head_c_ref,
                    stage_e, stage_h, par_e, par_h, emb_rows_out, head_rows_out, emb_cols_out, head_cols_out, scale_out,
                    both_e, sum_e, both_h, in1, in2, peer,
                    rows, old_rows, old_cols, rp_own, rp_sum, rp_in, col_acc, t_acc, rsum, psum, m_own, m_in, m_sum, s_own, s_in,
                    s0e_r, s0h_r, s1_r, s2_r, swap_r, rp_r, ry_r, fw_r, send, last_r, in_sem, token):
    model = lax.axis_index("model")
    data = lax.axis_index("data")
    c = data % 2
    x = (data // 2) % 2
    y = data // 4
    oc, ox, oy = 1 - c, 1 - x, 1 - y

    def plane_id(fy, fx, fc):
        step = fy * (4 - 8 * y) + fx * (2 - 4 * x) + fc * (1 - 2 * c)
        return (model, data + step)

    def column_id(dz, fc):
        return ((model + dz) % 4, data + fc * (1 - 2 * c))

    core_peer, x_peer, y_peer = plane_id(0, 0, 1), plane_id(0, 1, 0), plane_id(1, 0, 0)

    def remote(src, dst, send_sem, recv_sem, peer_id):
        return pltpu.make_async_remote_copy(src_ref=src, dst_ref=dst, send_sem=send_sem, recv_sem=recv_sem,
                                            device_id=peer_id, device_id_type=MESH)

    def arrived(ref, sem):
        pltpu.make_async_copy(ref, ref, sem).wait()

    def vocab_at(core, first, count):
        return pl.ds(pl.multiple_of(core * (ROWS // 2) + first * LANES, LANES), count * LANES)

    half_of = 4 * COLS

    def first_e(q):
        cols = pl.ds(pl.multiple_of((oy if q == 0 else y) * half_of, LANES), half_of)
        return (pltpu.make_async_copy(emb_ref.at[vocab_at(c, 0, 1), cols], both_e.at[0, 0:LANES, cols], s0e_r.at[q]),
                remote(emb_ref.at[vocab_at(oc, 0, 1), cols], both_e.at[1, 0:LANES, cols], send.at[0], s0e_r.at[q], core_peer))

    def first_h(q):
        part = ox if q == 0 else x
        return (pltpu.make_async_copy(head_ref.at[:, part, :, :, vocab_at(c, 0, 1)], both_h.at[0, 0, :, part], s0h_r.at[q]),
                remote(head_ref.at[:, part, :, :, vocab_at(oc, 0, 1)], both_h.at[1, 0, :, part], send.at[1], s0h_r.at[q], core_peer))

    def group_e(i):
        first, count = GROUPS[i]
        at = slice(first * LANES, (first + count) * LANES)
        return (pltpu.make_async_copy(emb_ref.at[vocab_at(c, first, count), :], both_e.at[0, at, :], s0e_r.at[i + 1]),
                remote(emb_ref.at[vocab_at(oc, first, count), :], both_e.at[1, at, :], send.at[0], s0e_r.at[i + 1], core_peer))

    def group_h(i):
        first, count = GROUPS[i]
        pairs = []
        for j in range(first, first + count):
            pairs.append((pltpu.make_async_copy(head_ref.at[:, :, :, :, vocab_at(c, j, 1)], both_h.at[0, j], s0h_r.at[i + 1]),
                          remote(head_ref.at[:, :, :, :, vocab_at(oc, j, 1)], both_h.at[1, j], send.at[1], s0h_r.at[i + 1],
                                 core_peer)))
        return pairs

    def one_e(k):
        return remote(sum_e.at[k, oy], in1.at[k, 0], send.at[2], s1_r.at[k % RING], y_peer)

    def one_h(k):
        return remote(both_h.at[0, k, :, ox], in1.at[k, 1], send.at[2], s1_r.at[k % RING], x_peer)

    def two_e(k):
        return remote(in1.at[k, 0, ox], in2.at[k, 0], send.at[3], s2_r.at[k % RING], x_peer)

    def two_h(k):
        return remote(in1.at[k, 1, oy], in2.at[k, 1], send.at[3], s2_r.at[k % RING], y_peer)

    def swap(q):
        return [remote(in2.at[pl.ds(2 * q, 2), t, oc], peer.at[q, t], send.at[4], swap_r.at[q % SWAPS], core_peer)
                for t in range(2)]

    def row_msg(q, i):
        fy, fx = PLANE[i]
        return remote(rp_own.at[q], rp_in.at[3 * q + i], send.at[5], rp_r.at[q % SHORT], plane_id(fy, fx, 0))

    def sum_msg(q):
        return remote(rp_sum.at[q], rp_in.at[3 * q + 1], send.at[5], ry_r.at[q % SHORT], y_peer)

    def row_fwd(q):
        return remote(rows.at[c * PAIRS + q], rows.at[c * PAIRS + q], send.at[6], fw_r.at[q % SWAPS], core_peer)

    small_loads = [pltpu.make_async_copy(src, dst, in_sem.at[i]) for i, (src, dst) in (
        (0, (emb_p_ref, par_e)), (1, (head_p_ref, par_h)), (2, (emb_r_ref, old_rows.at[0])), (2, (head_r_ref, old_rows.at[1])),
        (3, (emb_c_ref, old_cols.at[0, c])), (3, (head_c_ref, old_cols.at[1, c])))]
    old_cols_out = [remote(src, old_cols.at[t, c], send.at[8], in_sem.at[4], core_peer)
                    for t, src in enumerate((emb_c_ref, head_c_ref))]

    barrier = pltpu.get_barrier_semaphore()
    above, below = column_id(1, 0), column_id(3, 0)
    for peer_id in (core_peer, x_peer, y_peer):
        pl.semaphore_signal(barrier, inc=1, device_id=peer_id, device_id_type=MESH)

    z_count = 1 + model * (3 - model) // 2

    def along_z(act):
        @pl.when(model < 3)
        def _():
            act(above)

        @pl.when(model > 0)
        def _():
            act(below)

    along_z(lambda peer_id: pl.semaphore_signal(barrier, inc=1, device_id=peer_id, device_id_type=MESH))
    for q in range(2):
        first_e(q)[0].start()
        first_h(q)[0].start()
    for i in range(1, len(GROUPS)):
        group_e(i)[0].start()
        for cp, _ in group_h(i):
            cp.start()
    pl.semaphore_wait(barrier, 3 + z_count)

    for q in range(2):
        first_e(q)[1].start()
        first_h(q)[1].start()
    for cp in old_cols_out:
        cp.start()
    for i in range(1, len(GROUPS)):
        group_e(i)[1].start()
        for _, cp in group_h(i):
            cp.start()
    for cp in small_loads:
        cp.start()
    along_z(lambda peer_id: pl.semaphore_signal(token.at[0], inc=1, device_id=peer_id, device_id_type=MESH))

    col_acc[...] = jnp.zeros_like(col_acc)
    t_acc[...] = jnp.zeros_like(t_acc)
    rsum[...] = jnp.zeros_like(rsum)
    psum[...] = jnp.zeros_like(psum)

    def flip_e(k, half):
        at = pl.ds(pl.multiple_of(k * LANES, LANES), LANES)
        for j in range(half_of // LANES):
            cols = pl.ds(pl.multiple_of(half * half_of + j * LANES, LANES), LANES)
            strip = (both_e[0, at, cols] + both_e[1, at, cols]).T
            done = 0
            while done < LANES:
                block, row = divmod(LANES * j + done, COLS)
                size = min(LANES - done, COLS - row)
                sum_e[k, half, block // 2, block % 2, row:row + size, :] = strip[done:done + size, :]
                done += size

    def add_h(k, part):
        for a in range(2):
            for b in range(2):
                both_h[0, k, a, part, b] = both_h[0, k, a, part, b] + both_h[1, k, a, part, b]

    def combine_cores(k):
        flip_e(k, oy)
        one_e(k).start()
        add_h(k, ox)
        one_h(k).start()
        flip_e(k, y)
        add_h(k, x)

    def first_sum(k):
        arrived(in1.at[k], s1_r.at[k % RING])
        in1[k, 0, ox] = in1[k, 0, ox] + sum_e[k, y, ox]
        two_e(k).start()
        in1[k, 1, oy] = in1[k, 1, oy] + both_h[0, k, oy, x]
        two_h(k).start()
        in1[k, 0, x] = in1[k, 0, x] + sum_e[k, y, x]
        in1[k, 1, y] = in1[k, 1, y] + both_h[0, k, y, x]

    def finish(k, q, i):
        arrived(in2.at[k], s2_r.at[k % RING])
        for t, mine in enumerate((x, y)):
            for core in range(2):
                in2[k, t, core] = in2[k, t, core] + in1[k, t, mine, core]
        for t in range(2):
            row_part = jnp.zeros((1, LANES), jnp.float32)
            for core in range(2):
                g = in2[k, t, core]
                sq = g * g + EPS_ONE
                col_acc[t, core] = col_acc[t, core] + sq
                row_part = row_part + jnp.sum(sq, axis=0, keepdims=True)
            rp_own[q, 2 * t + i:2 * t + i + 1, :] = row_part

    def send_rows(q):
        for i in (2, 1, 0):
            row_msg(q, i).start()

    def send_swap(q):
        for cp in swap(q):
            cp.start()

    def relay_rows(q):
        row_msg(q, 0).wait_recv()
        rp_sum[q] = rp_own[q] + rp_in[3 * q]
        sum_msg(q).start()

    def new_rows(q, relayed=False):
        if relayed:
            sum_msg(q).wait_recv()
        else:
            arrived(rp_in.at[pl.ds(3 * q, 3)], rp_r.at[q % SHORT])
        block = c * PAIRS + q
        if relayed:
            row_sq = rp_sum[q] + rp_in[3 * q + 1]
        else:
            row_sq = (rp_own[q] + rp_in[3 * q]) + (rp_in[3 * q + 1] + rp_in[3 * q + 2])
        old = jnp.concatenate([old_rows[0, block], old_rows[1, block]], axis=0)
        row_new = BETA_TWO * old + (1.0 - BETA_TWO) * (row_sq / EMBED)
        rows[block] = row_new
        return row_new

    def row_stats(q, relayed=False):
        row_new = new_rows(q, relayed)
        rsum[...] = rsum[...] + row_new
        inv = 1.0 / row_new
        for t in range(2):
            for core in range(2):
                acc = t_acc[t, core]
                for i in range(2):
                    g = in2[2 * q + i, t, core]
                    acc = acc + (g * g) * inv[2 * t + i:2 * t + i + 1, :]
                t_acc[t, core] = acc

    def scale_rows(block, get):
        factor = lax.rsqrt(rows[block])
        base = pl.multiple_of(block * (2 * LANES), 2 * LANES)
        for t, stage in enumerate((stage_e, stage_h)):
            for i in range(2):
                stage[:, pl.ds(base + i * LANES, LANES)] = get(t, i) * factor[2 * t + i:2 * t + i + 1, :]

    def scale_own(q):
        scale_rows(c * PAIRS + q, lambda t, i: in2[2 * q + i, t, c])

    def scale_peer(q):
        arrived(rows.at[oc * PAIRS + q], fw_r.at[q % SWAPS])
        arrived(peer.at[q], swap_r.at[q % SWAPS])
        scale_rows(oc * PAIRS + q, lambda t, i: peer[q, t, i])

    def param_sq(k):
        size = ROWS // CHUNKS * 2
        at = pl.ds(pl.multiple_of(k * size, size), size)
        for t, par in enumerate((par_e, par_h)):
            v = par[:, at]
            v = jnp.sum(v * v, axis=0, keepdims=True)
            for i in range(size // LANES):
                psum[t:t + 1, :] = psum[t:t + 1, :] + v[:, i * LANES:(i + 1) * LANES]

    for q in range(2):
        cols = pl.ds(pl.multiple_of((oy if q == 0 else y) * half_of, LANES), half_of)
        arrived(both_e.at[:, 0:LANES, cols], s0e_r.at[q])
        flip_e(0, oy if q == 0 else y)
        if q == 0:
            @pl.when(c == 0)
            def _():
                one_e(0).start()

        part = ox if q == 0 else x
        arrived(both_h.at[:, 0, :, part], s0h_r.at[q])
        add_h(0, part)
        if q == 0:
            @pl.when(c == 0)
            def _():
                one_h(0).start()

    def group_arrived(i):
        first, count = GROUPS[i]
        arrived(both_e.at[:, first * LANES:(first + count) * LANES, :], s0e_r.at[i + 1])
        arrived(both_h.at[:, first:first + count], s0h_r.at[i + 1])

    group_arrived(1)

    @pl.when(c == 0)
    def _():
        combine_cores(1)

    group_arrived(2)

    @pl.when(c == 1)
    def _():
        one_e(0).start()
        one_h(0).start()
        combine_cores(1)


    @pl.loop(0, CHUNKS)
    def _(k):
        for i in range(3, len(GROUPS)):
            @pl.when(k + AHEAD == GROUPS[i][0])
            def _():
                group_arrived(i)

        @pl.when(k + AHEAD < CHUNKS)
        def _():
            combine_cores(k + AHEAD)

        first_sum(k)
        pair = k // 2

        @pl.when(k == 1)
        def _():
            pl.semaphore_wait(token.at[0], z_count)
            along_z(lambda peer_id: pl.semaphore_signal(token.at[1], inc=1, device_id=peer_id, device_id_type=MESH))

        @pl.when(k == 2)
        def _():
            pl.semaphore_wait(token.at[1], z_count)

        @pl.when(k == 3)
        def _():
            arrived(par_e, in_sem.at[0])
            arrived(par_h, in_sem.at[1])
            arrived(old_rows, in_sem.at[2])

        @pl.when(k >= CHUNKS // 2)
        def _():
            param_sq(k - CHUNKS // 2)

        @pl.when((k >= 2) & (k % 2 == 0))
        def _():
            finish(k - 2, pair - 1, 0)

        @pl.when((k >= 3) & (k % 2 == 1))
        def _():
            finish(k - 2, pair - 1, 1)

            @pl.when(pair - 1 < RELAY)
            def _():
                row_msg(pair - 1, 0).start()

            @pl.when(pair - 1 >= RELAY)
            def _():
                send_rows(pair - 1)

            send_swap(pair - 1)

        @pl.when((k >= 9) & (k % 2 == 1))
        def _():
            scale_peer(pair - 4)

        @pl.when((k >= 5) & (k % 2 == 1) & (pair - 2 < RELAY))
        def _():
            relay_rows(pair - 2)

        @pl.when((k >= 7) & (k % 2 == 1))
        def _():
            row_stats(pair - 3, True)
            row_fwd(pair - 3).start()
            scale_own(pair - 3)

    row_stats(PAIRS - 3)
    row_fwd(PAIRS - 3).start()
    scale_own(PAIRS - 3)

    lane = lax.broadcasted_iota(jnp.int32, (1, LANES), 1)
    diag = lax.broadcasted_iota(jnp.int32, (COLS, LANES), 0) == lax.broadcasted_iota(jnp.int32, (COLS, LANES), 1)

    def as_row(acc):
        col = jnp.sum(acc, axis=1, keepdims=True)
        return jnp.sum(jnp.where(diag, col, 0.0), axis=0, keepdims=True)

    def total_of(v):
        return jnp.sum(jnp.sum(v, axis=0, keepdims=True), axis=1, keepdims=True)

    def to_column(kind):
        for z in range(4):
            for fc in (1, 0):
                def send_it(z=z, fc=fc):
                    remote(m_own.at[kind], m_in.at[2 * model + c, kind], send.at[7], last_r.at[0], (z, data + fc * (1 - 2 * c))).start()

                if fc:
                    send_it()
                else:
                    pl.when(model != z)(send_it)

    def send_weighted():
        for t in range(2):
            r_part = total_of(rsum[2 * t:2 * t + 2, :])
            p_part = jnp.sum(psum[t:t + 1, :], axis=1, keepdims=True)
            for core in range(2):
                row = as_row(t_acc[t, core])
                row = jnp.where(lane == COLS, r_part, jnp.where(lane == COLS + 1, p_part, row))
                m_own[0, core, t:t + 1, :] = row
        to_column(0)

    late = (PAIRS - 2, PAIRS - 1)

    pl.when(c == 1)(send_weighted)
    finish(CHUNKS - 2, PAIRS - 1, 0)
    finish(CHUNKS - 1, PAIRS - 1, 1)
    send_rows(PAIRS - 1)
    for t in range(2):
        for core in range(2):
            m_own[1, core, t:t + 1, :] = as_row(col_acc[t, core])
    to_column(1)
    send_swap(PAIRS - 1)

    @pl.when(c == 0)
    def _():
        for q in late:
            row_stats(q)
            row_fwd(q).start()
        send_weighted()

    m_in[2 * model + c] = m_own[...]
    arrived(old_cols.at[:, c], in_sem.at[3])
    arrived(old_cols.at[:, oc], in_sem.at[4])
    arrived(m_in.at[0:7], last_r.at[0])
    m_sum[...] = jnp.sum(m_in[...], axis=0)
    chip = 4 * model + data // 2

    @pl.when(c == 1)
    def _():
        message = jnp.zeros((1, LANES), jnp.float32)
        u_firsts, weights = [], []
        for t in range(2):
            u_first = jnp.zeros((1, COLS), jnp.float32)
            for core in range(2):
                col_new = BETA_TWO * old_cols[t, core] + (1.0 - BETA_TWO) * (m_sum[1, core, t:t + 1, :COLS] / VOCAB)
                weight = 1.0 / col_new
                u_first = u_first + m_sum[0, core, t:t + 1, :COLS] * weight
                weights.append(jnp.sum(jnp.where(diag[:, :COLS], weight, 0.0), axis=1, keepdims=True))
            u_firsts.append(0.25 * jnp.sum(u_first, axis=1, keepdims=True))
        row_new = [new_rows(q) for q in late]
        inv = [1.0 / r for r in row_new]
        for t in range(2):
            acc = jnp.zeros((COLS, LANES), jnp.float32)
            for core in range(2):
                part = jnp.zeros((COLS, LANES), jnp.float32)
                for q, r in zip(late, inv):
                    for i in range(2):
                        g = in2[2 * q + i, t, core]
                        part = part + (g * g) * r[2 * t + i:2 * t + i + 1, :]
                acc = acc + part * weights[2 * t + core]
            r_early, p_col = [jnp.sum(jnp.where(lane == COLS + i, m_sum[0, 0, t:t + 1, :], 0.0), axis=1, keepdims=True) for i in range(2)]
            r_mean = (0.0625 * r_early + 0.25 * total_of((row_new[0] + row_new[1])[2 * t:2 * t + 2, :])) / VOCAB
            for i, value in enumerate((u_firsts[t] + total_of(acc), 0.25 * p_col, r_mean)):
                message = jnp.where(lane == 3 * t + i, value, message)
        s_own[...] = message
        s_in[chip] = message
        for z in range(4):
            for fy, fx, fc in ((1, 1, 1), (1, 1, 0), (0, 1, 1), (1, 0, 1), (0, 1, 0), (1, 0, 0), (0, 0, 1), (0, 0, 0)):
                def send_it(z=z, fy=fy, fx=fx, fc=fc):
                    remote(s_own, s_in.at[chip], send.at[9], last_r.at[1], (z, plane_id(fy, fx, fc)[1])).start()

                if fy + fx + fc:
                    send_it()
                else:
                    pl.when(model != z)(send_it)

        for q in late:
            row_fwd(q).start()

    for q in late:
        scale_own(q)

    factor_cols = []
    for t, c_out in enumerate((emb_cols_out, head_cols_out)):
        cols = m_sum[1, c, t:t + 1, :]
        col_new = BETA_TWO * old_cols[t, c] + (1.0 - BETA_TWO) * (cols[:, :COLS] / VOCAB)
        c_out[...] = col_new
        factor_cols.append(jnp.sum(jnp.where(diag[:, :COLS], lax.rsqrt(col_new), 0.0), axis=1, keepdims=True))

    @pl.loop(PAIRS - 4, PAIRS)
    def _(q):
        scale_peer(q)

    emb_rows_out[...] = rows[:, :2, :]
    head_rows_out[...] = rows[:, 2:, :]
    arrived(both_e.at[0], send.at[0])
    arrived(both_h.at[0], send.at[1])
    arrived(in1, send.at[2])
    arrived(in2, send.at[3])
    arrived(peer, send.at[4])
    arrived(rp_in.at[0:2 * RELAY + 3 * (PAIRS - RELAY)], send.at[5])
    arrived(rows.at[0:PAIRS], send.at[6])
    arrived(m_in.at[0:7], send.at[7])
    arrived(old_cols.at[:, c], send.at[8])

    @pl.when(c == 0)
    def _():
        arrived(s_in.at[0:16], last_r.at[1])

    @pl.when(c == 1)
    def _():
        arrived(s_in.at[0:15], last_r.at[1])

    message = jnp.sum(s_in[0:16], axis=0)
    count = float(VOCAB * EMBED)
    for t in range(2):
        u_sq, p_sq, r_mean = [jnp.sum(jnp.where(lane == 3 * t + i, message, 0.0), axis=1, keepdims=True) for i in range(3)]
        u_rms = jnp.sqrt(u_sq * r_mean / count)
        p_rms = jnp.sqrt(p_sq / count)
        step = LEARN_RATE * jnp.maximum(SCALE_FLOOR, p_rms) / jnp.maximum(1.0, u_rms / CLIP_LIMIT)
        scale_out[t] = jnp.broadcast_to(factor_cols[t] * (step * jnp.sqrt(r_mean)), (COLS, LANES))

    @pl.when(c == 1)
    def _():
        arrived(s_in.at[0:31], send.at[9])


def update_kernel(emb_g, head_g, emb_p, head_p, emb_rows, head_rows, emb_cols, head_cols, scale,
                  emb_new, head_new, emb_rows_new, head_rows_new, emb_cols_new, head_cols_new, emb_half, head_half,
                  new_buf, half_buf, small_sem, big_sem):
    small = [pltpu.make_async_copy(src, dst, small_sem.at[i]) for i, (src, dst) in enumerate(
        ((emb_rows, emb_rows_new), (head_rows, head_rows_new), (emb_cols, emb_cols_new), (head_cols, head_cols_new)))]
    for cp in small:
        cp.start()
    size = ROWS // PARTS
    tables = ((emb_p, emb_g, emb_new, emb_half), (head_p, head_g, head_new, head_half))
    for i in range(PARTS):
        part = slice(i * size, (i + 1) * size)
        for t, (p, g, new, half) in enumerate(tables):
            value = p[:, part] - g[:, part] * scale[t, :, 0:1]
            new_buf[t, :, part] = value
            half_buf[t, :, part] = value.astype(jnp.bfloat16)
            pltpu.make_async_copy(new_buf.at[t, :, part], new.at[:, part], big_sem.at[0]).start()
            pltpu.make_async_copy(half_buf.at[t, :, part], half.at[:, part], big_sem.at[1]).start()
    for cp in small:
        cp.wait()
    pltpu.make_async_copy(new_buf, new_buf, big_sem.at[0]).wait()
    pltpu.make_async_copy(half_buf, half_buf, big_sem.at[1]).wait()


def local_step(emb_p, head_p, emb_g, head_g, emb_r, emb_c, head_r, head_c):
    f32 = jnp.float32
    n = CHUNKS
    dma = pltpu.SemaphoreType.DMA
    hbm = pl.BlockSpec(memory_space=pltpu.HBM)
    vmem = pl.BlockSpec(memory_space=pltpu.VMEM)
    rows_shape = (BLOCKS, 2, LANES)
    table = jax.ShapeDtypeStruct((COLS, ROWS), f32)
    half = jax.ShapeDtypeStruct((COLS, ROWS), jnp.bfloat16)
    emb_p = emb_p.T
    shapes = [(2, ROWS // 2, EMBED), (n, 2, 2, 2, COLS, LANES), (2, n, 2, 2, 2, COLS, LANES)]
    shapes += [(n, 2, 2, 2, COLS, LANES), (n, 2, 2, COLS, LANES), (PAIRS, 2, 2, COLS, LANES)]
    shapes += [(BLOCKS, 4, LANES), (2, *rows_shape), (2, 2, 1, COLS)]
    shapes += [(PAIRS, 4, LANES), (PAIRS, 4, LANES), (3 * PAIRS, 4, LANES)]
    shapes += [(2, 2, COLS, LANES)] * 2 + [(4, LANES), (2, LANES)]
    shapes += [(2, 2, 2, LANES), (8, 2, 2, 2, LANES), (2, 2, 2, LANES), (1, LANES), (32, 1, LANES)]
    scratch = [pltpu.VMEM(shape, f32) for shape in shapes]
    scratch += [dma((len(GROUPS) + 1,))] * 2 + [dma((RING,))] * 2 + [dma((SWAPS,))] + [dma((SHORT,))] * 2 + [dma((SWAPS,))]
    scratch += [dma((10,)), dma((2,)), dma((5,)), pltpu.SemaphoreType.REGULAR((2,))]
    kept = [pltpu.VMEM((COLS, ROWS), f32)] * 4 + [pltpu.VMEM(rows_shape, f32)] * 2 + [pltpu.VMEM((1, COLS), f32)] * 2
    kept.append(pltpu.VMEM((2, COLS, LANES), f32))
    state = pl.pallas_call(
        exchange_kernel,
        out_shape=tuple(kept),
        in_specs=[hbm] * 8,
        out_specs=(vmem,) * 9,
        scratch_shapes=scratch,
        compiler_params=pltpu.CompilerParams(collective_id=0, has_side_effects=True, vmem_limit_bytes=60_000_000),
        name="exchange",
    )(emb_g.reshape(ROWS, EMBED), head_g.reshape(2, 2, 2, COLS, ROWS), emb_p, head_p,
      emb_r.reshape(rows_shape), head_r.reshape(rows_shape), emb_c.reshape(1, COLS), head_c.reshape(1, COLS))

    outs = pl.pallas_call(
        update_kernel,
        out_shape=(table, table, jax.ShapeDtypeStruct(rows_shape, f32), jax.ShapeDtypeStruct(rows_shape, f32),
                   jax.ShapeDtypeStruct((1, COLS), f32), jax.ShapeDtypeStruct((1, COLS), f32), half, half),
        in_specs=[vmem] * 9,
        out_specs=(hbm,) * 8,
        scratch_shapes=[pltpu.VMEM((2, COLS, ROWS), f32), pltpu.VMEM((2, COLS, ROWS), jnp.bfloat16),
                        dma((4,)), dma((2,))],
        compiler_params=pltpu.CompilerParams(vmem_limit_bytes=16 * 2 ** 20),
        name="update",
    )(*state)
    emb_new, head_new, emb_rn, head_rn, emb_cn, head_cn, emb_half, head_half = outs
    return (emb_new.T, head_new, emb_rn.reshape(ROWS), emb_cn.reshape(COLS), head_rn.reshape(ROWS),
            head_cn.reshape(COLS), emb_half.T, head_half)


def solution(mesh):
    arg_specs = (P("model", "data"), P("data", "model"), P("data", "model", None), P("data", None, "model"),
                 P("model"), P("data"), P("model"), P("data"))
    result_specs = (P("model", "data"), P("data", "model"), P("model"), P("data"), P("model"), P("data"),
                    P("model", "data"), P("data", "model"))
    mapped = jax.shard_map(local_step, mesh=mesh, in_specs=arg_specs, out_specs=result_specs, check_vma=False)

    def update_tables(emb_param, head_param, emb_grad, head_grad, emb_row, emb_col, head_row, head_col):
        return mapped(emb_param, head_param, emb_grad, head_grad, emb_row, emb_col, head_row, head_col)

    return update_tables
```

```python
import functools

import jax
import jax.numpy as jnp
from jax import lax
from jax.experimental import pallas as pl
from jax.experimental.pallas import tpu as pltpu
from jax.sharding import PartitionSpec as P

TRAIN_STEP = 10
DECAY_EXP = 0.8
EPS_ONE = 1e-30
CLIP_LIMIT = 1.0
SCALE_FLOOR = 1e-3
LEARN_RATE = float(TRAIN_STEP) ** -0.5
BETA_TWO = 1.0 - float(TRAIN_STEP) ** -DECAY_EXP

VOCAB = 16384
EMBED = 768
ROWS = VOCAB // 4
COLS = EMBED // 8
LANES = 128
CHUNKS = ROWS // 2 // LANES
GROUPS = ((0, 1), (1, 1), (2, 2), (4, 12))
PAIRS = CHUNKS // 2
BLOCKS = 2 * PAIRS
AHEAD = 2
RING = 6
SHORT = 4
SWAPS = 5
RELAY = 5
PARTS = 32
MESH = pl.DeviceIdType.MESH
PLANE = ((0, 1), (1, 0), (1, 1))


def exchange_kernel(emb_ref, head_ref, emb_p_ref, head_p_ref, emb_r_ref, head_r_ref, emb_c_ref, head_c_ref,
                    stage_e, stage_h, par_e, par_h, emb_rows_out, head_rows_out, emb_cols_out, head_cols_out, scale_out,
                    both_e, sum_e, both_h, in1, in2, peer,
                    rows, old_rows, old_cols, rp_own, rp_sum, rp_in, col_acc, t_acc, rsum, psum, m_own, m_in, m_sum, s_own, s_in,
                    s0e_r, s0h_r, s1_r, s2_r, swap_r, rp_r, ry_r, fw_r, send, last_r, in_sem, token):
    model = lax.axis_index("model")
    data = lax.axis_index("data")
    c = data % 2
    x = (data // 2) % 2
    y = data // 4
    oc, ox, oy = 1 - c, 1 - x, 1 - y

    def plane_id(fy, fx, fc):
        step = fy * (4 - 8 * y) + fx * (2 - 4 * x) + fc * (1 - 2 * c)
        return (model, data + step)

    def column_id(dz, fc):
        return ((model + dz) % 4, data + fc * (1 - 2 * c))

    core_peer, x_peer, y_peer = plane_id(0, 0, 1), plane_id(0, 1, 0), plane_id(1, 0, 0)

    def remote(src, dst, send_sem, recv_sem, peer_id):
        return pltpu.make_async_remote_copy(src_ref=src, dst_ref=dst, send_sem=send_sem, recv_sem=recv_sem,
                                            device_id=peer_id, device_id_type=MESH)

    def arrived(ref, sem):
        pltpu.make_async_copy(ref, ref, sem).wait()

    def vocab_at(core, first, count):
        return pl.ds(pl.multiple_of(core * (ROWS // 2) + first * LANES, LANES), count * LANES)

    half_of = 4 * COLS

    def first_e(q):
        cols = pl.ds(pl.multiple_of((oy if q == 0 else y) * half_of, LANES), half_of)
        return (pltpu.make_async_copy(emb_ref.at[vocab_at(c, 0, 1), cols], both_e.at[0, 0:LANES, cols], s0e_r.at[q]),
                remote(emb_ref.at[vocab_at(oc, 0, 1), cols], both_e.at[1, 0:LANES, cols], send.at[0], s0e_r.at[q], core_peer))

    def first_h(q):
        part = ox if q == 0 else x
        return (pltpu.make_async_copy(head_ref.at[:, part, :, :, vocab_at(c, 0, 1)], both_h.at[0, 0, :, part], s0h_r.at[q]),
                remote(head_ref.at[:, part, :, :, vocab_at(oc, 0, 1)], both_h.at[1, 0, :, part], send.at[1], s0h_r.at[q], core_peer))

    def group_e(i):
        first, count = GROUPS[i]
        at = slice(first * LANES, (first + count) * LANES)
        return (pltpu.make_async_copy(emb_ref.at[vocab_at(c, first, count), :], both_e.at[0, at, :], s0e_r.at[i + 1]),
                remote(emb_ref.at[vocab_at(oc, first, count), :], both_e.at[1, at, :], send.at[0], s0e_r.at[i + 1], core_peer))

    def group_h(i):
        first, count = GROUPS[i]
        pairs = []
        for j in range(first, first + count):
            pairs.append((pltpu.make_async_copy(head_ref.at[:, :, :, :, vocab_at(c, j, 1)], both_h.at[0, j], s0h_r.at[i + 1]),
                          remote(head_ref.at[:, :, :, :, vocab_at(oc, j, 1)], both_h.at[1, j], send.at[1], s0h_r.at[i + 1],
                                 core_peer)))
        return pairs

    def one_e(k):
        return remote(sum_e.at[k, oy], in1.at[k, 0], send.at[2], s1_r.at[k % RING], y_peer)

    def one_h(k):
        return remote(both_h.at[0, k, :, ox], in1.at[k, 1], send.at[2], s1_r.at[k % RING], x_peer)

    def two_e(k):
        return remote(in1.at[k, 0, ox], in2.at[k, 0], send.at[3], s2_r.at[k % RING], x_peer)

    def two_h(k):
        return remote(in1.at[k, 1, oy], in2.at[k, 1], send.at[3], s2_r.at[k % RING], y_peer)

    def swap(q):
        return [remote(in2.at[pl.ds(2 * q, 2), t, oc], peer.at[q, t], send.at[4], swap_r.at[q % SWAPS], core_peer)
                for t in range(2)]

    def row_msg(q, i):
        fy, fx = PLANE[i]
        return remote(rp_own.at[q], rp_in.at[3 * q + i], send.at[5], rp_r.at[q % SHORT], plane_id(fy, fx, 0))

    def sum_msg(q):
        return remote(rp_sum.at[q], rp_in.at[3 * q + 1], send.at[5], ry_r.at[q % SHORT], y_peer)

    def row_fwd(q):
        return remote(rows.at[c * PAIRS + q], rows.at[c * PAIRS + q], send.at[6], fw_r.at[q % SWAPS], core_peer)

    small_loads = [pltpu.make_async_copy(src, dst, in_sem.at[i]) for i, (src, dst) in (
        (0, (emb_p_ref, par_e)), (1, (head_p_ref, par_h)), (2, (emb_r_ref, old_rows.at[0])), (2, (head_r_ref, old_rows.at[1])),
        (3, (emb_c_ref, old_cols.at[0, c])), (3, (head_c_ref, old_cols.at[1, c])))]
    old_cols_out = [remote(src, old_cols.at[t, c], send.at[8], in_sem.at[3], core_peer)
                    for t, src in enumerate((emb_c_ref, head_c_ref))]

    barrier = pltpu.get_barrier_semaphore()
    above, below = column_id(1, 0), column_id(3, 0)
    for peer_id in (core_peer, x_peer, y_peer):
        pl.semaphore_signal(barrier, inc=1, device_id=peer_id, device_id_type=MESH)

    z_count = 1 + model * (3 - model) // 2

    def along_z(act):
        @pl.when(model < 3)
        def _():
            act(above)

        @pl.when(model > 0)
        def _():
            act(below)

    along_z(lambda peer_id: pl.semaphore_signal(barrier, inc=1, device_id=peer_id, device_id_type=MESH))
    for q in range(2):
        first_e(q)[0].start()
        first_h(q)[0].start()
    for i in range(1, len(GROUPS)):
        group_e(i)[0].start()
        for cp, _ in group_h(i):
            cp.start()
    pl.semaphore_wait(barrier, 3 + z_count)

    for q in range(2):
        first_e(q)[1].start()
        first_h(q)[1].start()
    for cp in old_cols_out:
        cp.start()
    for i in range(1, len(GROUPS)):
        group_e(i)[1].start()
        for _, cp in group_h(i):
            cp.start()
    for cp in small_loads:
        cp.start()
    along_z(lambda peer_id: pl.semaphore_signal(token.at[0], inc=1, device_id=peer_id, device_id_type=MESH))

    col_acc[...] = jnp.zeros_like(col_acc)
    t_acc[...] = jnp.zeros_like(t_acc)
    rsum[...] = jnp.zeros_like(rsum)
    psum[...] = jnp.zeros_like(psum)

    def flip_e(k, half):
        at = pl.ds(pl.multiple_of(k * LANES, LANES), LANES)
        for j in range(half_of // LANES):
            cols = pl.ds(pl.multiple_of(half * half_of + j * LANES, LANES), LANES)
            strip = (both_e[0, at, cols] + both_e[1, at, cols]).T
            done = 0
            while done < LANES:
                block, row = divmod(LANES * j + done, COLS)
                size = min(LANES - done, COLS - row)
                sum_e[k, half, block // 2, block % 2, row:row + size, :] = strip[done:done + size, :]
                done += size

    def add_h(k, part):
        for a in range(2):
            for b in range(2):
                both_h[0, k, a, part, b] = both_h[0, k, a, part, b] + both_h[1, k, a, part, b]

    def combine_cores(k):
        flip_e(k, oy)
        one_e(k).start()
        add_h(k, ox)
        one_h(k).start()
        flip_e(k, y)
        add_h(k, x)

    def first_sum(k):
        arrived(in1.at[k], s1_r.at[k % RING])
        in1[k, 0, ox] = in1[k, 0, ox] + sum_e[k, y, ox]
        two_e(k).start()
        in1[k, 1, oy] = in1[k, 1, oy] + both_h[0, k, oy, x]
        two_h(k).start()
        in1[k, 0, x] = in1[k, 0, x] + sum_e[k, y, x]
        in1[k, 1, y] = in1[k, 1, y] + both_h[0, k, y, x]

    def finish(k, q, i):
        arrived(in2.at[k], s2_r.at[k % RING])
        for t, mine in enumerate((x, y)):
            for core in range(2):
                in2[k, t, core] = in2[k, t, core] + in1[k, t, mine, core]
        for t in range(2):
            row_part = jnp.zeros((1, LANES), jnp.float32)
            for core in range(2):
                g = in2[k, t, core]
                sq = g * g + EPS_ONE
                col_acc[t, core] = col_acc[t, core] + sq
                row_part = row_part + jnp.sum(sq, axis=0, keepdims=True)
            rp_own[q, 2 * t + i:2 * t + i + 1, :] = row_part

    def send_rows(q):
        for i in (2, 1, 0):
            row_msg(q, i).start()

    def send_swap(q):
        for cp in swap(q):
            cp.start()

    def relay_rows(q):
        row_msg(q, 0).wait_recv()
        rp_sum[q] = rp_own[q] + rp_in[3 * q]
        sum_msg(q).start()

    def new_rows(q, relayed=False):
        if relayed:
            sum_msg(q).wait_recv()
        else:
            arrived(rp_in.at[pl.ds(3 * q, 3)], rp_r.at[q % SHORT])
        block = c * PAIRS + q
        if relayed:
            row_sq = rp_sum[q] + rp_in[3 * q + 1]
        else:
            row_sq = (rp_own[q] + rp_in[3 * q]) + (rp_in[3 * q + 1] + rp_in[3 * q + 2])
        old = jnp.concatenate([old_rows[0, block], old_rows[1, block]], axis=0)
        row_new = BETA_TWO * old + (1.0 - BETA_TWO) * (row_sq / EMBED)
        rows[block] = row_new
        return row_new

    def row_stats(q, relayed=False):
        row_new = new_rows(q, relayed)
        rsum[...] = rsum[...] + row_new
        inv = 1.0 / row_new
        for t in range(2):
            for core in range(2):
                acc = t_acc[t, core]
                for i in range(2):
                    g = in2[2 * q + i, t, core]
                    acc = acc + (g * g) * inv[2 * t + i:2 * t + i + 1, :]
                t_acc[t, core] = acc

    def scale_rows(block, get):
        factor = lax.rsqrt(rows[block])
        base = pl.multiple_of(block * (2 * LANES), 2 * LANES)
        for t, stage in enumerate((stage_e, stage_h)):
            for i in range(2):
                stage[:, pl.ds(base + i * LANES, LANES)] = get(t, i) * factor[2 * t + i:2 * t + i + 1, :]

    def scale_own(q):
        scale_rows(c * PAIRS + q, lambda t, i: in2[2 * q + i, t, c])

    def scale_peer(q):
        arrived(rows.at[oc * PAIRS + q], fw_r.at[q % SWAPS])
        arrived(peer.at[q], swap_r.at[q % SWAPS])
        scale_rows(oc * PAIRS + q, lambda t, i: peer[q, t, i])

    def param_sq(k):
        size = ROWS // CHUNKS * 2
        at = pl.ds(pl.multiple_of(k * size, size), size)
        for t, par in enumerate((par_e, par_h)):
            v = par[:, at]
            v = jnp.sum(v * v, axis=0, keepdims=True)
            for i in range(size // LANES):
                psum[t:t + 1, :] = psum[t:t + 1, :] + v[:, i * LANES:(i + 1) * LANES]

    for q in range(2):
        cols = pl.ds(pl.multiple_of((oy if q == 0 else y) * half_of, LANES), half_of)
        arrived(both_e.at[:, 0:LANES, cols], s0e_r.at[q])
        flip_e(0, oy if q == 0 else y)
        if q == 0:
            @pl.when(c == 0)
            def _():
                one_e(0).start()

        part = ox if q == 0 else x
        arrived(both_h.at[:, 0, :, part], s0h_r.at[q])
        add_h(0, part)
        if q == 0:
            @pl.when(c == 0)
            def _():
                one_h(0).start()

    def group_arrived(i):
        first, count = GROUPS[i]
        arrived(both_e.at[:, first * LANES:(first + count) * LANES, :], s0e_r.at[i + 1])
        arrived(both_h.at[:, first:first + count], s0h_r.at[i + 1])

    group_arrived(1)

    @pl.when(c == 0)
    def _():
        combine_cores(1)

    group_arrived(2)

    @pl.when(c == 1)
    def _():
        one_e(0).start()
        one_h(0).start()
        combine_cores(1)


    @pl.loop(0, CHUNKS)
    def _(k):
        for i in range(3, len(GROUPS)):
            @pl.when(k + AHEAD == GROUPS[i][0])
            def _():
                group_arrived(i)

        @pl.when(k + AHEAD < CHUNKS)
        def _():
            combine_cores(k + AHEAD)

        first_sum(k)
        pair = k // 2

        @pl.when(k == 1)
        def _():
            pl.semaphore_wait(token.at[0], z_count)
            along_z(lambda peer_id: pl.semaphore_signal(token.at[1], inc=1, device_id=peer_id, device_id_type=MESH))

        @pl.when(k == 2)
        def _():
            pl.semaphore_wait(token.at[1], z_count)

        @pl.when(k == 3)
        def _():
            arrived(par_e, in_sem.at[0])
            arrived(par_h, in_sem.at[1])
            arrived(old_rows, in_sem.at[2])

        @pl.when(k >= CHUNKS // 2)
        def _():
            param_sq(k - CHUNKS // 2)

        @pl.when((k >= 2) & (k % 2 == 0))
        def _():
            finish(k - 2, pair - 1, 0)

        @pl.when((k >= 3) & (k % 2 == 1))
        def _():
            finish(k - 2, pair - 1, 1)

            @pl.when(pair - 1 < RELAY)
            def _():
                row_msg(pair - 1, 0).start()

            @pl.when(pair - 1 >= RELAY)
            def _():
                send_rows(pair - 1)

            send_swap(pair - 1)

        @pl.when((k >= 9) & (k % 2 == 1))
        def _():
            scale_peer(pair - 4)

        @pl.when((k >= 5) & (k % 2 == 1) & (pair - 2 < RELAY))
        def _():
            relay_rows(pair - 2)

        @pl.when((k >= 7) & (k % 2 == 1))
        def _():
            row_stats(pair - 3, True)
            row_fwd(pair - 3).start()
            scale_own(pair - 3)

    row_stats(PAIRS - 3)
    row_fwd(PAIRS - 3).start()
    scale_own(PAIRS - 3)

    lane = lax.broadcasted_iota(jnp.int32, (1, LANES), 1)
    diag = lax.broadcasted_iota(jnp.int32, (COLS, LANES), 0) == lax.broadcasted_iota(jnp.int32, (COLS, LANES), 1)

    def as_row(acc):
        col = jnp.sum(acc, axis=1, keepdims=True)
        return jnp.sum(jnp.where(diag, col, 0.0), axis=0, keepdims=True)

    def total_of(v):
        return jnp.sum(jnp.sum(v, axis=0, keepdims=True), axis=1, keepdims=True)

    def to_column(kind):
        for z in range(4):
            for fc in (1, 0):
                def send_it(z=z, fc=fc):
                    remote(m_own.at[kind], m_in.at[2 * model + c, kind], send.at[7], last_r.at[0], (z, data + fc * (1 - 2 * c))).start()

                if fc:
                    send_it()
                else:
                    pl.when(model != z)(send_it)

    def send_weighted():
        for t in range(2):
            r_part = total_of(rsum[2 * t:2 * t + 2, :])
            p_part = jnp.sum(psum[t:t + 1, :], axis=1, keepdims=True)
            for core in range(2):
                row = as_row(t_acc[t, core])
                row = jnp.where(lane == COLS, r_part, jnp.where(lane == COLS + 1, p_part, row))
                m_own[0, core, t:t + 1, :] = row
        to_column(0)

    late = (PAIRS - 2, PAIRS - 1)

    pl.when(c == 1)(send_weighted)
    finish(CHUNKS - 2, PAIRS - 1, 0)
    finish(CHUNKS - 1, PAIRS - 1, 1)
    send_rows(PAIRS - 1)
    for t in range(2):
        for core in range(2):
            m_own[1, core, t:t + 1, :] = as_row(col_acc[t, core])
    to_column(1)
    send_swap(PAIRS - 1)

    @pl.when(c == 0)
    def _():
        for q in late:
            row_stats(q)
            row_fwd(q).start()
        send_weighted()

    m_in[2 * model + c] = m_own[...]
    arrived(old_cols, in_sem.at[3])
    arrived(m_in.at[0:7], last_r.at[0])
    m_sum[...] = jnp.sum(m_in[...], axis=0)
    chip = 4 * model + data // 2

    @pl.when(c == 1)
    def _():
        message = jnp.zeros((1, LANES), jnp.float32)
        u_firsts, weights = [], []
        for t in range(2):
            u_first = jnp.zeros((1, COLS), jnp.float32)
            for core in range(2):
                col_new = BETA_TWO * old_cols[t, core] + (1.0 - BETA_TWO) * (m_sum[1, core, t:t + 1, :COLS] / VOCAB)
                weight = 1.0 / col_new
                u_first = u_first + m_sum[0, core, t:t + 1, :COLS] * weight
                weights.append(jnp.sum(jnp.where(diag[:, :COLS], weight, 0.0), axis=1, keepdims=True))
            u_firsts.append(0.25 * jnp.sum(u_first, axis=1, keepdims=True))
        row_new = [new_rows(q) for q in late]
        inv = [1.0 / r for r in row_new]
        for t in range(2):
            acc = jnp.zeros((COLS, LANES), jnp.float32)
            for core in range(2):
                part = jnp.zeros((COLS, LANES), jnp.float32)
                for q, r in zip(late, inv):
                    for i in range(2):
                        g = in2[2 * q + i, t, core]
                        part = part + (g * g) * r[2 * t + i:2 * t + i + 1, :]
                acc = acc + part * weights[2 * t + core]
            r_early, p_col = [jnp.sum(jnp.where(lane == COLS + i, m_sum[0, 0, t:t + 1, :], 0.0), axis=1, keepdims=True) for i in range(2)]
            r_mean = (0.0625 * r_early + 0.25 * total_of((row_new[0] + row_new[1])[2 * t:2 * t + 2, :])) / VOCAB
            for i, value in enumerate((u_firsts[t] + total_of(acc), 0.25 * p_col, r_mean)):
                message = jnp.where(lane == 3 * t + i, value, message)
        s_own[...] = message
        s_in[chip] = message
        for z in range(4):
            for fy, fx, fc in ((1, 1, 1), (1, 1, 0), (0, 1, 1), (1, 0, 1), (0, 1, 0), (1, 0, 0), (0, 0, 1), (0, 0, 0)):
                def send_it(z=z, fy=fy, fx=fx, fc=fc):
                    remote(s_own, s_in.at[chip], send.at[9], last_r.at[1], (z, plane_id(fy, fx, fc)[1])).start()

                if fy + fx + fc:
                    send_it()
                else:
                    pl.when(model != z)(send_it)

        for q in late:
            row_fwd(q).start()

    for q in late:
        scale_own(q)

    factor_cols = []
    for t, c_out in enumerate((emb_cols_out, head_cols_out)):
        cols = m_sum[1, c, t:t + 1, :]
        col_new = BETA_TWO * old_cols[t, c] + (1.0 - BETA_TWO) * (cols[:, :COLS] / VOCAB)
        c_out[...] = col_new
        factor_cols.append(jnp.sum(jnp.where(diag[:, :COLS], lax.rsqrt(col_new), 0.0), axis=1, keepdims=True))

    @pl.loop(PAIRS - 4, PAIRS)
    def _(q):
        scale_peer(q)

    emb_rows_out[...] = rows[:, :2, :]
    head_rows_out[...] = rows[:, 2:, :]
    arrived(both_e.at[0], send.at[0])
    arrived(both_h.at[0], send.at[1])
    arrived(in1, send.at[2])
    arrived(in2, send.at[3])
    arrived(peer, send.at[4])
    arrived(rp_in.at[0:2 * RELAY + 3 * (PAIRS - RELAY)], send.at[5])
    arrived(rows.at[0:PAIRS], send.at[6])
    arrived(m_in.at[0:7], send.at[7])
    arrived(old_cols.at[:, c], send.at[8])

    @pl.when(c == 0)
    def _():
        arrived(s_in.at[0:16], last_r.at[1])

    @pl.when(c == 1)
    def _():
        arrived(s_in.at[0:15], last_r.at[1])

    message = jnp.sum(s_in[0:16], axis=0)
    count = float(VOCAB * EMBED)
    for t in range(2):
        u_sq, p_sq, r_mean = [jnp.sum(jnp.where(lane == 3 * t + i, message, 0.0), axis=1, keepdims=True) for i in range(3)]
        u_rms = jnp.sqrt(u_sq * r_mean / count)
        p_rms = jnp.sqrt(p_sq / count)
        step = LEARN_RATE * jnp.maximum(SCALE_FLOOR, p_rms) / jnp.maximum(1.0, u_rms / CLIP_LIMIT)
        scale_out[t] = jnp.broadcast_to(factor_cols[t] * (step * jnp.sqrt(r_mean)), (COLS, LANES))

    @pl.when(c == 1)
    def _():
        arrived(s_in.at[0:31], send.at[9])


def update_kernel(emb_g, head_g, emb_p, head_p, emb_rows, head_rows, emb_cols, head_cols, scale,
                  emb_new, head_new, emb_rows_new, head_rows_new, emb_cols_new, head_cols_new, emb_half, head_half,
                  new_buf, half_buf, small_sem, big_sem):
    small = [pltpu.make_async_copy(src, dst, small_sem.at[i]) for i, (src, dst) in enumerate(
        ((emb_rows, emb_rows_new), (head_rows, head_rows_new), (emb_cols, emb_cols_new), (head_cols, head_cols_new)))]
    for cp in small:
        cp.start()
    size = ROWS // PARTS
    tables = ((emb_p, emb_g, emb_new, emb_half), (head_p, head_g, head_new, head_half))
    for i in range(PARTS):
        part = slice(i * size, (i + 1) * size)
        for t, (p, g, new, half) in enumerate(tables):
            value = p[:, part] - g[:, part] * jnp.concatenate([scale[t]] * (size // LANES), axis=1)
            new_buf[t, :, part] = value
            half_buf[t, :, part] = value.astype(jnp.bfloat16)
            pltpu.make_async_copy(new_buf.at[t, :, part], new.at[:, part], big_sem.at[0]).start()
            pltpu.make_async_copy(half_buf.at[t, :, part], half.at[:, part], big_sem.at[1]).start()
    for cp in small:
        cp.wait()
    pltpu.make_async_copy(new_buf, new_buf, big_sem.at[0]).wait()
    pltpu.make_async_copy(half_buf, half_buf, big_sem.at[1]).wait()


def local_step(emb_p, head_p, emb_g, head_g, emb_r, emb_c, head_r, head_c):
    f32 = jnp.float32
    n = CHUNKS
    dma = pltpu.SemaphoreType.DMA
    hbm = pl.BlockSpec(memory_space=pltpu.HBM)
    vmem = pl.BlockSpec(memory_space=pltpu.VMEM)
    rows_shape = (BLOCKS, 2, LANES)
    table = jax.ShapeDtypeStruct((COLS, ROWS), f32)
    half = jax.ShapeDtypeStruct((COLS, ROWS), jnp.bfloat16)
    emb_p = emb_p.T
    shapes = [(2, ROWS // 2, EMBED), (n, 2, 2, 2, COLS, LANES), (2, n, 2, 2, 2, COLS, LANES)]
    shapes += [(n, 2, 2, 2, COLS, LANES), (n, 2, 2, COLS, LANES), (PAIRS, 2, 2, COLS, LANES)]
    shapes += [(BLOCKS, 4, LANES), (2, *rows_shape), (2, 2, 1, COLS)]
    shapes += [(PAIRS, 4, LANES), (PAIRS, 4, LANES), (3 * PAIRS, 4, LANES)]
    shapes += [(2, 2, COLS, LANES)] * 2 + [(4, LANES), (2, LANES)]
    shapes += [(2, 2, 2, LANES), (8, 2, 2, 2, LANES), (2, 2, 2, LANES), (1, LANES), (32, 1, LANES)]
    scratch = [pltpu.VMEM(shape, f32) for shape in shapes]
    scratch += [dma((len(GROUPS) + 1,))] * 2 + [dma((RING,))] * 2 + [dma((SWAPS,))] + [dma((SHORT,))] * 2 + [dma((SWAPS,))]
    scratch += [dma((10,)), dma((2,)), dma((4,)), pltpu.SemaphoreType.REGULAR((2,))]
    kept = [pltpu.VMEM((COLS, ROWS), f32)] * 4 + [pltpu.VMEM(rows_shape, f32)] * 2 + [pltpu.VMEM((1, COLS), f32)] * 2
    kept.append(pltpu.VMEM((2, COLS, LANES), f32))
    state = pl.pallas_call(
        exchange_kernel,
        out_shape=tuple(kept),
        in_specs=[hbm] * 8,
        out_specs=(vmem,) * 9,
        scratch_shapes=scratch,
        compiler_params=pltpu.CompilerParams(collective_id=0, has_side_effects=True, vmem_limit_bytes=60_000_000),
        name="exchange",
    )(emb_g.reshape(ROWS, EMBED), head_g.reshape(2, 2, 2, COLS, ROWS), emb_p, head_p,
      emb_r.reshape(rows_shape), head_r.reshape(rows_shape), emb_c.reshape(1, COLS), head_c.reshape(1, COLS))

    outs = pl.pallas_call(
        update_kernel,
        out_shape=(table, table, jax.ShapeDtypeStruct(rows_shape, f32), jax.ShapeDtypeStruct(rows_shape, f32),
                   jax.ShapeDtypeStruct((1, COLS), f32), jax.ShapeDtypeStruct((1, COLS), f32), half, half),
        in_specs=[vmem] * 9,
        out_specs=(hbm,) * 8,
        scratch_shapes=[pltpu.VMEM((2, COLS, ROWS), f32), pltpu.VMEM((2, COLS, ROWS), jnp.bfloat16),
                        dma((4,)), dma((2,))],
        compiler_params=pltpu.CompilerParams(vmem_limit_bytes=16 * 2 ** 20),
        name="update",
    )(*state)
    emb_new, head_new, emb_rn, head_rn, emb_cn, head_cn, emb_half, head_half = outs
    return (emb_new.T, head_new, emb_rn.reshape(ROWS), emb_cn.reshape(COLS), head_rn.reshape(ROWS),
            head_cn.reshape(COLS), emb_half.T, head_half)


def solution(mesh):
    arg_specs = (P("model", "data"), P("data", "model"), P("data", "model", None), P("data", None, "model"),
                 P("model"), P("data"), P("model"), P("data"))
    result_specs = (P("model", "data"), P("data", "model"), P("model"), P("data"), P("model"), P("data"),
                    P("model", "data"), P("data", "model"))
    mapped = jax.shard_map(local_step, mesh=mesh, in_specs=arg_specs, out_specs=result_specs, check_vma=False)

    def update_tables(emb_param, head_param, emb_grad, head_grad, emb_row, emb_col, head_row, head_col):
        return mapped(emb_param, head_param, emb_grad, head_grad, emb_row, emb_col, head_row, head_col)

    return update_tables
```
